32 devices in a mesh: grid: 4 (over z), line: 8 (over y, x, core).
Axes of the slice: x: 2, y: 2, z: 4, core: 2. Of those that a mesh axis runs over, the one named last changes fastest.
Arguments:
- les: float32 [24, 4, 1024], P(None, 'grid', 'line'), may hold values from -6 to 6
- lines: float32 [4, 8, 128, 24, 128], P('grid', 'line'), may hold values from -6 to 6
- triplet_start: int32 [2, 4, 8, 128], P(None, 'grid', 'line'), may hold values from 0 to 80
- splice_owner: int32 [2, 4, 8, 128, 1], P(None, 'grid', 'line'), may hold values from 0 to 31; in each aligned block of 128 rows (0 to 127, 128 to 255, ..., all dimensions but the last counted through in order) at most 8 rows name the same one
- splice_line: int32 [2, 4, 8, 128], P(None, 'grid', 'line'), may hold values from 0 to 127
- splice_from: int32 [2, 4, 8, 128], P(None, 'grid', 'line'), may hold values from 0 to 7
- splice_to: int32 [2, 4, 8, 128], P(None, 'grid', 'line'), may hold values from 0 to 7
- chem_counts: int32 [4, 8, 128], P('grid', 'line'), may hold values from 1 to 6, as said below
- diffusivity: float32 [24], replicated, may hold values from 0.5 to 20
- rates: float32 [24, 24], replicated, may hold values from -1.25 to 1.25
- frozen_inverse: float32 [24, 24], replicated, may hold values from -0.3 to 0.5
Outputs:
- les_out: float32 [24, 4, 1024], P(None, 'grid', 'line')
- lines_out: float32 [4, 8, 128, 24, 128], P('grid', 'line')
The draws below stay inside these ranges and needn't reach their ends.
Inputs may be any that keep to these rules, and one draw needn't show every extreme that they name: `splice_owner`: in the rows of one device and one step no owner is named more than 8 times, a bound that some block reaches. `chem_counts`: some line has 6 substeps.
All inputs are finite; a program needn't handle non-finite values.
Results may differ from the reference program's by a relative error of at most 0.0003.
Values sent between devices are 32-bit elements; how exact they have to be, the bound alone decides.
A program may use at most 64 MiB of HBM per device.

```python
import math
import jax
import jax.numpy as jnp
import numpy as np
from jax import lax

S = 24
P_SIZE = 128
SEG = 16
TRIP = 48
KMAX = 6
STEPS = 2
CX = 1
CY = 128
LINES_DEV = 128
NX = 4
NY = 1024
NSEG = 8
CAP = 8
N_GRID = 4
N_LINE = 8
DEVICES = 32


def draw_chem_counts(key, part):
    first = jax.random.fold_in(key, 11)
    second = jax.random.fold_in(key, 12)
    ceiling = jax.random.randint(first, (N_GRID, N_LINE, 1), 1, KMAX + 1)
    ceiling = ceiling.at[0, 0, 0].set(KMAX)
    counts = 1 + jax.random.randint(second, (N_GRID, N_LINE, LINES_DEV), 0, ceiling)
    counts = counts.at[0, 0, 0].set(KMAX)
    return counts.astype(jnp.int32)


def draw_frozen_inverse(key, part):
    first = jax.random.fold_in(key, 21)
    second = jax.random.fold_in(key, 22)
    diagonal = jax.random.uniform(first, (S,), jnp.float32, 0.2, 0.5)
    off_diag = jnp.clip(0.06 * jax.random.normal(second, (S, S), jnp.float32), -0.3, 0.3)
    ident = jnp.eye(S, dtype=jnp.float32)
    return (ident * diagonal[None, :] + (1.0 - ident) * off_diag).astype(jnp.float32)


def plant(values, rng, smallest, high):
    shape = values.shape
    spot = [jax.random.randint(jax.random.fold_in(rng, axis), (), 0, shape[axis]) for axis in range(len(shape))]
    values = values.at[tuple(spot)].set(smallest)
    longest = shape.index(max(shape))
    spot[longest] = (spot[longest] + 1) % shape[longest]
    return values.at[tuple(spot)].set(high)


def block_levels(key, extent, shards, smallest, largest):
    factor_of = 1.0
    for axis_at, blocks in shards:
        heights = jax.random.uniform(jax.random.fold_in(jax.random.fold_in(key, 6), axis_at), (blocks,), jnp.float32, smallest / len(shards), largest / len(shards))
        factor_of = factor_of * jnp.repeat(jnp.exp(heights), extent[axis_at] // blocks).reshape((-1,) + (1,) * (len(extent) - 1 - axis_at))
    return factor_of


def routed_block(own_key, own, number, rows, count, top, limit, slope):
    sequence = jax.random.permutation(own_key, count)
    crowded, common = load_shares(count, rows * top, limit, slope, True), load_shares(count, rows * top, limit, slope, False)
    places = jnp.arange(count)

    def named(sizes, turn):
        used = int((sizes > 0).sum())
        fixed = max(1, used // 4)
        passed = fixed + (places - fixed + turn * (used - fixed)) % max(1, count - fixed)
        return jnp.zeros((count,), jnp.int32).at[sequence[jnp.where(places < fixed, places, passed)]].set(jnp.asarray(sizes, jnp.int32))

    sizes = jnp.where(number % 4 == 0, named(crowded, number // 4), named(common, number - number // 4 - 1))
    mixed = jax.random.permutation(jax.random.fold_in(own, 3), count)
    donor, receiver = mixed[0:count // 2 * 2:2], mixed[1:count // 2 * 2:2]
    room = jnp.minimum(sizes[donor] - 1, limit - sizes[receiver]) // 2
    room = jnp.where((donor == sequence[0]) | (receiver == sequence[0]) | (sizes[receiver] == 0), 0, jnp.maximum(room, 0))
    passed = jax.random.randint(jax.random.fold_in(own, 4), (count // 2,), 0, 1 << 20) % (room + 1)
    sizes = sizes.at[donor].add(-passed).at[receiver].add(passed)
    labels = jnp.searchsorted(jnp.cumsum(sizes), jnp.arange(rows * top), side="right").astype(jnp.int32)
    listing = labels.reshape(top, rows).T
    listing = listing[jax.random.permutation(jax.random.fold_in(own, 1), rows)]
    turn = jax.random.randint(jax.random.fold_in(own, 2), (rows, 1), 0, top)
    return jnp.take_along_axis(listing, (jnp.arange(top)[None, :] + turn) % top, axis=1)


def load_shares(number_of, total, most, slope, full):
    loads = [(1 << 20) // math.isqrt(grade ** slope) + 1 for grade in range(1, number_of + 1)]
    largest = most if full else min(most, max(-(-total // number_of), total * loads[0] // sum(loads)))
    least = 1 if total - largest >= number_of - 1 else 0
    given, spare = [largest] + [least] * (number_of - 1), total - largest - least * (number_of - 1)
    while spare > 0:
        free = [i for i in range(1, number_of) if given[i] < largest] or [i for i in range(1, number_of) if given[i] < most]
        pool, left = sum([loads[i] for i in free]), spare
        for i in free:
            addition = min(most - given[i], max(1, left * loads[i] // pool), spare)
            given[i] = given[i] + addition
            spare = spare - addition
    return np.array(given)


def centred(rng, dims, width, bound, shards=(), held_as=jnp.bfloat16):
    drawn = width * jax.random.normal(rng, dims, jnp.float32)
    if shards:
        drawn = drawn * block_levels(rng, dims, shards, -0.22, 0.18)
    return jnp.clip(drawn, -bound, bound).astype(held_as)


def setup_inputs(seed: int = 0) -> dict:
    key_of = jax.random.split(jax.random.key(seed), 12)
    les = centred(key_of[0], (S, NX, NY), 1.0, 6.0, ((1, 4), (2, 8)), jnp.float32)
    lines = centred(key_of[1], (N_GRID, N_LINE, LINES_DEV, S, P_SIZE), 1.0, 6.0, ((0, 4), (1, 8)), jnp.float32)
    triplet_start = plant(jax.random.randint(key_of[2], (STEPS, N_GRID, N_LINE, LINES_DEV), 0, P_SIZE - TRIP + 1), jax.random.fold_in(key_of[2], 1), 0, P_SIZE - TRIP).astype(jnp.int32)
    splice_owner_keys = jax.random.split(jax.random.fold_in(key_of[3], 1), STEPS * N_GRID * N_LINE * LINES_DEV // LINES_DEV)
    splice_owner_turns = jax.random.permutation(jax.random.fold_in(key_of[3], 3), STEPS * N_GRID * N_LINE * LINES_DEV // LINES_DEV)
    splice_owner = jax.vmap(lambda own, number: routed_block(jax.random.fold_in(key_of[3], 2), own, number, LINES_DEV, DEVICES, 1, CAP, 2))(splice_owner_keys, splice_owner_turns).reshape((STEPS, N_GRID, N_LINE, LINES_DEV, 1))
    splice_line = plant(jax.random.randint(key_of[4], (STEPS, N_GRID, N_LINE, LINES_DEV), 0, LINES_DEV), jax.random.fold_in(key_of[4], 1), 0, LINES_DEV - 1).astype(jnp.int32)
    splice_from = plant(jax.random.randint(key_of[5], (STEPS, N_GRID, N_LINE, LINES_DEV), 0, NSEG), jax.random.fold_in(key_of[5], 1), 0, NSEG - 1).astype(jnp.int32)
    splice_to = plant(jax.random.randint(key_of[6], (STEPS, N_GRID, N_LINE, LINES_DEV), 0, NSEG), jax.random.fold_in(key_of[6], 1), 0, NSEG - 1).astype(jnp.int32)
    chem_counts = draw_chem_counts(jax.random.fold_in(key_of[11], 71), 0)
    diffusivity = jnp.clip(jnp.exp(jax.random.uniform(key_of[8], (S,), jnp.float32, math.log(0.5), math.log(20.0))), 0.5, 20.0)
    rates = centred(key_of[9], (S, S), S ** -0.5, 1.25, (), jnp.float32)
    frozen_inverse = draw_frozen_inverse(jax.random.fold_in(key_of[11], 71), 0)
    return dict(les=les, lines=lines, triplet_start=triplet_start, splice_owner=splice_owner, splice_line=splice_line, splice_from=splice_from, splice_to=splice_to, chem_counts=chem_counts, diffusivity=diffusivity, rates=rates, frozen_inverse=frozen_inverse)


les_rate = 0.2
relax_rate = 0.5
splice_weight = 0.5

def diffusion_inverse(diffusivity, points):
    place = jnp.arange(points)
    ends = ((place == 0) | (place == points - 1)).astype(jnp.float32)
    coeff = diffusivity[:, None]
    main = 1.0 + coeff * (2.0 - ends[None, :])
    off_diag = -coeff * jnp.ones((1, points), jnp.float32)
    lower = jnp.where(place[None, :] == 0, jnp.float32(0.0), off_diag)
    upper = jnp.where(place[None, :] == points - 1, jnp.float32(0.0), off_diag)
    ident = jnp.broadcast_to(jnp.eye(points, dtype=jnp.float32), (diffusivity.shape[0], points, points))
    return lax.linalg.tridiagonal_solve(lower, main, upper, ident)

def triplet_index(start, points, length):
    place = jnp.arange(points).astype(jnp.int32)
    rel = place[None, :] - start[:, None].astype(jnp.int32)
    third = length // 3
    source = jnp.where(rel < third, 3 * rel, jnp.where(rel < 2 * third, 3 * (2 * third - 1 - rel) + 1, 3 * (rel - 2 * third) + 2))
    inside = (rel >= 0) & (rel < length)
    return jnp.where(inside, source + start[:, None].astype(jnp.int32), place[None, :]).astype(jnp.int32)

def chemistry(state, counts, rates, frozen_inverse):
    for sub in range(KMAX):
        active = (counts > sub)[:, None, None]
        source = jnp.einsum('st,ltp->lsp', rates, jnp.tanh(state), precision=lax.Precision.HIGHEST)
        change = jnp.einsum('st,ltp->lsp', frozen_inverse, source, precision=lax.Precision.HIGHEST)
        state = jnp.where(active, state + change, state)
    return state

def reference(les, lines, triplet_start, splice_owner, splice_line, splice_from, splice_to, chem_counts, diffusivity, rates, frozen_inverse):
    inverse = diffusion_inverse(diffusivity, P_SIZE)
    total = N_GRID * N_LINE * LINES_DEV
    field = les
    state = lines.reshape(total, S, P_SIZE)
    counts = chem_counts.reshape(total)
    rows = jnp.arange(total).astype(jnp.int32)
    for step in range(STEPS):
        padded = jnp.pad(field, ((0, 0), (1, 1), (1, 1)))
        beside = padded[:, 2:, 1:-1] + padded[:, :-2, 1:-1] + padded[:, 1:-1, 2:] + padded[:, 1:-1, :-2]
        mid = field + les_rate * (beside - 4.0 * field)
        cellwise = mid.reshape(S, N_GRID, CX, N_LINE, CY).transpose(1, 3, 2, 4, 0).reshape(total, S)
        state = state + relax_rate * (cellwise - jnp.mean(state, axis=2))[:, :, None]
        index = triplet_index(triplet_start[step].reshape(total), P_SIZE, TRIP)
        state = jnp.take_along_axis(state, index[:, None, :], axis=2)
        state = jnp.einsum('lsp,sqp->lsq', state, inverse, precision=lax.Precision.HIGHEST)
        state = chemistry(state, counts, rates, frozen_inverse)
        four = state.reshape(total, S, NSEG, SEG)
        outgoing = four[rows, :, splice_from[step].reshape(total).astype(jnp.int32), :]
        target = (splice_owner[step].reshape(total) * LINES_DEV + splice_line[step].reshape(total)).astype(jnp.int32)
        landing = splice_to[step].reshape(total).astype(jnp.int32)
        previous = four[target, :, landing, :]
        four = four.at[target, :, landing, :].add(splice_weight * (outgoing - previous))
        state = four.reshape(total, S, P_SIZE)
        filtered = jnp.mean(state, axis=2)
        back = filtered.reshape(N_GRID, N_LINE, CX, CY, S).transpose(4, 0, 2, 1, 3).reshape(S, NX, NY)
        field = 0.5 * mid + 0.5 * back
    return (field, state.reshape(lines.shape))
```

```python
import functools

import jax
import jax.numpy as jnp
from jax import lax
from jax.experimental import pallas as pl
from jax.experimental.pallas import tpu as pltpu
from jax.sharding import PartitionSpec as P

SEG = 16
TRIP = 48
STEPS = 2
SUBSTEPS = 6

les_rate = 0.2
relax_rate = 0.5
splice_weight = 0.5

NAMES = ("grid", "line")
MESH = pl.DeviceIdType.MESH
VMEM = pl.BlockSpec(memory_space=pltpu.VMEM)
SMEM = pl.BlockSpec(memory_space=pltpu.SMEM)
ANY = pl.BlockSpec(memory_space=pl.ANY)
f32 = jnp.float32
bf16 = jnp.bfloat16
i32 = jnp.int32

dot = functools.partial(jnp.dot, preferred_element_type=jnp.float32)


def halves(value):
    top = value.astype(bf16)
    return top, (value - top.astype(f32)).astype(bf16)


def column(row):
    points = row.shape[1]
    return jnp.transpose(jnp.broadcast_to(row, (points, points)))


def iota(shape, axis):
    return lax.broadcasted_iota(i32, shape, axis)


def bits(size):
    assert size & (size - 1) == 0
    return size.bit_length() - 1


def when(condition, value):
    return jnp.where(condition, value, 0)


def total_of(value, axis):
    return jnp.sum(value, axis=axis, keepdims=True, dtype=i32)


def kernel(
    slots,
    les_ref,
    lines_ref,
    start_ref,
    owner_ref,
    line_ref,
    from_ref,
    to_ref,
    matrix_ref,
    coeff_ref,
    counts_ref,
    les_out,
    lines_out,
    y_ref,
    z_ref,
    m_top,
    m_rest,
    send_ref,
    recv_0,
    recv_1,
    sums_ref,
    weight_ref,
    rim_ref,
    field_ref,
    mid_ref,
    aim_ref,
    got_ref,
    flat_ref,
    tab_ref,
    tab_smem,
    load_sem,
    tab_sem,
    rim_send,
    rim_recv,
    aim_send,
    aim_recv,
    send_sem,
    recv_sem,
    out_sem,
):
    species, lines = les_ref.shape
    points = y_ref.shape[2]
    segments = points // SEG
    size = [lax.axis_size(n) for n in NAMES]
    at = [lax.axis_index(n) for n in NAMES]
    groups = size[0] * size[1]
    me = at[0] * size[1] + at[1]
    total = groups * slots
    blocks = total // points
    recv_refs = (recv_0, recv_1)

    def place(j):
        peer = lax.rem(me + j, groups)
        return peer, (peer // size[1], lax.rem(peer, size[1]))

    barrier = pltpu.get_barrier_semaphore()

    def greet(j, carry):
        pl.semaphore_signal(barrier, inc=1, device_id=place(j)[1], device_id_type=MESH)
        return carry

    lax.fori_loop(1, groups, greet, 0)
    load = pltpu.make_async_copy(lines_ref, y_ref, load_sem)
    load.start()

    rims = []
    for axis in (0, 1):
        for move in (1, size[axis] - 1):
            there = list(at)
            there[axis] = lax.rem(at[axis] + move, size[axis])
            rims.append(tuple(there))

    def rim_copies(step):
        return [
            pltpu.make_async_remote_copy(
                src_ref=field_ref.at[step],
                dst_ref=rim_ref.at[step, k],
                send_sem=rim_send.at[step, k],
                recv_sem=rim_recv.at[step, k],
                device_id=rims[k],
                device_id_type=MESH,
            )
            for k in range(4)
        ]

    def aim_copy(j):
        peer, device = place(j)
        return pltpu.make_async_remote_copy(
            src_ref=aim_ref.at[(peer * slots) // points],
            dst_ref=got_ref.at[me],
            send_sem=aim_send.at[j],
            recv_sem=aim_recv.at[j],
            device_id=device,
            device_id_type=MESH,
        )

    def data_copy(step, j):
        peer, device = place(j)
        return pltpu.make_async_remote_copy(
            src_ref=send_ref.at[step, peer],
            dst_ref=recv_refs[step].at[me],
            send_sem=send_sem.at[step, j],
            recv_sem=recv_sem.at[step, j],
            device_id=device,
            device_id_type=MESH,
        )

    field_ref[0] = les_ref[...]

    lane = iota((points, points), 1)
    row = iota((points, points), 0)
    for step in range(STEPS):
        owner = owner_ref[step : step + 1, :]
        rank = total_of(when((column(owner) == owner) & (row < lane), 1), 0)
        spot = column(owner * slots + rank)
        code = column(iota((1, points), 1) * segments + from_ref[step : step + 1, :])
        aim = column(line_ref[step : step + 1, :] * segments + to_ref[step : step + 1, :] + 1)
        for b in range(blocks):
            hit = spot == lane + b * points
            tab_ref[step * blocks + b] = total_of(when(hit, code), 0)
            aim_ref[b, step : step + 1, :] = total_of(when(hit, aim), 0)
    send_rows = STEPS * blocks
    send_table = pltpu.make_async_copy(tab_ref.at[pl.ds(0, send_rows)], tab_smem.at[pl.ds(0, send_rows)], tab_sem.at[0])
    send_table.start()

    apart = jnp.abs(lane - row).astype(f32)
    both = (lane + row).astype(f32)

    def inverse(s, carry):
        coeff = jnp.full((8, points), coeff_ref[s], f32)
        root = jnp.sqrt(4.0 * coeff + 1.0)
        theta = -jnp.log(2.0 * coeff / (2.0 * coeff + 1.0 + root))
        scale = 1.0 / (root * (1.0 - jnp.exp(-2.0 * points * theta)))
        theta = theta[:1]
        value = jnp.exp(-apart * theta) + jnp.exp((apart - 2.0 * points) * theta)
        value = value + jnp.exp(-(both + 1.0) * theta) + jnp.exp((both + 1.0 - 2.0 * points) * theta)
        top, rest = halves(value * scale[:1] - relax_rate / points)
        m_top[s] = top
        m_rest[s] = rest
        return carry

    lax.fori_loop(0, species, inverse, 0)

    pl.semaphore_wait(barrier, groups - 1)
    for copy in rim_copies(0):
        copy.start()

    def aim_start(j, carry):
        aim_copy(j).start()
        return carry

    lax.fori_loop(1, groups, aim_start, 0)
    got_ref[me] = aim_ref[(me * slots) // points]

    flat_y = y_ref.reshape(lines * species, points)
    flat_z = z_ref.reshape(lines * species, points)

    def diffuse(step):
        rel = lane - column(start_ref[step : step + 1, :])
        third = TRIP // 3
        source = jnp.where(
            rel < third,
            3 * rel,
            jnp.where(rel < 2 * third, 3 * (2 * third - 1 - rel) + 1, 3 * (rel - 2 * third) + 2),
        )
        index = jnp.where((rel >= 0) & (rel < TRIP), source + (lane - rel), lane)

        def one(s, carry):
            y = flat_y[pl.ds(s, lines, stride=species), :]
            y = jnp.take_along_axis(y, index, axis=1, mode="promise_in_bounds")
            top, rest = halves(y)
            out = dot(top, m_top[s]) + dot(rest, m_top[s]) + dot(top, m_rest[s])
            flat_z[pl.ds(s, lines, stride=species), :] = out
            return carry

        lax.fori_loop(0, species, one, 0, unroll=4)

    lane_s = lax.broadcasted_iota(i32, (species, points), 1)

    def middle(step):
        field = field_ref[step]
        up = jnp.where(at[0] > 0, rim_ref[step, 0], 0.0)
        down = jnp.where(at[0] < size[0] - 1, rim_ref[step, 1], 0.0)
        left = jnp.where(at[1] > 0, rim_ref[step, 2], 0.0)
        right = jnp.where(at[1] < size[1] - 1, rim_ref[step, 3], 0.0)
        before = pltpu.roll(jnp.where(lane_s == points - 1, left, field), 1, 1)
        after = pltpu.roll(jnp.where(lane_s == 0, right, field), points - 1, 1)
        mid_ref[...] = field + les_rate * (up + down + before + after - 4.0 * field)

    matrix = matrix_ref[...]
    chunk = 64

    def substep(sub, in_ref, out_ref, lift):
        def part(c, inner):
            base = c * chunk
            mid = mid_ref[...] if lift else None
            for q in range(0, chunk, 4):
                columns = []
                state = []
                for h in (0, 2):
                    y = in_ref[pl.ds(base + q + h, 2)].reshape(2 * species, points)
                    if lift:
                        add = [
                            jnp.take_along_axis(
                                mid, jnp.full((species, points), base + q + h + k, i32), axis=1, mode="promise_in_bounds"
                            )
                            for k in (0, 1)
                        ]
                        y = y + relax_rate * jnp.concatenate(add, axis=0)
                    state.append(y)
                    top, rest = halves(jnp.tanh(y))
                    columns.append(jnp.concatenate([top, top, rest], axis=0))
                right = jnp.concatenate(columns, axis=1)
                change = dot(matrix, right)
                for h in (0, 1):
                    for k in (0, 1):
                        l = base + q + 2 * h + k
                        factor = jnp.where(counts_ref[l] > sub, f32(1.0), f32(0.0))
                        rows = slice(k * species, (k + 1) * species)
                        value = state[h][rows] + factor * change[rows, h * points : (h + 1) * points]
                        out_ref[l] = value
            return inner

        lax.fori_loop(0, lines // chunk, part, 0)

    def chemistry():
        substep(0, z_ref, y_ref, True)

        def two(pair, carry):
            substep(2 * pair + 1, y_ref, z_ref, False)
            substep(2 * pair + 2, z_ref, y_ref, False)
            return carry

        lax.fori_loop(0, SUBSTEPS // 2 - 1, two, 0)
        substep(SUBSTEPS - 1, y_ref, z_ref, False)

    segment = lane_s // SEG

    def pack(step, peer):
        tile = jnp.zeros((species, points), f32)
        for k in range(slots):
            q = peer * slots + k
            code = tab_smem[step * blocks + q // points, 0, lax.rem(q, points)]
            value = z_ref[code >> bits(segments)]
            value = pltpu.roll(value, (SEG * (k - (code & (segments - 1)))) & (points - 1), 1)
            tile = jnp.where(segment == k, value, tile)
        return tile

    def exchange(step):
        def begin(j, carry):
            peer, _ = place(j)
            send_ref[step, peer] = pack(step, peer)

            @pl.when(j > 1)
            def _():
                data_copy(step, j - 1).start()

            return carry

        lax.fori_loop(1, groups, begin, 0)
        recv_refs[step][me] = pack(step, me)
        data_copy(step, groups - 1).start()

    def arrivals():
        number = iota((total, 1), 0)
        lane_t = iota((total, points), 1)
        number_r = iota((1, total), 1)
        offset = lax.rem(me * slots, points)
        mine = offset + (iota((total, points), 0) & (slots - 1))
        for step in range(STEPS):
            for r in range(groups):
                flat_ref[r * slots : (r + 1) * slots, :] = jnp.broadcast_to(
                    got_ref[r, step : step + 1, :], (slots, points)
                )
            code = total_of(when(lane_t == mine, flat_ref[...]), 1)
            valid = code > 0
            code = code - 1
            line = jnp.where(valid, code >> bits(segments), lines)
            seg = code & (segments - 1)
            line_c = jnp.broadcast_to(line, (total, points))
            line_r = jnp.concatenate(
                [jnp.transpose(line_c[b * points : (b + 1) * points])[:1] for b in range(blocks)], axis=1
            )
            key_r = line_r * total + number_r
            key_c = line * total + number
            below = key_r < key_c
            position = total_of(when(below, 1), 1)
            same = total_of(when(below & (line_r == line), 1), 1)
            value = (number * segments + seg) * 2 + when(same == 0, 1)
            base = send_rows + step * (blocks + 1)
            for b in range(blocks):
                tab_ref[base + b] = total_of(when(position == lane_t + b * points, value), 0)
            upto = total_of(when(line_c <= lane_t, 1), 0)
            many = total_of(when(line_c == lane_t, 1), 0)
            tab_ref[base + blocks] = jnp.maximum(upto - 1, 0) * 2 + when(many > 0, 1)
            lands = jnp.where(line_r == iota((lines, total), 0), 1.0, 0.0).astype(bf16)
            covers = jnp.where(seg == (lane_t >> bits(SEG)), 1.0, 0.0).astype(bf16)
            weight_ref[step] = 1.0 - splice_weight * dot(lands, covers)
        rows = STEPS * (blocks + 1)
        copy = pltpu.make_async_copy(
            tab_ref.at[pl.ds(send_rows, rows)], tab_smem.at[pl.ds(send_rows, rows)], tab_sem.at[1]
        )
        copy.start()
        copy.wait()

    def collect(step):
        def finish(j, carry):
            data_copy(step, j).wait()
            return carry

        lax.fori_loop(1, groups, finish, 0)

    def land(step):
        base = send_rows + step * (blocks + 1)

        def run(n, acc):
            code = tab_smem[base + n // points, 0, lax.rem(n, points)]
            first = code & 1
            seg = (code >> 1) & (segments - 1)
            number = code >> bits(2 * segments)
            source = number >> bits(slots)
            k = number & (slots - 1)
            value = pltpu.roll(recv_refs[step][source], (SEG * (seg - k)) & (points - 1), 1)
            value = jnp.where(segment == seg, value, 0.0)
            acc = value + jnp.where(first == 1, f32(0.0), f32(1.0)) * acc
            sums_ref[n] = acc
            return acc

        lax.fori_loop(0, total, run, jnp.zeros((species, points), f32), unroll=8)

        def settle(l, sums):
            code = tab_smem[base + blocks, 0, l]
            factor = jnp.where((code & 1) == 1, f32(splice_weight), f32(0.0))
            value = z_ref[l] * weight_ref[step, pl.ds(l, 1), :] + factor * sums_ref[code >> 1]
            y_ref[l] = value
            return jnp.where(lane_s == l, jnp.sum(value, axis=1, keepdims=True), sums)

        sums = lax.fori_loop(0, lines, settle, jnp.zeros((species, points), f32), unroll=8)
        return 0.5 * mid_ref[...] + (0.5 / points) * sums

    load.wait()
    diffuse(0)
    for copy in rim_copies(0):
        copy.wait()
    middle(0)
    send_table.wait()
    chemistry()
    exchange(0)

    def aim_finish(j, carry):
        aim_copy(j).wait()
        return carry

    lax.fori_loop(1, groups, aim_finish, 0)
    arrivals()
    collect(0)
    field_ref[1] = land(0)
    for copy in rim_copies(1):
        copy.start()
    diffuse(1)
    for copy in rim_copies(1):
        copy.wait()
    middle(1)
    chemistry()
    exchange(1)
    collect(1)
    les_out[...] = land(1)
    out = pltpu.make_async_copy(y_ref, lines_out, out_sem)
    out.start()
    out.wait()


def body(
    les,
    lines,
    triplet_start,
    splice_owner,
    splice_line,
    splice_from,
    splice_to,
    chem_counts,
    diffusivity,
    rates,
    frozen_inverse,
):
    groups = lax.axis_size("grid") * lax.axis_size("line")
    _, _, count, species, points = lines.shape
    segments = points // SEG
    slots = min(segments, max(2, 2 * count // groups))
    total = groups * slots
    blocks = total // points
    rows = STEPS * (2 * blocks + 1)

    joint = jnp.dot(frozen_inverse, rates, precision=lax.Precision.HIGHEST)
    twice = jnp.kron(jnp.eye(2, dtype=f32), joint)
    top = lax.reduce_precision(twice, 8, 7)
    rest = lax.reduce_precision(twice - top, 8, 7)
    matrix = jnp.concatenate([top, rest, top], axis=1).astype(bf16)

    dma = pltpu.SemaphoreType.DMA
    field, state = pl.pallas_call(
        functools.partial(kernel, slots),
        out_shape=(
            jax.ShapeDtypeStruct((species, count), f32),
            jax.ShapeDtypeStruct((count, species, points), f32),
        ),
        in_specs=[VMEM, ANY] + [VMEM] * 6 + [SMEM] * 2,
        out_specs=(VMEM, ANY),
        scratch_shapes=[
            pltpu.VMEM((count, species, points), f32),
            pltpu.VMEM((count, species, points), f32),
            pltpu.VMEM((species, points, points), bf16),
            pltpu.VMEM((species, points, points), bf16),
            pltpu.VMEM((STEPS, groups, species, points), f32),
            pltpu.VMEM((groups, species, points), f32),
            pltpu.VMEM((groups, species, points), f32),
            pltpu.VMEM((total, species, points), f32),
            pltpu.VMEM((STEPS, count, points), f32),
            pltpu.VMEM((STEPS, 4, species, count), f32),
            pltpu.VMEM((STEPS, species, count), f32),
            pltpu.VMEM((species, count), f32),
            pltpu.VMEM((blocks, STEPS, points), i32),
            pltpu.VMEM((groups, STEPS, points), i32),
            pltpu.VMEM((total, points), i32),
            pltpu.VMEM((rows, 1, points), i32),
            pltpu.SMEM((rows, 1, points), i32),
            dma,
            dma((2,)),
            dma((STEPS, 4)),
            dma((STEPS, 4)),
            dma((groups,)),
            dma((groups,)),
            dma((STEPS, groups)),
            dma((STEPS, groups)),
            dma,
        ],
        compiler_params=pltpu.CompilerParams(
            collective_id=0, has_side_effects=True, vmem_limit_bytes=40 * 1024 * 1024
        ),
        name="steps",
    )(
        les.reshape(species, count),
        lines.reshape(count, species, points),
        triplet_start.reshape(STEPS, count),
        splice_owner.reshape(STEPS, count),
        splice_line.reshape(STEPS, count),
        splice_from.reshape(STEPS, count),
        splice_to.reshape(STEPS, count),
        matrix,
        diffusivity,
        chem_counts.reshape(count),
    )
    return (field.reshape(les.shape), state.reshape(lines.shape))


def solution(mesh):
    in_specs = (
        P(None, "grid", "line"),
        P("grid", "line", None, None, None),
        P(None, "grid", "line", None),
        P(None, "grid", "line", None, None),
        P(None, "grid", "line", None),
        P(None, "grid", "line", None),
        P(None, "grid", "line", None),
        P("grid", "line", None),
        P(),
        P(),
        P(),
    )
    out_specs = (P(None, "grid", "line"), P("grid", "line", None, None, None))
    return jax.shard_map(body, mesh=mesh, in_specs=in_specs, out_specs=out_specs, check_vma=False)
```

```python
import functools

import jax
import jax.numpy as jnp
from jax import lax
from jax.experimental import pallas as pl
from jax.experimental.pallas import tpu as pltpu
from jax.sharding import PartitionSpec as P

SEG = 16
TRIP = 48
STEPS = 2
SUBSTEPS = 6

les_rate = 0.2
relax_rate = 0.5
splice_weight = 0.5

NAMES = ("grid", "line")
MESH = pl.DeviceIdType.MESH
VMEM = pl.BlockSpec(memory_space=pltpu.VMEM)
SMEM = pl.BlockSpec(memory_space=pltpu.SMEM)
HBM = pl.BlockSpec(memory_space=pltpu.HBM)
f32 = jnp.float32
bf16 = jnp.bfloat16
i32 = jnp.int32

dot = functools.partial(jnp.dot, preferred_element_type=jnp.float32)


def halves(value):
    top = value.astype(bf16)
    return top, (value - top.astype(f32)).astype(bf16)


def column(row):
    points = row.shape[1]
    return jnp.transpose(jnp.broadcast_to(row, (points, points)))


def iota(shape, axis):
    return lax.broadcasted_iota(i32, shape, axis)


def bits(size):
    assert size & (size - 1) == 0
    return size.bit_length() - 1


def when(condition, value):
    return jnp.where(condition, value, 0)


def total_of(value, axis):
    return jnp.sum(value, axis=axis, keepdims=True, dtype=i32)


def kernel(
    slots,
    les_hbm,
    lines_hbm,
    start_hbm,
    owner_hbm,
    line_hbm,
    from_hbm,
    to_hbm,
    matrix_hbm,
    coeff_hbm,
    counts_hbm,
    les_out,
    lines_out,
    les_ref,
    start_ref,
    owner_ref,
    line_ref,
    from_ref,
    to_ref,
    matrix_ref,
    coeff_ref,
    counts_ref,
    y_ref,
    z_ref,
    m_top,
    m_rest,
    send_ref,
    recv_0,
    recv_1,
    sums_ref,
    weight_ref,
    rim_ref,
    field_ref,
    mid_ref,
    aim_ref,
    got_ref,
    flat_ref,
    tab_ref,
    tab_smem,
    load_sem,
    tab_sem,
    rim_send,
    rim_recv,
    aim_send,
    aim_recv,
    send_sem,
    recv_sem,
    out_sem,
):
    parts = out_sem.shape[0] - 1
    species, _, lines = les_ref.shape
    points = y_ref.shape[2]
    segments = points // SEG
    size = [lax.axis_size(n) for n in NAMES]
    at = [lax.axis_index(n) for n in NAMES]
    groups = size[0] * size[1]
    me = at[0] * size[1] + at[1]
    total = groups * slots
    blocks = total // points
    recv_refs = (recv_0, recv_1)

    def place(j):
        peer = lax.rem(me + j, groups)
        return peer, (peer // size[1], lax.rem(peer, size[1]))

    barrier = pltpu.get_barrier_semaphore()

    def greet(j, carry):
        pl.semaphore_signal(barrier, inc=1, device_id=place(j)[1], device_id_type=MESH)
        return carry

    lax.fori_loop(1, groups, greet, 0)
    tables = [
        pltpu.make_async_copy(source, target, load_sem.at[n])
        for n, (source, target) in enumerate(
            [
                (coeff_hbm, coeff_ref),
                (owner_hbm, owner_ref),
                (from_hbm, from_ref),
                (line_hbm, line_ref),
                (to_hbm, to_ref),
                (les_hbm, les_ref),
                (start_hbm, start_ref),
                (counts_hbm, counts_ref),
                (matrix_hbm, matrix_ref),
            ]
        )
    ]
    load = pltpu.make_async_copy(lines_hbm, y_ref, load_sem.at[len(tables)])
    for copy in tables:
        copy.start()
    load.start()

    rims = []
    for axis in (0, 1):
        for move in (1, size[axis] - 1):
            there = list(at)
            there[axis] = lax.rem(at[axis] + move, size[axis])
            rims.append(tuple(there))

    def rim_copies(step):
        return [
            pltpu.make_async_remote_copy(
                src_ref=field_ref.at[step],
                dst_ref=rim_ref.at[step, k],
                send_sem=rim_send.at[step, k],
                recv_sem=rim_recv.at[step, k],
                device_id=rims[k],
                device_id_type=MESH,
            )
            for k in range(4)
        ]

    def aim_copy(j):
        peer, device = place(j)
        return pltpu.make_async_remote_copy(
            src_ref=aim_ref.at[(peer * slots) // points],
            dst_ref=got_ref.at[me],
            send_sem=aim_send.at[j],
            recv_sem=aim_recv.at[j],
            device_id=device,
            device_id_type=MESH,
        )

    def data_copy(step, j):
        peer, device = place(j)
        return pltpu.make_async_remote_copy(
            src_ref=send_ref.at[step, peer],
            dst_ref=recv_refs[step].at[me],
            send_sem=send_sem.at[step, j],
            recv_sem=recv_sem.at[step, j],
            device_id=device,
            device_id_type=MESH,
        )

    for copy in tables:
        copy.wait()
    field_ref[0] = les_ref[...].reshape(species, lines)

    lane = iota((points, points), 1)
    row = iota((points, points), 0)
    for step in range(STEPS):
        owner = owner_ref[step : step + 1, :]
        rank = total_of(when((column(owner) == owner) & (row < lane), 1), 0)
        spot = column(owner * slots + rank)
        code = column(iota((1, points), 1) * segments + from_ref[step : step + 1, :])
        aim = column(line_ref[step : step + 1, :] * segments + to_ref[step : step + 1, :] + 1)
        for b in range(blocks):
            hit = spot == lane + b * points
            tab_ref[step * blocks + b] = total_of(when(hit, code), 0)
            aim_ref[b, step : step + 1, :] = total_of(when(hit, aim), 0)
    send_rows = STEPS * blocks
    send_table = pltpu.make_async_copy(tab_ref.at[pl.ds(0, send_rows)], tab_smem.at[pl.ds(0, send_rows)], tab_sem.at[0])
    send_table.start()

    apart = jnp.abs(lane - row).astype(f32)
    both = (lane + row).astype(f32)

    def inverse(s, carry):
        coeff = jnp.full((8, points), coeff_ref[s], f32)
        root = jnp.sqrt(4.0 * coeff + 1.0)
        theta = -jnp.log(2.0 * coeff / (2.0 * coeff + 1.0 + root))
        scale = 1.0 / (root * (1.0 - jnp.exp(-2.0 * points * theta)))
        theta = theta[:1]
        value = jnp.exp(-apart * theta) + jnp.exp((apart - 2.0 * points) * theta)
        value = value + jnp.exp(-(both + 1.0) * theta) + jnp.exp((both + 1.0 - 2.0 * points) * theta)
        top, rest = halves(value * scale[:1] - relax_rate / points)
        m_top[s] = top
        m_rest[s] = rest
        return carry

    lax.fori_loop(0, species, inverse, 0)

    pl.semaphore_wait(barrier, groups - 1)
    for copy in rim_copies(0):
        copy.start()

    def aim_start(j, carry):
        aim_copy(j).start()
        return carry

    lax.fori_loop(1, groups, aim_start, 0)
    got_ref[me] = aim_ref[(me * slots) // points]

    flat_y = y_ref.reshape(lines * species, points)
    flat_z = z_ref.reshape(lines * species, points)

    def diffuse(step):
        rel = lane - column(start_ref[step : step + 1, :])
        third = TRIP // 3
        source = jnp.where(
            rel < third,
            3 * rel,
            jnp.where(rel < 2 * third, 3 * (2 * third - 1 - rel) + 1, 3 * (rel - 2 * third) + 2),
        )
        index = jnp.where((rel >= 0) & (rel < TRIP), source + (lane - rel), lane)

        def one(s, carry):
            y = flat_y[pl.ds(s, lines, stride=species), :]
            y = jnp.take_along_axis(y, index, axis=1, mode="promise_in_bounds")
            top, rest = halves(y)
            out = dot(top, m_top[s]) + dot(rest, m_top[s]) + dot(top, m_rest[s])
            flat_z[pl.ds(s, lines, stride=species), :] = out
            return carry

        lax.fori_loop(0, species, one, 0, unroll=4)

    lane_s = lax.broadcasted_iota(i32, (species, points), 1)

    def middle(step):
        field = field_ref[step]
        up = jnp.where(at[0] > 0, rim_ref[step, 0], 0.0)
        down = jnp.where(at[0] < size[0] - 1, rim_ref[step, 1], 0.0)
        left = jnp.where(at[1] > 0, rim_ref[step, 2], 0.0)
        right = jnp.where(at[1] < size[1] - 1, rim_ref[step, 3], 0.0)
        before = pltpu.roll(jnp.where(lane_s == points - 1, left, field), 1, 1)
        after = pltpu.roll(jnp.where(lane_s == 0, right, field), points - 1, 1)
        mid_ref[...] = field + les_rate * (up + down + before + after - 4.0 * field)

    matrix = matrix_ref[...]
    chunk = 64

    def substep(sub, in_ref, out_ref, lift):
        def part(c, inner):
            base = c * chunk
            mid = mid_ref[...] if lift else None
            for q in range(0, chunk, 4):
                columns = []
                state = []
                for h in (0, 2):
                    y = in_ref[pl.ds(base + q + h, 2)].reshape(2 * species, points)
                    if lift:
                        add = [
                            jnp.take_along_axis(
                                mid, jnp.full((species, points), base + q + h + k, i32), axis=1, mode="promise_in_bounds"
                            )
                            for k in (0, 1)
                        ]
                        y = y + relax_rate * jnp.concatenate(add, axis=0)
                    state.append(y)
                    top, rest = halves(jnp.tanh(y))
                    columns.append(jnp.concatenate([top, top, rest], axis=0))
                right = jnp.concatenate(columns, axis=1)
                change = dot(matrix, right)
                for h in (0, 1):
                    for k in (0, 1):
                        l = base + q + 2 * h + k
                        factor = jnp.where(counts_ref[l] > sub, f32(1.0), f32(0.0))
                        rows = slice(k * species, (k + 1) * species)
                        value = state[h][rows] + factor * change[rows, h * points : (h + 1) * points]
                        out_ref[l] = value
            return inner

        lax.fori_loop(0, lines // chunk, part, 0)

    def chemistry():
        substep(0, z_ref, y_ref, True)

        def two(pair, carry):
            substep(2 * pair + 1, y_ref, z_ref, False)
            substep(2 * pair + 2, z_ref, y_ref, False)
            return carry

        lax.fori_loop(0, SUBSTEPS // 2 - 1, two, 0)
        substep(SUBSTEPS - 1, y_ref, z_ref, False)

    segment = lane_s // SEG

    def pack(step, peer):
        tile = jnp.zeros((species, points), f32)
        for k in range(slots):
            q = peer * slots + k
            code = tab_smem[step * blocks + q // points, 0, lax.rem(q, points)]
            value = z_ref[code >> bits(segments)]
            value = pltpu.roll(value, (SEG * (k - (code & (segments - 1)))) & (points - 1), 1)
            tile = jnp.where(segment == k, value, tile)
        return tile

    def exchange(step):
        def begin(j, carry):
            peer, _ = place(j)
            send_ref[step, peer] = pack(step, peer)

            @pl.when(j > 1)
            def _():
                data_copy(step, j - 1).start()

            return carry

        lax.fori_loop(1, groups, begin, 0)
        recv_refs[step][me] = pack(step, me)
        data_copy(step, groups - 1).start()

    def arrivals():
        number = iota((total, 1), 0)
        lane_t = iota((total, points), 1)
        number_r = iota((1, total), 1)
        offset = lax.rem(me * slots, points)
        mine = offset + (iota((total, points), 0) & (slots - 1))
        for step in range(STEPS):
            for r in range(groups):
                flat_ref[r * slots : (r + 1) * slots, :] = jnp.broadcast_to(
                    got_ref[r, step : step + 1, :], (slots, points)
                )
            code = total_of(when(lane_t == mine, flat_ref[...]), 1)
            valid = code > 0
            code = code - 1
            line = jnp.where(valid, code >> bits(segments), lines)
            seg = code & (segments - 1)
            line_c = jnp.broadcast_to(line, (total, points))
            line_r = jnp.concatenate(
                [jnp.transpose(line_c[b * points : (b + 1) * points])[:1] for b in range(blocks)], axis=1
            )
            key_r = line_r * total + number_r
            key_c = line * total + number
            below = key_r < key_c
            position = total_of(when(below, 1), 1)
            same = total_of(when(below & (line_r == line), 1), 1)
            value = (number * segments + seg) * 2 + when(same == 0, 1)
            base = send_rows + step * (blocks + 1)
            for b in range(blocks):
                tab_ref[base + b] = total_of(when(position == lane_t + b * points, value), 0)
            upto = total_of(when(line_c <= lane_t, 1), 0)
            many = total_of(when(line_c == lane_t, 1), 0)
            tab_ref[base + blocks] = jnp.maximum(upto - 1, 0) * 2 + when(many > 0, 1)
            lands = jnp.where(line_r == iota((lines, total), 0), 1.0, 0.0).astype(bf16)
            covers = jnp.where(seg == (lane_t >> bits(SEG)), 1.0, 0.0).astype(bf16)
            weight_ref[step] = 1.0 - splice_weight * dot(lands, covers)
        rows = STEPS * (blocks + 1)
        copy = pltpu.make_async_copy(
            tab_ref.at[pl.ds(send_rows, rows)], tab_smem.at[pl.ds(send_rows, rows)], tab_sem.at[1]
        )
        copy.start()
        copy.wait()

    def collect(step):
        def finish(j, carry):
            data_copy(step, j).wait()
            return carry

        lax.fori_loop(1, groups, finish, 0)

    def land(step, out):
        base = send_rows + step * (blocks + 1)

        def run(n, acc):
            code = tab_smem[base + n // points, 0, lax.rem(n, points)]
            first = code & 1
            seg = (code >> 1) & (segments - 1)
            number = code >> bits(2 * segments)
            source = number >> bits(slots)
            k = number & (slots - 1)
            value = pltpu.roll(recv_refs[step][source], (SEG * (seg - k)) & (points - 1), 1)
            value = jnp.where(segment == seg, value, 0.0)
            acc = value + jnp.where(first == 1, f32(0.0), f32(1.0)) * acc
            sums_ref[n] = acc
            return acc

        lax.fori_loop(0, total, run, jnp.zeros((species, points), f32), unroll=8)

        def settle(l, sums):
            code = tab_smem[base + blocks, 0, l]
            factor = jnp.where((code & 1) == 1, f32(splice_weight), f32(0.0))
            value = z_ref[l] * weight_ref[step, pl.ds(l, 1), :] + factor * sums_ref[code >> 1]
            y_ref[l] = value
            return jnp.where(lane_s == l, jnp.sum(value, axis=1, keepdims=True), sums)

        sums = jnp.zeros((species, points), f32)
        for p in range(parts):
            sums = lax.fori_loop(p * lines // parts, (p + 1) * lines // parts, settle, sums, unroll=8)
            if out:
                out[p].start()
        return 0.5 * mid_ref[...] + (0.5 / points) * sums

    load.wait()
    diffuse(0)
    for copy in rim_copies(0):
        copy.wait()
    middle(0)
    send_table.wait()
    chemistry()
    exchange(0)

    def aim_finish(j, carry):
        aim_copy(j).wait()
        return carry

    lax.fori_loop(1, groups, aim_finish, 0)
    arrivals()
    collect(0)
    field_ref[1] = land(0, None)
    for copy in rim_copies(1):
        copy.start()
    diffuse(1)
    for copy in rim_copies(1):
        copy.wait()
    middle(1)
    chemistry()
    exchange(1)
    collect(1)
    out = [
        pltpu.make_async_copy(
            y_ref.at[pl.ds(p * lines // parts, lines // parts)],
            lines_out.at[pl.ds(p * lines // parts, lines // parts)],
            out_sem.at[p],
        )
        for p in range(parts)
    ]
    les_ref[...] = land(1, out).reshape(species, 1, lines)
    last = pltpu.make_async_copy(les_ref, les_out, out_sem.at[parts])
    last.start()
    for copy in out + [last]:
        copy.wait()


def body(
    les,
    lines,
    triplet_start,
    splice_owner,
    splice_line,
    splice_from,
    splice_to,
    chem_counts,
    diffusivity,
    rates,
    frozen_inverse,
):
    groups = lax.axis_size("grid") * lax.axis_size("line")
    _, _, count, species, points = lines.shape
    segments = points // SEG
    slots = min(segments, max(2, 2 * count // groups))
    total = groups * slots
    blocks = total // points
    rows = STEPS * (2 * blocks + 1)

    joint = jnp.dot(frozen_inverse, rates, precision=lax.Precision.HIGHEST)
    twice = jnp.kron(jnp.eye(2, dtype=f32), joint)
    top = lax.reduce_precision(twice, 8, 7)
    rest = lax.reduce_precision(twice - top, 8, 7)
    matrix = jnp.concatenate([top, rest, top], axis=1).astype(bf16)

    dma = pltpu.SemaphoreType.DMA
    field, state = pl.pallas_call(
        functools.partial(kernel, slots),
        out_shape=(
            jax.ShapeDtypeStruct((species, 1, count), f32),
            jax.ShapeDtypeStruct((count, species, points), f32),
        ),
        in_specs=[HBM] * 10,
        out_specs=(HBM, HBM),
        scratch_shapes=[
            pltpu.VMEM((species, 1, count), f32),
            *[pltpu.VMEM((STEPS, count), i32)] * 5,
            pltpu.VMEM(matrix.shape, bf16),
            pltpu.SMEM((species,), f32),
            pltpu.SMEM((count,), i32),
            pltpu.VMEM((count, species, points), f32),
            pltpu.VMEM((count, species, points), f32),
            pltpu.VMEM((species, points, points), bf16),
            pltpu.VMEM((species, points, points), bf16),
            pltpu.VMEM((STEPS, groups, species, points), f32),
            pltpu.VMEM((groups, species, points), f32),
            pltpu.VMEM((groups, species, points), f32),
            pltpu.VMEM((total, species, points), f32),
            pltpu.VMEM((STEPS, count, points), f32),
            pltpu.VMEM((STEPS, 4, species, count), f32),
            pltpu.VMEM((STEPS, species, count), f32),
            pltpu.VMEM((species, count), f32),
            pltpu.VMEM((blocks, STEPS, points), i32),
            pltpu.VMEM((groups, STEPS, points), i32),
            pltpu.VMEM((total, points), i32),
            pltpu.VMEM((rows, 1, points), i32),
            pltpu.SMEM((rows, 1, points), i32),
            dma((10,)),
            dma((2,)),
            dma((STEPS, 4)),
            dma((STEPS, 4)),
            dma((groups,)),
            dma((groups,)),
            dma((STEPS, groups)),
            dma((STEPS, groups)),
            dma((5,)),
        ],
        compiler_params=pltpu.CompilerParams(
            collective_id=0, has_side_effects=True, vmem_limit_bytes=67043328
        ),
        name="steps",
    )(
        les.reshape(species, 1, count),
        lines.reshape(count, species, points),
        triplet_start.reshape(STEPS, count),
        splice_owner.reshape(STEPS, count),
        splice_line.reshape(STEPS, count),
        splice_from.reshape(STEPS, count),
        splice_to.reshape(STEPS, count),
        matrix,
        diffusivity,
        chem_counts.reshape(count),
    )
    return (field.reshape(les.shape), state.reshape(lines.shape))


def solution(mesh):
    in_specs = (
        P(None, "grid", "line"),
        P("grid", "line", None, None, None),
        P(None, "grid", "line", None),
        P(None, "grid", "line", None, None),
        P(None, "grid", "line", None),
        P(None, "grid", "line", None),
        P(None, "grid", "line", None),
        P("grid", "line", None),
        P(),
        P(),
        P(),
    )
    out_specs = (P(None, "grid", "line"), P("grid", "line", None, None, None))
    return jax.shard_map(body, mesh=mesh, in_specs=in_specs, out_specs=out_specs, check_vma=False)
```

```python
import functools

import jax
import jax.numpy as jnp
from jax import lax
from jax.experimental import pallas as pl
from jax.experimental.pallas import tpu as pltpu
from jax.sharding import PartitionSpec as P

SEG = 16
TRIP = 48
STEPS = 2
SUBSTEPS = 6

les_rate = 0.2
relax_rate = 0.5
splice_weight = 0.5

NAMES = ("grid", "line")
MESH = pl.DeviceIdType.MESH
VMEM = pl.BlockSpec(memory_space=pltpu.VMEM)
SMEM = pl.BlockSpec(memory_space=pltpu.SMEM)
HBM = pl.BlockSpec(memory_space=pltpu.HBM)
f32 = jnp.float32
bf16 = jnp.bfloat16
i32 = jnp.int32

dot = functools.partial(jnp.dot, preferred_element_type=jnp.float32)


def halves(value):
    top = value.astype(bf16)
    return top, (value - top.astype(f32)).astype(bf16)


def column(row):
    points = row.shape[1]
    return jnp.transpose(jnp.broadcast_to(row, (points, points)))


def iota(shape, axis):
    return lax.broadcasted_iota(i32, shape, axis)


def bits(size):
    assert size & (size - 1) == 0
    return size.bit_length() - 1


def when(condition, value):
    return jnp.where(condition, value, 0)


def total_of(value, axis):
    return jnp.sum(value, axis=axis, keepdims=True, dtype=i32)


def kernel(
    slots,
    les_hbm,
    lines_hbm,
    start_hbm,
    owner_hbm,
    line_hbm,
    from_hbm,
    to_hbm,
    rates_hbm,
    frozen_hbm,
    coeff_hbm,
    counts_hbm,
    les_out,
    lines_out,
    les_ref,
    start_ref,
    owner_ref,
    line_ref,
    from_ref,
    to_ref,
    rates_ref,
    frozen_ref,
    coeff_ref,
    counts_ref,
    y_ref,
    z_ref,
    m_top,
    m_rest,
    send_ref,
    recv_0,
    recv_1,
    sums_ref,
    mask_ref,
    keep_ref,
    into_ref,
    fold_ref,
    weight_ref,
    rim_ref,
    field_ref,
    mid_ref,
    aim_ref,
    got_ref,
    flat_ref,
    tab_ref,
    tab_smem,
    load_sem,
    tab_sem,
    rim_send,
    rim_recv,
    aim_send,
    aim_recv,
    send_sem,
    recv_sem,
    out_sem,
):
    parts = out_sem.shape[0] - 1
    species, _, lines = les_ref.shape
    points = y_ref.shape[2]
    segments = points // SEG
    size = [lax.axis_size(n) for n in NAMES]
    at = [lax.axis_index(n) for n in NAMES]
    groups = size[0] * size[1]
    me = at[0] * size[1] + at[1]
    total = groups * slots
    blocks = total // points
    recv_refs = (recv_0, recv_1)

    def place(j):
        peer = (me + j) & (groups - 1)
        return peer, (peer >> bits(size[1]), peer & (size[1] - 1))

    barrier = pltpu.get_barrier_semaphore()

    def greet(j, carry):
        pl.semaphore_signal(barrier, inc=1, device_id=place(j)[1], device_id_type=MESH)
        return carry

    lax.fori_loop(1, groups, greet, 0)
    tables = [
        pltpu.make_async_copy(source, target, load_sem.at[n])
        for n, (source, target) in enumerate(
            [
                (coeff_hbm, coeff_ref),
                (owner_hbm, owner_ref),
                (from_hbm, from_ref),
                (line_hbm, line_ref),
                (to_hbm, to_ref),
                (les_hbm, les_ref),
                (start_hbm, start_ref),
                (counts_hbm, counts_ref),
                (rates_hbm, rates_ref),
                (frozen_hbm, frozen_ref),
            ]
        )
    ]
    load = pltpu.make_async_copy(lines_hbm, y_ref, load_sem.at[len(tables)])
    for copy in tables:
        copy.start()
    load.start()

    rims = []
    for axis in (0, 1):
        for move in (1, size[axis] - 1):
            there = list(at)
            there[axis] = lax.rem(at[axis] + move, size[axis])
            rims.append(tuple(there))

    def rim_copies(step):
        return [
            pltpu.make_async_remote_copy(
                src_ref=field_ref.at[step],
                dst_ref=rim_ref.at[step, k],
                send_sem=rim_send.at[step, k],
                recv_sem=rim_recv.at[step, k],
                device_id=rims[k],
                device_id_type=MESH,
            )
            for k in range(4)
        ]

    def aim_copy(j):
        peer, device = place(j)
        return pltpu.make_async_remote_copy(
            src_ref=aim_ref.at[(peer * slots) >> bits(points)],
            dst_ref=got_ref.at[me],
            send_sem=aim_send.at[j],
            recv_sem=aim_recv.at[j],
            device_id=device,
            device_id_type=MESH,
        )

    def data_copy(step, j):
        peer, device = place(j)
        return pltpu.make_async_remote_copy(
            src_ref=send_ref.at[step, peer],
            dst_ref=recv_refs[step].at[me],
            send_sem=send_sem.at[step, j],
            recv_sem=recv_sem.at[step, j],
            device_id=device,
            device_id_type=MESH,
        )

    for copy in tables:
        copy.wait()
    field_ref[0] = les_ref[...].reshape(species, lines)

    lane = iota((points, points), 1)
    row = iota((points, points), 0)
    for step in range(STEPS):
        owner = owner_ref[step : step + 1, :]
        rank = total_of(when((column(owner) == owner) & (row < lane), 1), 0)
        spot = column(owner * slots + rank)
        turn = (SEG * (rank - from_ref[step : step + 1, :])) & (points - 1)
        code = column(iota((1, points), 1) * points + turn)
        aim = column(line_ref[step : step + 1, :] * segments + to_ref[step : step + 1, :] + 1)
        for b in range(blocks):
            hit = spot == lane + b * points
            tab_ref[step * blocks + b] = total_of(when(hit, code), 0)
            aim_ref[b, step : step + 1, :] = total_of(when(hit, aim), 0)
    send_rows = STEPS * blocks
    send_table = pltpu.make_async_copy(tab_ref.at[pl.ds(0, send_rows)], tab_smem.at[pl.ds(0, send_rows)], tab_sem.at[0])
    send_table.start()

    apart = jnp.abs(lane - row).astype(f32)
    both = (lane + row).astype(f32)

    def inverse(s, carry):
        coeff = jnp.full((8, points), coeff_ref[s], f32)
        root = jnp.sqrt(4.0 * coeff + 1.0)
        theta = -jnp.log(2.0 * coeff / (2.0 * coeff + 1.0 + root))
        scale = 1.0 / (root * (1.0 - jnp.exp(-2.0 * points * theta)))
        theta = theta[:1]
        value = jnp.exp(-apart * theta) + jnp.exp((apart - 2.0 * points) * theta)
        value = value + jnp.exp(-(both + 1.0) * theta) + jnp.exp((both + 1.0 - 2.0 * points) * theta)
        top, rest = halves(value * scale[:1] - relax_rate / points)
        m_top[s] = top
        m_rest[s] = rest
        return carry

    lax.fori_loop(0, species, inverse, 0)

    pl.semaphore_wait(barrier, groups - 1)
    for copy in rim_copies(0):
        copy.start()

    def aim_start(j, carry):
        aim_copy(j).start()
        return carry

    lax.fori_loop(1, groups, aim_start, 0)
    got_ref[me] = aim_ref[(me * slots) >> bits(points)]

    flat_y = y_ref.reshape(lines * species, points)
    flat_z = z_ref.reshape(lines * species, points)

    def diffuse(step):
        rel = lane - column(start_ref[step : step + 1, :])
        third = TRIP // 3
        source = jnp.where(
            rel < third,
            3 * rel,
            jnp.where(rel < 2 * third, 3 * (2 * third - 1 - rel) + 1, 3 * (rel - 2 * third) + 2),
        )
        index = jnp.where((rel >= 0) & (rel < TRIP), source + (lane - rel), lane)

        def one(s, carry):
            y = flat_y[pl.ds(s, lines, stride=species), :]
            y = jnp.take_along_axis(y, index, axis=1, mode="promise_in_bounds")
            top, rest = halves(y)
            out = dot(top, m_top[s]) + dot(rest, m_top[s]) + dot(top, m_rest[s])
            flat_z[pl.ds(s, lines, stride=species), :] = out
            return carry

        lax.fori_loop(0, species, one, 0, unroll=12)

    lane_s = lax.broadcasted_iota(i32, (species, points), 1)

    def middle(step):
        field = field_ref[step]
        up = jnp.where(at[0] > 0, rim_ref[step, 0], 0.0)
        down = jnp.where(at[0] < size[0] - 1, rim_ref[step, 1], 0.0)
        left = jnp.where(at[1] > 0, rim_ref[step, 2], 0.0)
        right = jnp.where(at[1] < size[1] - 1, rim_ref[step, 3], 0.0)
        before = pltpu.roll(jnp.where(lane_s == points - 1, left, field), 1, 1)
        after = pltpu.roll(jnp.where(lane_s == 0, right, field), points - 1, 1)
        mid_ref[...] = field + les_rate * (up + down + before + after - 4.0 * field)

    joint = jnp.dot(
        frozen_ref[...], rates_ref[...], precision=lax.Precision.HIGHEST, preferred_element_type=f32
    )
    joint_top, joint_rest = halves(joint)
    wide = (2 * species, 6 * species)
    place_c = iota(wide, 1)
    block_c = sum((place_c >= species * n).astype(i32) for n in range(1, 6))
    pick = jnp.where(
        iota((species, 6 * species), 0) == (place_c - species * block_c)[:species], 1.0, 0.0
    ).astype(bf16)
    twice_top = dot(jnp.concatenate([joint_top.astype(f32)] * 2, axis=0).astype(bf16), pick)
    twice_rest = dot(jnp.concatenate([joint_rest.astype(f32)] * 2, axis=0).astype(bf16), pick)
    entries = jnp.where((block_c >> 1) == 1, twice_rest, twice_top)
    matrix = jnp.where((iota(wide, 0) >= species).astype(i32) == (block_c & 1), entries, 0.0).astype(bf16)

    def substep(sub, in_ref, out_ref, lift):
        mid = relax_rate * mid_ref[...] if lift else None
        for q in range(0, lines, 4):
            columns = []
            state = []
            for h in (0, 2):
                y = in_ref[pl.ds(q + h, 2)].reshape(2 * species, points)
                if lift:
                    add = [
                        jnp.broadcast_to(mid[:, l : l + 1], (species, points)) for l in (q + h, q + h + 1)
                    ]
                    y = y + jnp.concatenate(add, axis=0)
                state.append(y)
                top, rest = halves(jnp.tanh(y))
                columns.append(jnp.concatenate([top, top, rest], axis=0))
            right = jnp.concatenate(columns, axis=1)
            change = dot(matrix, right)
            for h in (0, 1):
                for k in (0, 1):
                    l = q + 2 * h + k
                    factor = jnp.where(counts_ref[l] > sub, f32(1.0), f32(0.0))
                    rows = slice(k * species, (k + 1) * species)
                    out_ref[l] = state[h][rows] + factor * change[rows, h * points : (h + 1) * points]

    def chemistry():
        substep(0, z_ref, y_ref, True)

        def two(pair, carry):
            substep(2 * pair + 1, y_ref, z_ref, False)
            substep(2 * pair + 2, z_ref, y_ref, False)
            return carry

        lax.fori_loop(0, SUBSTEPS // 2 - 1, two, 0)
        substep(SUBSTEPS - 1, y_ref, z_ref, False)

    segment = lane_s // SEG

    def pack(step, peer):
        tile = jnp.zeros((species, points), f32)
        first = peer * slots
        for k in range(slots):
            code = tab_smem[step * blocks + (first >> bits(points)), 0, (first & (points - 1)) + k]
            value = pltpu.roll(z_ref[code >> bits(points)], code & (points - 1), 1)
            tile = jnp.where(segment == k, value, tile)
        return tile

    def exchange(step):
        def begin(j, carry):
            peer, _ = place(j)
            send_ref[step, peer] = pack(step, peer)

            @pl.when(j > 1)
            def _():
                data_copy(step, j - 1).start()

            return carry

        lax.fori_loop(1, groups, begin, 0)
        recv_refs[step][me] = pack(step, me)
        data_copy(step, groups - 1).start()

    def arrivals():
        number = iota((total, 1), 0)
        lane_t = iota((total, points), 1)
        number_r = iota((1, total), 1)
        offset = (me * slots) & (points - 1)
        mine = offset + (iota((total, points), 0) & (slots - 1))
        for step in range(STEPS):
            for r in range(groups):
                flat_ref[r * slots : (r + 1) * slots, :] = jnp.broadcast_to(
                    got_ref[r, step : step + 1, :], (slots, points)
                )
            code = total_of(when(lane_t == mine, flat_ref[...]), 1)
            valid = code > 0
            code = code - 1
            line = jnp.where(valid, code >> bits(segments), lines)
            seg = code & (segments - 1)
            line_c = jnp.broadcast_to(line, (total, points))
            line_r = jnp.concatenate(
                [jnp.transpose(line_c[b * points : (b + 1) * points])[:1] for b in range(blocks)], axis=1
            )
            key_r = line_r * total + number_r
            key_c = line * total + number
            below = key_r < key_c
            position = total_of(when(below, 1), 1)
            same = total_of(when(below & (line_r == line), 1), 1)
            turn = (SEG * (seg - (number & (slots - 1)))) & (points - 1)
            value = (number >> bits(slots)) * points + turn
            kind = seg * 2 + when(same == 0, 1)
            base = send_rows + step * (blocks + 1)
            for b in range(blocks):
                hit = position == lane_t + b * points
                tab_ref[base + b] = total_of(when(hit, value), 0)
                kinds = column(total_of(when(hit, kind), 0))
                at_b = pl.ds(b * points, points)
                mask_ref[step, at_b, :] = jnp.where((kinds >> 1) == (lane >> bits(SEG)), splice_weight, 0.0)
                keep_ref[step, at_b, :] = jnp.where((kinds & 1) == 1, 0.0, 1.0)
            upto = total_of(when(line_c <= lane_t, 1), 0)
            many = total_of(when(line_c == lane_t, 1), 0)
            tab_ref[base + blocks] = jnp.where(many > 0, upto - 1, total)
            lands = jnp.where(line_r == iota((lines, total), 0), 1.0, 0.0).astype(bf16)
            covers = jnp.where(seg == (lane_t >> bits(SEG)), 1.0, 0.0).astype(bf16)
            weight_ref[step] = 1.0 - splice_weight * dot(lands, covers)
            into_ref[step] = jnp.where(line_c == lane_t, splice_weight, 0.0)
        rows = STEPS * (blocks + 1)
        copy = pltpu.make_async_copy(
            tab_ref.at[pl.ds(send_rows, rows)], tab_smem.at[pl.ds(send_rows, rows)], tab_sem.at[1]
        )
        copy.start()
        copy.wait()

    def collect(step):
        def finish(j, carry):
            data_copy(step, j).wait()
            return carry

        lax.fori_loop(1, groups, finish, 0)

    def prepare(step):
        def rows(j, carry):
            block = jnp.broadcast_to(into_ref[step, pl.ds(j, 1), :], (SEG, lines))
            fold_ref[pl.ds(pl.multiple_of(j * SEG, SEG), SEG), :] = block.astype(bf16)
            return carry

        lax.fori_loop(0, total, rows, 0, unroll=8)

        def scale(l, sums):
            value = z_ref[l] * weight_ref[step, pl.ds(l, 1), :]
            z_ref[l] = value
            return jnp.where(lane_s == l, jnp.sum(value, axis=1, keepdims=True), sums)

        return lax.fori_loop(0, lines, scale, jnp.zeros((species, points), f32), unroll=8)

    def filtered(step, sums):
        depth = slots * SEG

        def add(r, acc):
            top, rest = halves(recv_refs[step][r][:, :depth])
            right = fold_ref[pl.ds(pl.multiple_of(r * depth, depth), depth), :]
            return acc + dot(jnp.concatenate([top.astype(f32), rest.astype(f32)], axis=0).astype(bf16), right)

        acc = lax.fori_loop(0, groups, add, jnp.zeros((2 * species, points), f32), unroll=8)
        return 0.5 * mid_ref[...] + (0.5 / points) * (sums + (acc[:species] + acc[species:]))

    def land(step, out):
        base = send_rows + step * (blocks + 1)
        sums_ref[total] = jnp.zeros((species, points), f32)
        acc = jnp.zeros((species, points), f32)
        for b in range(blocks):

            def run(i, acc):
                code = tab_smem[base + b, 0, i]
                value = pltpu.roll(recv_refs[step][code >> bits(points)], code & (points - 1), 1)
                n = b * points + i
                acc = value * mask_ref[step, pl.ds(n, 1), :] + acc * keep_ref[step, pl.ds(n, 1), :]
                sums_ref[n] = acc
                return acc

            acc = lax.fori_loop(0, points, run, acc, unroll=16)

        def settle(l, carry):
            y_ref[l] = z_ref[l] + sums_ref[tab_smem[base + blocks, 0, l]]
            return carry

        for p in range(parts):
            lax.fori_loop(p * lines // parts, (p + 1) * lines // parts, settle, 0, unroll=16)
            if out:
                out[p].start()

    load.wait()
    diffuse(0)
    for copy in rim_copies(0):
        copy.wait()
    middle(0)
    send_table.wait()
    chemistry()
    exchange(0)

    def aim_finish(j, carry):
        aim_copy(j).wait()
        return carry

    lax.fori_loop(1, groups, aim_finish, 0)
    arrivals()
    sums = prepare(0)
    collect(0)
    field_ref[1] = filtered(0, sums)
    for copy in rim_copies(1):
        copy.start()
    land(0, None)
    diffuse(1)
    for copy in rim_copies(1):
        copy.wait()
    middle(1)
    chemistry()
    exchange(1)
    sums = prepare(1)
    collect(1)
    les_ref[...] = filtered(1, sums).reshape(species, 1, lines)
    last = pltpu.make_async_copy(les_ref, les_out, out_sem.at[parts])
    last.start()
    out = [
        pltpu.make_async_copy(
            y_ref.at[pl.ds(p * lines // parts, lines // parts)],
            lines_out.at[pl.ds(p * lines // parts, lines // parts)],
            out_sem.at[p],
        )
        for p in range(parts)
    ]
    land(1, out)
    for copy in out + [last]:
        copy.wait()


def deliver_kernel(les_in, lines_in, les_out, lines_out, les_ref, lines_ref, in_sem, out_sem):
    parts = in_sem.shape[0] - 1
    size = lines_ref.shape[0] // parts
    pairs = [(les_in, les_ref, les_out)]
    for p in range(parts):
        at = pl.ds(p * size, size)
        pairs.append((lines_in.at[at], lines_ref.at[at], lines_out.at[at]))
    takes = [pltpu.make_async_copy(a, b, in_sem.at[n]) for n, (a, b, c) in enumerate(pairs)]
    gives = [pltpu.make_async_copy(b, c, out_sem.at[n]) for n, (a, b, c) in enumerate(pairs)]
    for take in takes:
        take.start()
    for take, give in zip(takes, gives):
        take.wait()
        give.start()
    for give in gives:
        give.wait()


def body(
    les,
    lines,
    triplet_start,
    splice_owner,
    splice_line,
    splice_from,
    splice_to,
    chem_counts,
    diffusivity,
    rates,
    frozen_inverse,
):
    groups = lax.axis_size("grid") * lax.axis_size("line")
    _, _, count, species, points = lines.shape
    segments = points // SEG
    slots = min(segments, max(2, 2 * count // groups))
    total = groups * slots
    blocks = total // points
    rows = STEPS * (2 * blocks + 1)

    dma = pltpu.SemaphoreType.DMA
    field, state = pl.pallas_call(
        functools.partial(kernel, slots),
        out_shape=(
            jax.ShapeDtypeStruct((species, 1, count), f32),
            jax.ShapeDtypeStruct((count, species, points), f32),
        ),
        in_specs=[HBM] * 11,
        out_specs=(HBM, HBM),
        scratch_shapes=[
            pltpu.VMEM((species, 1, count), f32),
            *[pltpu.VMEM((STEPS, count), i32)] * 5,
            pltpu.VMEM((species, species), f32),
            pltpu.VMEM((species, species), f32),
            pltpu.SMEM((species,), f32),
            pltpu.SMEM((count,), i32),
            pltpu.VMEM((count, species, points), f32),
            pltpu.VMEM((count, species, points), f32),
            pltpu.VMEM((species, points, points), bf16),
            pltpu.VMEM((species, points, points), bf16),
            pltpu.VMEM((STEPS, groups, species, points), f32),
            pltpu.VMEM((groups, species, points), f32),
            pltpu.VMEM((groups, species, points), f32),
            pltpu.VMEM((total + 1, species, points), f32),
            pltpu.VMEM((STEPS, total, points), f32),
            pltpu.VMEM((STEPS, total, points), f32),
            pltpu.VMEM((STEPS, total, count), f32),
            pltpu.VMEM((total * SEG, count), bf16),
            pltpu.VMEM((STEPS, count, points), f32),
            pltpu.VMEM((STEPS, 4, species, count), f32),
            pltpu.VMEM((STEPS, species, count), f32),
            pltpu.VMEM((species, count), f32),
            pltpu.VMEM((blocks, STEPS, points), i32),
            pltpu.VMEM((groups, STEPS, points), i32),
            pltpu.VMEM((total, points), i32),
            pltpu.VMEM((rows, 1, points), i32),
            pltpu.SMEM((rows, 1, points), i32),
            dma((11,)),
            dma((2,)),
            dma((STEPS, 4)),
            dma((STEPS, 4)),
            dma((groups,)),
            dma((groups,)),
            dma((STEPS, groups)),
            dma((STEPS, groups)),
            dma((5,)),
        ],
        compiler_params=pltpu.CompilerParams(
            collective_id=0, has_side_effects=True, vmem_limit_bytes=67043328
        ),
        name="steps",
    )(
        les.reshape(species, 1, count),
        lines.reshape(count, species, points),
        triplet_start.reshape(STEPS, count),
        splice_owner.reshape(STEPS, count),
        splice_line.reshape(STEPS, count),
        splice_from.reshape(STEPS, count),
        splice_to.reshape(STEPS, count),
        rates,
        frozen_inverse,
        diffusivity,
        chem_counts.reshape(count),
    )
    field, state = pl.pallas_call(
        deliver_kernel,
        out_shape=(jax.ShapeDtypeStruct(field.shape, f32), jax.ShapeDtypeStruct(state.shape, f32)),
        in_specs=[HBM] * 2,
        out_specs=(HBM, HBM),
        scratch_shapes=[
            pltpu.VMEM(field.shape, f32),
            pltpu.VMEM(state.shape, f32),
            dma((9,)),
            dma((9,)),
        ],
        compiler_params=pltpu.CompilerParams(vmem_limit_bytes=67043328),
        name="deliver",
    )(field, state)
    return (field.reshape(les.shape), state.reshape(lines.shape))


def solution(mesh):
    in_specs = (
        P(None, "grid", "line"),
        P("grid", "line", None, None, None),
        P(None, "grid", "line", None),
        P(None, "grid", "line", None, None),
        P(None, "grid", "line", None),
        P(None, "grid", "line", None),
        P(None, "grid", "line", None),
        P("grid", "line", None),
        P(),
        P(),
        P(),
    )
    out_specs = (P(None, "grid", "line"), P("grid", "line", None, None, None))
    return jax.shard_map(body, mesh=mesh, in_specs=in_specs, out_specs=out_specs, check_vma=False)
```

```python
import functools

import jax
import jax.numpy as jnp
from jax import lax
from jax.experimental import pallas as pl
from jax.experimental.pallas import tpu as pltpu
from jax.sharding import PartitionSpec as P

SEG = 16
TRIP = 48
STEPS = 2
SUBSTEPS = 6

les_rate = 0.2
relax_rate = 0.5
splice_weight = 0.5

NAMES = ("grid", "line")
MESH = pl.DeviceIdType.MESH
VMEM = pl.BlockSpec(memory_space=pltpu.VMEM)
SMEM = pl.BlockSpec(memory_space=pltpu.SMEM)
HBM = pl.BlockSpec(memory_space=pltpu.HBM)
f32 = jnp.float32
bf16 = jnp.bfloat16
i32 = jnp.int32

dot = functools.partial(jnp.dot, preferred_element_type=jnp.float32)


def halves(value):
    top = value.astype(bf16)
    return top, (value - top.astype(f32)).astype(bf16)


def column(row):
    points = row.shape[1]
    return jnp.transpose(jnp.broadcast_to(row, (points, points)))


def iota(shape, axis):
    return lax.broadcasted_iota(i32, shape, axis)


def bits(size):
    assert size & (size - 1) == 0
    return size.bit_length() - 1


def when(condition, value):
    return jnp.where(condition, value, 0)


def total_of(value, axis):
    return jnp.sum(value, axis=axis, keepdims=True, dtype=i32)


def kernel(
    slots,
    les_hbm,
    lines_hbm,
    start_hbm,
    owner_hbm,
    line_hbm,
    from_hbm,
    to_hbm,
    rates_hbm,
    frozen_hbm,
    coeff_hbm,
    counts_hbm,
    les_out,
    lines_out,
    les_ref,
    start_ref,
    owner_ref,
    line_ref,
    from_ref,
    to_ref,
    rates_ref,
    frozen_ref,
    coeff_ref,
    counts_ref,
    coeffs_ref,
    apart_ref,
    ends_ref,
    y_ref,
    z_ref,
    m_top,
    m_rest,
    send_ref,
    recv_0,
    recv_1,
    sums_ref,
    mask_ref,
    keep_ref,
    into_ref,
    fold_ref,
    both_ref,
    weight_ref,
    rim_ref,
    field_ref,
    mid_ref,
    aim_ref,
    got_ref,
    flat_ref,
    tab_ref,
    tab_smem,
    load_sem,
    tab_sem,
    rim_send,
    rim_recv,
    aim_send,
    aim_recv,
    send_sem,
    recv_sem,
    out_sem,
):
    parts = out_sem.shape[0] - 1
    species, _, lines = les_ref.shape
    points = y_ref.shape[2]
    segments = points // SEG
    size = [lax.axis_size(n) for n in NAMES]
    at = [lax.axis_index(n) for n in NAMES]
    groups = size[0] * size[1]
    me = at[0] * size[1] + at[1]
    total = groups * slots
    blocks = total // points
    recv_refs = (recv_0, recv_1)

    def place(j):
        peer = (me + j) & (groups - 1)
        return peer, (peer >> bits(size[1]), peer & (size[1] - 1))

    barrier = pltpu.get_barrier_semaphore()

    def greet(j, carry):
        pl.semaphore_signal(barrier, inc=1, device_id=place(j)[1], device_id_type=MESH)
        return carry

    lax.fori_loop(1, groups, greet, 0)
    tables = [
        pltpu.make_async_copy(source, target, load_sem.at[n])
        for n, (source, target) in enumerate(
            [
                (coeff_hbm, coeff_ref),
                (owner_hbm, owner_ref),
                (from_hbm, from_ref),
                (line_hbm, line_ref),
                (to_hbm, to_ref),
                (les_hbm, les_ref),
                (start_hbm, start_ref),
                (counts_hbm, counts_ref),
                (rates_hbm, rates_ref),
                (frozen_hbm, frozen_ref),
            ]
        )
    ]
    load = pltpu.make_async_copy(lines_hbm, y_ref, load_sem.at[len(tables)])
    for copy in tables:
        copy.start()
    load.start()

    rims = []
    for axis in (0, 1):
        for move in (1, size[axis] - 1):
            there = list(at)
            there[axis] = lax.rem(at[axis] + move, size[axis])
            rims.append(tuple(there))

    def rim_copies(step):
        return [
            pltpu.make_async_remote_copy(
                src_ref=field_ref.at[step],
                dst_ref=rim_ref.at[step, k],
                send_sem=rim_send.at[step, k],
                recv_sem=rim_recv.at[step, k],
                device_id=rims[k],
                device_id_type=MESH,
            )
            for k in range(4)
        ]

    def aim_copy(j):
        peer, device = place(j)
        return pltpu.make_async_remote_copy(
            src_ref=aim_ref.at[(peer * slots) >> bits(points)],
            dst_ref=got_ref.at[me],
            send_sem=aim_send.at[j],
            recv_sem=aim_recv.at[j],
            device_id=device,
            device_id_type=MESH,
        )

    def data_copy(step, j):
        peer, device = place(j)
        return pltpu.make_async_remote_copy(
            src_ref=send_ref.at[step, peer],
            dst_ref=recv_refs[step].at[me],
            send_sem=send_sem.at[step, j],
            recv_sem=recv_sem.at[step, j],
            device_id=device,
            device_id_type=MESH,
        )

    tables[0].wait()
    lane = iota((points, points), 1)
    row = iota((points, points), 0)
    for n in range(species):
        coeffs_ref[n : n + 1, :] = jnp.full((1, points), coeff_ref[n], f32)
    coeff = coeffs_ref[...]
    root = jnp.sqrt(4.0 * coeff + 1.0)
    theta = -jnp.log(2.0 * coeff / (2.0 * coeff + 1.0 + root))
    scale = 1.0 / (root * (1.0 - jnp.exp(-2.0 * points * theta)))
    along = iota((species, points), 1).astype(f32)
    apart_ref[...] = scale * (jnp.exp(-along * theta) + jnp.exp((along - 2.0 * points) * theta)) - relax_rate / points
    ends_ref[...] = scale * (jnp.exp(-(along + 1.0) * theta) + jnp.exp((along + 1.0 - 2.0 * points) * theta))
    apart = jnp.abs(lane - row)
    ends = jnp.minimum(lane + row, 2 * points - 2 - lane - row)

    def spread(ref, n, index):
        value = jnp.broadcast_to(ref[pl.ds(n, 1), :], (points, points))
        return jnp.take_along_axis(value, index, axis=1, mode="promise_in_bounds")

    def inverse(n, carry):
        top, rest = halves(spread(apart_ref, n, apart) + spread(ends_ref, n, ends))
        m_top[n] = top
        m_rest[n] = rest
        return carry

    lax.fori_loop(0, species, inverse, 0, unroll=4)
    for copy in tables[1:]:
        copy.wait()
    field_ref[0] = les_ref[...].reshape(species, lines)


    for step in range(STEPS):
        owner = owner_ref[step : step + 1, :]
        rank = total_of(when((column(owner) == owner) & (row < lane), 1), 0)
        spot = column(owner * slots + rank)
        turn = (SEG * (rank - from_ref[step : step + 1, :])) & (points - 1)
        code = column(iota((1, points), 1) * points + turn)
        aim = column(line_ref[step : step + 1, :] * segments + to_ref[step : step + 1, :] + 1)
        for b in range(blocks):
            hit = spot == lane + b * points
            tab_ref[step * blocks + b] = total_of(when(hit, code), 0)
            aim_ref[b, step : step + 1, :] = total_of(when(hit, aim), 0)
    send_rows = STEPS * blocks
    send_table = pltpu.make_async_copy(tab_ref.at[pl.ds(0, send_rows)], tab_smem.at[pl.ds(0, send_rows)], tab_sem.at[0])
    send_table.start()

    pl.semaphore_wait(barrier, groups - 1)
    for copy in rim_copies(0):
        copy.start()

    def aim_start(j, carry):
        aim_copy(j).start()
        return carry

    lax.fori_loop(1, groups, aim_start, 0)
    got_ref[me] = aim_ref[(me * slots) >> bits(points)]

    flat_y = y_ref.reshape(lines * species, points)
    flat_z = z_ref.reshape(lines * species, points)

    def diffuse(step):
        rel = lane - column(start_ref[step : step + 1, :])
        third = TRIP // 3
        source = jnp.where(
            rel < third,
            3 * rel,
            jnp.where(rel < 2 * third, 3 * (2 * third - 1 - rel) + 1, 3 * (rel - 2 * third) + 2),
        )
        index = jnp.where((rel >= 0) & (rel < TRIP), source + (lane - rel), lane)

        def one(s, carry):
            y = flat_y[pl.ds(s, lines, stride=species), :]
            y = jnp.take_along_axis(y, index, axis=1, mode="promise_in_bounds")
            top, rest = halves(y)
            out = dot(top, m_top[s]) + dot(rest, m_top[s]) + dot(top, m_rest[s])
            flat_z[pl.ds(s, lines, stride=species), :] = out
            return carry

        lax.fori_loop(0, species, one, 0, unroll=12)

    lane_s = lax.broadcasted_iota(i32, (species, points), 1)

    def middle(step):
        field = field_ref[step]
        up = jnp.where(at[0] > 0, rim_ref[step, 0], 0.0)
        down = jnp.where(at[0] < size[0] - 1, rim_ref[step, 1], 0.0)
        left = jnp.where(at[1] > 0, rim_ref[step, 2], 0.0)
        right = jnp.where(at[1] < size[1] - 1, rim_ref[step, 3], 0.0)
        before = pltpu.roll(jnp.where(lane_s == points - 1, left, field), 1, 1)
        after = pltpu.roll(jnp.where(lane_s == 0, right, field), points - 1, 1)
        mid_ref[...] = field + les_rate * (up + down + before + after - 4.0 * field)

    joint = jnp.dot(
        frozen_ref[...], rates_ref[...], precision=lax.Precision.HIGHEST, preferred_element_type=f32
    )
    joint_top, joint_rest = halves(joint)
    wide = (2 * species, 6 * species)
    place_c = iota(wide, 1)
    block_c = sum((place_c >= species * n).astype(i32) for n in range(1, 6))
    pick = jnp.where(
        iota((species, 6 * species), 0) == (place_c - species * block_c)[:species], 1.0, 0.0
    ).astype(bf16)
    twice_top = dot(jnp.concatenate([joint_top.astype(f32)] * 2, axis=0).astype(bf16), pick)
    twice_rest = dot(jnp.concatenate([joint_rest.astype(f32)] * 2, axis=0).astype(bf16), pick)
    entries = jnp.where((block_c >> 1) == 1, twice_rest, twice_top)
    matrix = jnp.where((iota(wide, 0) >= species).astype(i32) == (block_c & 1), entries, 0.0).astype(bf16)

    def substep(sub, in_ref, out_ref, lift):
        mid = relax_rate * mid_ref[...] if lift else None
        for q in range(0, lines, 4):
            columns = []
            state = []
            for h in (0, 2):
                y = in_ref[pl.ds(q + h, 2)].reshape(2 * species, points)
                if lift:
                    add = [
                        jnp.broadcast_to(mid[:, l : l + 1], (species, points)) for l in (q + h, q + h + 1)
                    ]
                    y = y + jnp.concatenate(add, axis=0)
                state.append(y)
                top, rest = halves(jnp.tanh(y))
                columns.append(jnp.concatenate([top, top, rest], axis=0))
            right = jnp.concatenate(columns, axis=1)
            change = dot(matrix, right)
            for h in (0, 1):
                for k in (0, 1):
                    l = q + 2 * h + k
                    factor = jnp.where(counts_ref[l] > sub, f32(1.0), f32(0.0))
                    rows = slice(k * species, (k + 1) * species)
                    out_ref[l] = state[h][rows] + factor * change[rows, h * points : (h + 1) * points]

    def chemistry():
        substep(0, z_ref, y_ref, True)

        def two(pair, carry):
            substep(2 * pair + 1, y_ref, z_ref, False)
            substep(2 * pair + 2, z_ref, y_ref, False)
            return carry

        lax.fori_loop(0, SUBSTEPS // 2 - 1, two, 0)
        substep(SUBSTEPS - 1, y_ref, z_ref, False)

    segment = lane_s // SEG

    def pack(step, peer):
        tile = jnp.zeros((species, points), f32)
        first = peer * slots
        for k in range(slots):
            code = tab_smem[step * blocks + (first >> bits(points)), 0, (first & (points - 1)) + k]
            value = pltpu.roll(z_ref[code >> bits(points)], code & (points - 1), 1)
            tile = jnp.where(segment == k, value, tile)
        return tile

    def exchange(step):
        def begin(i, carry):
            for n in range(pair):
                peer, _ = place(pair * i + n)
                send_ref[step, peer] = pack(step, peer)
            for n in range(pair):
                before = pair * (i - 1) + n

                @pl.when(before > 0)
                def _():
                    data_copy(step, before).start()

            return carry

        pair = 2
        lax.fori_loop(0, groups // pair, begin, 0)
        recv_refs[step][me] = send_ref[step, me]
        for n in range(groups - pair, groups):
            data_copy(step, n).start()

    def arrivals():
        number = iota((total, 1), 0)
        lane_t = iota((total, points), 1)
        number_r = iota((1, total), 1)
        offset = (me * slots) & (points - 1)
        mine = offset + (iota((total, points), 0) & (slots - 1))
        for step in range(STEPS):
            for r in range(groups):
                flat_ref[r * slots : (r + 1) * slots, :] = jnp.broadcast_to(
                    got_ref[r, step : step + 1, :], (slots, points)
                )
            code = total_of(when(lane_t == mine, flat_ref[...]), 1)
            valid = code > 0
            code = code - 1
            line = jnp.where(valid, code >> bits(segments), lines)
            seg = code & (segments - 1)
            line_c = jnp.broadcast_to(line, (total, points))
            line_r = jnp.concatenate(
                [jnp.transpose(line_c[b * points : (b + 1) * points])[:1] for b in range(blocks)], axis=1
            )
            key_r = line_r * total + number_r
            key_c = line * total + number
            below = key_r < key_c
            position = total_of(when(below, 1), 1)
            same = total_of(when(below & (line_r == line), 1), 1)
            turn = (SEG * (seg - (number & (slots - 1)))) & (points - 1)
            value = (number >> bits(slots)) * points + turn
            kind = seg * 2 + when(same == 0, 1)
            base = send_rows + step * (blocks + 1)
            for b in range(blocks):
                hit = position == lane_t + b * points
                tab_ref[base + b] = total_of(when(hit, value), 0)
                kinds = column(total_of(when(hit, kind), 0))
                at_b = pl.ds(b * points, points)
                mask_ref[step, at_b, :] = jnp.where((kinds >> 1) == (lane >> bits(SEG)), splice_weight, 0.0)
                keep_ref[step, at_b, :] = jnp.where((kinds & 1) == 1, 0.0, 1.0)
            upto = total_of(when(line_c <= lane_t, 1), 0)
            many = total_of(when(line_c == lane_t, 1), 0)
            tab_ref[base + blocks] = jnp.where(many > 0, upto - 1, total)
            lands = jnp.where(line_r == iota((lines, total), 0), 1.0, 0.0).astype(bf16)
            covers = jnp.where(seg == (lane_t >> bits(SEG)), 1.0, 0.0).astype(bf16)
            weight_ref[step] = 1.0 - splice_weight * dot(lands, covers)
            into_ref[step] = jnp.where(line_c == lane_t, splice_weight, 0.0)
        rows = STEPS * (blocks + 1)
        copy = pltpu.make_async_copy(
            tab_ref.at[pl.ds(send_rows, rows)], tab_smem.at[pl.ds(send_rows, rows)], tab_sem.at[1]
        )
        copy.start()
        copy.wait()

    def collect(step):
        def finish(j, carry):
            data_copy(step, j).wait()
            return carry

        lax.fori_loop(1, groups, finish, 0)

    def prepare(step):
        def rows(j, carry):
            block = jnp.broadcast_to(into_ref[step, pl.ds(j, 1), :], (SEG, lines))
            first = (j >> bits(slots)) * points + (j & (slots - 1)) * SEG
            fold_ref[pl.ds(pl.multiple_of(first, SEG), SEG), :] = block.astype(bf16)
            return carry

        if slots < segments:
            fold_ref[...] = jnp.zeros_like(fold_ref)
        lax.fori_loop(0, total, rows, 0, unroll=8)

        def scale(l, sums):
            value = z_ref[l] * weight_ref[step, pl.ds(l, 1), :]
            z_ref[l] = value
            return jnp.where(lane_s == l, jnp.sum(value, axis=1, keepdims=True), sums)

        return lax.fori_loop(0, lines, scale, jnp.zeros((species, points), f32), unroll=8)

    def filtered(step, sums):
        for r in range(groups):
            value = recv_refs[step][r]
            rest = value - value.astype(bf16).astype(f32)
            both_ref[:, r * points : (r + 1) * points] = jnp.concatenate([value, rest], axis=0).astype(bf16)
        acc = dot(both_ref[...], fold_ref[...])
        return 0.5 * mid_ref[...] + (0.5 / points) * (sums + (acc[:species] + acc[species:]))

    def land(step, out):
        base = send_rows + step * (blocks + 1)
        sums_ref[total] = jnp.zeros((species, points), f32)
        acc = jnp.zeros((species, points), f32)
        for b in range(blocks):

            def run(i, acc):
                code = tab_smem[base + b, 0, i]
                value = pltpu.roll(recv_refs[step][code >> bits(points)], code & (points - 1), 1)
                n = b * points + i
                acc = value * mask_ref[step, pl.ds(n, 1), :] + acc * keep_ref[step, pl.ds(n, 1), :]
                sums_ref[n] = acc
                return acc

            acc = lax.fori_loop(0, points, run, acc, unroll=32)

        def settle(l, carry):
            y_ref[l] = z_ref[l] + sums_ref[tab_smem[base + blocks, 0, l]]
            return carry

        for p in range(parts):
            lax.fori_loop(p * lines // parts, (p + 1) * lines // parts, settle, 0, unroll=32)
            if out:
                out[p].start()

    load.wait()
    diffuse(0)
    for copy in rim_copies(0):
        copy.wait()
    middle(0)
    send_table.wait()
    chemistry()
    exchange(0)

    def aim_finish(j, carry):
        aim_copy(j).wait()
        return carry

    lax.fori_loop(1, groups, aim_finish, 0)
    arrivals()
    sums = prepare(0)
    collect(0)
    field_ref[1] = filtered(0, sums)
    for copy in rim_copies(1):
        copy.start()
    land(0, None)
    diffuse(1)
    for copy in rim_copies(1):
        copy.wait()
    middle(1)
    chemistry()
    exchange(1)
    sums = prepare(1)
    collect(1)
    les_ref[...] = filtered(1, sums).reshape(species, 1, lines)
    last = pltpu.make_async_copy(les_ref, les_out, out_sem.at[parts])
    last.start()
    out = [
        pltpu.make_async_copy(
            y_ref.at[pl.ds(p * lines // parts, lines // parts)],
            lines_out.at[pl.ds(p * lines // parts, lines // parts)],
            out_sem.at[p],
        )
        for p in range(parts)
    ]
    land(1, out)
    for copy in out + [last]:
        copy.wait()


def deliver_kernel(les_in, lines_in, les_out, lines_out, les_ref, lines_ref, in_sem, out_sem):
    parts = in_sem.shape[0] - 1
    size = lines_ref.shape[0] // parts
    pairs = [(les_in, les_ref, les_out)]
    for p in range(parts):
        at = pl.ds(p * size, size)
        pairs.append((lines_in.at[at], lines_ref.at[at], lines_out.at[at]))
    takes = [pltpu.make_async_copy(a, b, in_sem.at[n]) for n, (a, b, c) in enumerate(pairs)]
    gives = [pltpu.make_async_copy(b, c, out_sem.at[n]) for n, (a, b, c) in enumerate(pairs)]
    for take in takes:
        take.start()
    for take, give in zip(takes, gives):
        take.wait()
        give.start()
    for give in gives:
        give.wait()


def body(
    les,
    lines,
    triplet_start,
    splice_owner,
    splice_line,
    splice_from,
    splice_to,
    chem_counts,
    diffusivity,
    rates,
    frozen_inverse,
):
    groups = lax.axis_size("grid") * lax.axis_size("line")
    _, _, count, species, points = lines.shape
    segments = points // SEG
    slots = min(segments, max(2, 2 * count // groups))
    total = groups * slots
    blocks = total // points
    rows = STEPS * (2 * blocks + 1)

    dma = pltpu.SemaphoreType.DMA
    field, state = pl.pallas_call(
        functools.partial(kernel, slots),
        out_shape=(
            jax.ShapeDtypeStruct((species, 1, count), f32),
            jax.ShapeDtypeStruct((count, species, points), f32),
        ),
        in_specs=[HBM] * 11,
        out_specs=(HBM, HBM),
        scratch_shapes=[
            pltpu.VMEM((species, 1, count), f32),
            *[pltpu.VMEM((STEPS, count), i32)] * 5,
            pltpu.VMEM((species, species), f32),
            pltpu.VMEM((species, species), f32),
            pltpu.SMEM((species,), f32),
            pltpu.SMEM((count,), i32),
            *[pltpu.VMEM((species, points), f32)] * 3,
            pltpu.VMEM((count, species, points), f32),
            pltpu.VMEM((count, species, points), f32),
            pltpu.VMEM((species, points, points), bf16),
            pltpu.VMEM((species, points, points), bf16),
            pltpu.VMEM((STEPS, groups, species, points), f32),
            pltpu.VMEM((groups, species, points), f32),
            pltpu.VMEM((groups, species, points), f32),
            pltpu.VMEM((total + 1, species, points), f32),
            pltpu.VMEM((STEPS, total, points), f32),
            pltpu.VMEM((STEPS, total, points), f32),
            pltpu.VMEM((STEPS, total, count), f32),
            pltpu.VMEM((groups * points, count), bf16),
            pltpu.VMEM((2 * species, groups * points), bf16),
            pltpu.VMEM((STEPS, count, points), f32),
            pltpu.VMEM((STEPS, 4, species, count), f32),
            pltpu.VMEM((STEPS, species, count), f32),
            pltpu.VMEM((species, count), f32),
            pltpu.VMEM((blocks, STEPS, points), i32),
            pltpu.VMEM((groups, STEPS, points), i32),
            pltpu.VMEM((total, points), i32),
            pltpu.VMEM((rows, 1, points), i32),
            pltpu.SMEM((rows, 1, points), i32),
            dma((11,)),
            dma((2,)),
            dma((STEPS, 4)),
            dma((STEPS, 4)),
            dma((groups,)),
            dma((groups,)),
            dma((STEPS, groups)),
            dma((STEPS, groups)),
            dma((5,)),
        ],
        compiler_params=pltpu.CompilerParams(
            collective_id=0, has_side_effects=True, vmem_limit_bytes=67043328
        ),
        name="steps",
    )(
        les.reshape(species, 1, count),
        lines.reshape(count, species, points),
        triplet_start.reshape(STEPS, count),
        splice_owner.reshape(STEPS, count),
        splice_line.reshape(STEPS, count),
        splice_from.reshape(STEPS, count),
        splice_to.reshape(STEPS, count),
        rates,
        frozen_inverse,
        diffusivity,
        chem_counts.reshape(count),
    )
    field, state = pl.pallas_call(
        deliver_kernel,
        out_shape=(jax.ShapeDtypeStruct(field.shape, f32), jax.ShapeDtypeStruct(state.shape, f32)),
        in_specs=[HBM] * 2,
        out_specs=(HBM, HBM),
        scratch_shapes=[
            pltpu.VMEM(field.shape, f32),
            pltpu.VMEM(state.shape, f32),
            dma((9,)),
            dma((9,)),
        ],
        compiler_params=pltpu.CompilerParams(vmem_limit_bytes=67043328),
        name="deliver",
    )(field, state)
    return (field.reshape(les.shape), state.reshape(lines.shape))


def solution(mesh):
    in_specs = (
        P(None, "grid", "line"),
        P("grid", "line", None, None, None),
        P(None, "grid", "line", None),
        P(None, "grid", "line", None, None),
        P(None, "grid", "line", None),
        P(None, "grid", "line", None),
        P(None, "grid", "line", None),
        P("grid", "line", None),
        P(),
        P(),
        P(),
    )
    out_specs = (P(None, "grid", "line"), P("grid", "line", None, None, None))
    return jax.shard_map(body, mesh=mesh, in_specs=in_specs, out_specs=out_specs, check_vma=False)
```

```python
import functools

import jax
import jax.numpy as jnp
from jax import lax
from jax.experimental import pallas as pl
from jax.experimental.pallas import tpu as pltpu
from jax.sharding import PartitionSpec as P

SEG = 16
TRIP = 48
STEPS = 2
SUBSTEPS = 6
WAVES = 3
CHUNK = 64

les_rate = 0.2
relax_rate = 0.5
splice_weight = 0.5

NAMES = ("grid", "line")
MESH = pl.DeviceIdType.MESH
VMEM = pl.BlockSpec(memory_space=pltpu.VMEM)
SMEM = pl.BlockSpec(memory_space=pltpu.SMEM)
HBM = pl.BlockSpec(memory_space=pltpu.HBM)
f32 = jnp.float32
bf16 = jnp.bfloat16
i32 = jnp.int32

dot = functools.partial(jnp.dot, preferred_element_type=jnp.float32)


def halves(value):
    top = value.astype(bf16)
    return top, (value - top.astype(f32)).astype(bf16)


def column(row):
    points = row.shape[1]
    return jnp.transpose(jnp.broadcast_to(row, (points, points)))


def iota(shape, axis):
    return lax.broadcasted_iota(i32, shape, axis)


def bits(size):
    assert size & (size - 1) == 0
    return size.bit_length() - 1


def when(condition, value):
    return jnp.where(condition, value, 0)


def total_of(value, axis):
    return jnp.sum(value, axis=axis, keepdims=True, dtype=i32)


def kernel(
    slots,
    les_hbm,
    lines_hbm,
    start_hbm,
    owner_hbm,
    line_hbm,
    from_hbm,
    to_hbm,
    rates_hbm,
    frozen_hbm,
    coeff_hbm,
    counts_hbm,
    les_out,
    lines_out,
    les_ref,
    start_ref,
    owner_ref,
    line_ref,
    from_ref,
    to_ref,
    rates_ref,
    frozen_ref,
    coeff_ref,
    counts_row,
    coeffs_ref,
    apart_ref,
    ends_ref,
    y_ref,
    z_ref,
    s_ref,
    order_ref,
    matrix_ref,
    send_ref,
    recv_00,
    recv_01,
    recv_02,
    recv_10,
    recv_11,
    recv_12,
    sums_0,
    sums_1,
    sums_2,
    mask_ref,
    keep_ref,
    into_ref,
    fold_ref,
    both_ref,
    weight_ref,
    rim_ref,
    field_ref,
    mid_ref,
    middle_ref,
    aim_ref,
    got_ref,
    flat_ref,
    tab_ref,
    tab_smem,
    load_sem,
    tab_sem,
    rim_send,
    rim_recv,
    aim_send,
    aim_recv,
    send_sem,
    recv_sem,
    out_sem,
):
    parts = out_sem.shape[0] - 1
    waves = WAVES
    species, _, lines = les_ref.shape
    points = y_ref.shape[2]
    segments = points // SEG
    size = [lax.axis_size(n) for n in NAMES]
    at = [lax.axis_index(n) for n in NAMES]
    groups = size[0] * size[1]
    me = at[0] * size[1] + at[1]
    total = groups * slots
    blocks = total // points
    recv_refs = ((recv_00, recv_01, recv_02), (recv_10, recv_11, recv_12))
    sums_refs = (sums_0, sums_1, sums_2)

    def place(j):
        peer = (me + j) & (groups - 1)
        return peer, (peer >> bits(size[1]), peer & (size[1] - 1))

    half = groups // 2
    turns = ((half, groups), (0, half // 2), (half // 2, half))
    barrier = pltpu.get_barrier_semaphore()

    def greet(j, carry):
        pl.semaphore_signal(barrier, inc=1, device_id=place(j)[1], device_id_type=MESH)
        return carry

    lax.fori_loop(1, groups, greet, 0)
    tables = [
        pltpu.make_async_copy(source, target, load_sem.at[n])
        for n, (source, target) in enumerate(
            [
                (coeff_hbm, coeff_ref),
                (owner_hbm, owner_ref),
                (from_hbm, from_ref),
                (line_hbm, line_ref),
                (to_hbm, to_ref),
                (les_hbm, les_ref),
                (start_hbm, start_ref),
                (counts_hbm, counts_row),
                (rates_hbm, rates_ref),
                (frozen_hbm, frozen_ref),
            ]
        )
    ]
    load = pltpu.make_async_copy(lines_hbm, y_ref, load_sem.at[len(tables)])
    for copy in tables:
        copy.start()
    load.start()

    rims = []
    for axis in (0, 1):
        for move in (1, size[axis] - 1):
            there = list(at)
            there[axis] = lax.rem(at[axis] + move, size[axis])
            rims.append(tuple(there))

    def rim_copies(step):
        return [
            pltpu.make_async_remote_copy(
                src_ref=field_ref.at[step],
                dst_ref=rim_ref.at[step, k],
                send_sem=rim_send.at[step, k],
                recv_sem=rim_recv.at[step, k],
                device_id=rims[k],
                device_id_type=MESH,
            )
            for k in range(4)
        ]

    def aim_copy(j):
        peer, device = place(j)
        return pltpu.make_async_remote_copy(
            src_ref=aim_ref.at[(peer * slots) >> bits(points)],
            dst_ref=got_ref.at[me],
            send_sem=aim_send.at[j],
            recv_sem=aim_recv.at[j],
            device_id=device,
            device_id_type=MESH,
        )

    def turn_of(i, sign):
        low = (me + sign * i) & (half - 1)
        return jnp.where(i < half, me ^ half, me) & half | low

    def data_copy(step, wave, j):
        peer = turn_of(j, 1)
        device = (peer >> bits(size[1]), peer & (size[1] - 1))
        return pltpu.make_async_remote_copy(
            src_ref=send_ref.at[step, peer],
            dst_ref=recv_refs[step][wave].at[j - turns[wave][0]],
            send_sem=send_sem.at[step, j],
            recv_sem=recv_sem.at[step, j],
            device_id=device,
            device_id_type=MESH,
        )

    tables[0].wait()
    lane = iota((points, points), 1)
    row = iota((points, points), 0)
    for n in range(species):
        coeffs_ref[n : n + 1, :] = jnp.full((1, points), coeff_ref[n], f32)
    coeff = coeffs_ref[...]
    root = jnp.sqrt(4.0 * coeff + 1.0)
    theta = -jnp.log(2.0 * coeff / (2.0 * coeff + 1.0 + root))
    scale = 1.0 / (root * (1.0 - jnp.exp(-2.0 * points * theta)))
    along = iota((species, points), 1).astype(f32)
    apart_ref[...] = scale * (jnp.exp(-along * theta) + jnp.exp((along - 2.0 * points) * theta)) - relax_rate / points
    ends_ref[...] = scale * (jnp.exp(-(along + 1.0) * theta) + jnp.exp((along + 1.0 - 2.0 * points) * theta))
    apart = jnp.abs(lane - row)
    ends = jnp.minimum(lane + row, 2 * points - 2 - lane - row)

    def spread(ref, n, index):
        value = jnp.broadcast_to(ref[pl.ds(n, 1), :], (points, points))
        return jnp.take_along_axis(value, index, axis=1, mode="promise_in_bounds")

    def inverse(n, carry):
        top, rest = halves(spread(apart_ref, n, apart) + spread(ends_ref, n, ends))
        matrix_ref[n] = jnp.concatenate([top, rest], axis=1)
        return carry

    lax.fori_loop(0, species, inverse, 0, unroll=4)
    for copy in tables[1:]:
        copy.wait()
    field_ref[0] = les_ref[...].reshape(species, lines)


    for step in range(STEPS):
        owner = owner_ref[step : step + 1, :]
        rank = total_of(when((column(owner) == owner) & (row < lane), 1), 0)
        spot = column(owner * slots + rank)
        turn = (owner - me) & (half - 1)
        key = (jnp.where((owner ^ me) & half == 0, half, 0) + turn) * lines + iota((1, points), 1)
        spot_sorted = total_of(when(column(key) < key, 1), 0)
        first = step * (blocks + 2) + blocks
        tab_ref[first] = spot_sorted
        sorted_code = column(iota((1, points), 1) * 8 + counts_row[...])
        order = total_of(when(column(spot_sorted) == lane, sorted_code), 0)
        tab_ref[first + 1] = order
        order_ref[step] = jnp.broadcast_to(order >> 3, (species, points))
        turn = (SEG * (rank - from_ref[step : step + 1, :])) & (points - 1)
        code = column(spot_sorted * points + turn)
        aim = column(line_ref[step : step + 1, :] * segments + to_ref[step : step + 1, :] + 1)
        for b in range(blocks):
            hit = spot == lane + b * points
            tab_ref[step * (blocks + 2) + b] = total_of(when(hit, code), 0)
            aim_ref[b, step : step + 1, :] = total_of(when(hit, aim), 0)
    send_rows = STEPS * (blocks + 2)
    send_table = pltpu.make_async_copy(tab_ref.at[pl.ds(0, send_rows)], tab_smem.at[pl.ds(0, send_rows)], tab_sem.at[0])
    send_table.start()

    pl.semaphore_wait(barrier, groups - 1)
    for copy in rim_copies(0):
        copy.start()

    def aim_start(j, carry):
        aim_copy(j).start()
        return carry

    lax.fori_loop(1, groups, aim_start, 0)
    got_ref[me] = aim_ref[(me * slots) >> bits(points)]

    flat_y = y_ref.reshape(lines * species, points)
    flat_z = z_ref.reshape(lines * species, points)

    def diffuse(step):
        rel = lane - column(start_ref[step : step + 1, :])
        third = TRIP // 3
        source = jnp.where(
            rel < third,
            3 * rel,
            jnp.where(rel < 2 * third, 3 * (2 * third - 1 - rel) + 1, 3 * (rel - 2 * third) + 2),
        )
        index = jnp.where((rel >= 0) & (rel < TRIP), source + (lane - rel), lane)

        def one(s, carry):
            y = flat_y[pl.ds(s, lines, stride=species), :]
            y = jnp.take_along_axis(y, index, axis=1, mode="promise_in_bounds")
            right = matrix_ref[s]
            out = dot(jnp.concatenate(halves(y), axis=1), jnp.concatenate([right, right], axis=0))
            flat_z[pl.ds(s, lines, stride=species), :] = out[:, :points] + out[:, points:]
            return carry

        lax.fori_loop(0, species, one, 0, unroll=12)

    lane_s = lax.broadcasted_iota(i32, (species, points), 1)

    def middle(step):
        field = field_ref[step]
        up = jnp.where(at[0] > 0, rim_ref[step, 0], 0.0)
        down = jnp.where(at[0] < size[0] - 1, rim_ref[step, 1], 0.0)
        left = jnp.where(at[1] > 0, rim_ref[step, 2], 0.0)
        right = jnp.where(at[1] < size[1] - 1, rim_ref[step, 3], 0.0)
        before = pltpu.roll(jnp.where(lane_s == points - 1, left, field), 1, 1)
        after = pltpu.roll(jnp.where(lane_s == 0, right, field), points - 1, 1)
        mid_ref[...] = field + les_rate * (up + down + before + after - 4.0 * field)

    joint = jnp.dot(
        frozen_ref[...], rates_ref[...], precision=lax.Precision.HIGHEST, preferred_element_type=f32
    )
    joint_top, joint_rest = halves(joint)
    wide = (2 * species, 6 * species)
    place_c = iota(wide, 1)
    block_c = sum((place_c >= species * n).astype(i32) for n in range(1, 6))
    pick = jnp.where(
        iota((species, 6 * species), 0) == (place_c - species * block_c)[:species], 1.0, 0.0
    ).astype(bf16)
    twice_top = dot(jnp.concatenate([joint_top.astype(f32)] * 2, axis=0).astype(bf16), pick)
    twice_rest = dot(jnp.concatenate([joint_rest.astype(f32)] * 2, axis=0).astype(bf16), pick)
    entries = jnp.where((block_c >> 1) == 1, twice_rest, twice_top)
    matrix = jnp.where((iota(wide, 0) >= species).astype(i32) == (block_c & 1), entries, 0.0).astype(bf16)

    segment = lane_s // SEG

    def pack(step, peer):
        tile = jnp.zeros((species, points), f32)
        first = peer * slots
        for k in range(slots):
            code = tab_smem[step * (blocks + 2) + (first >> bits(points)), 0, (first & (points - 1)) + k]
            value = pltpu.roll(s_ref[code >> bits(points)], code & (points - 1), 1)
            tile = jnp.where(segment == k, value, tile)
        return tile

    def chemistry(step, base):
        orders = step * (blocks + 2) + blocks + 1
        mid = middle_ref[...]
        codes = [tab_smem[orders, 0, base + i] for i in range(CHUNK)]
        for sub in range(SUBSTEPS):
            for q in range(0, CHUNK, 4):
                columns = []
                state = []
                for h in (0, 2):
                    if sub == 0:
                        y = jnp.concatenate(
                            [
                                z_ref[codes[i] >> 3] + jnp.broadcast_to(mid[:, base + i : base + i + 1], (species, points))
                                for i in (q + h, q + h + 1)
                            ],
                            axis=0,
                        )
                    else:
                        y = s_ref[pl.ds(base + q + h, 2)].reshape(2 * species, points)
                    state.append(y)
                    top, rest = halves(jnp.tanh(y))
                    columns.append(jnp.concatenate([top, top, rest], axis=0))
                change = dot(matrix, jnp.concatenate(columns, axis=1))
                for h in (0, 1):
                    for k in (0, 1):
                        i = q + 2 * h + k
                        factor = jnp.where(codes[i] & 7 > sub, f32(1.0), f32(0.0))
                        rows = slice(k * species, (k + 1) * species)
                        s_ref[base + i] = state[h][rows] + factor * change[rows, h * points : (h + 1) * points]

    def exchange(step):
        middle_ref[...] = relax_rate * jnp.take_along_axis(
            mid_ref[...], order_ref[step], axis=1, mode="promise_in_bounds"
        )
        many = CHUNK // slots

        def wrap(i):
            peer = turn_of(i, 1)
            send_ref[step, peer] = pack(step, peer)

        for c in range(lines // CHUNK):
            chemistry(step, c * CHUNK)
            for n in range(many):
                wrap(c * many + n)
            for n in range(many):
                data_copy(step, 1 if c * many + n < half // 2 else 2, c * many + n).start()

        def near(i, carry):
            for n in range(2):
                wrap(half + 2 * i + n)
            for n in range(2):
                before = half + 2 * (i - 1) + n

                @pl.when(before > half)
                def _():
                    data_copy(step, 0, before).start()

            return carry

        lax.fori_loop(0, half // 2, near, 0)
        recv_refs[step][0][0] = send_ref[step, me]
        for n in range(groups - 2, groups):
            data_copy(step, 0, n).start()

    def arrivals():
        number = iota((total, 1), 0)
        lane_t = iota((total, points), 1)
        number_r = iota((1, total), 1)
        offset = (me * slots) & (points - 1)
        mine = offset + (iota((total, points), 0) & (slots - 1))
        for step in range(STEPS):
            for r in range(groups):
                flat_ref[r * slots : (r + 1) * slots, :] = jnp.broadcast_to(
                    got_ref[r, step : step + 1, :], (slots, points)
                )
            code = total_of(when(lane_t == mine, flat_ref[...]), 1)
            valid = code > 0
            code = code - 1
            line = jnp.where(valid, code >> bits(segments), lines)
            seg = code & (segments - 1)
            source = number >> bits(slots)
            deep = (me - source) & (half - 1)
            late = jnp.where((source ^ me) & half == 0, 0, jnp.where(deep >= half // 2, 2, 1))
            slot = jnp.where(late == 2, deep - half // 2, deep)
            line = line + late * (lines + 1)
            line_c = jnp.broadcast_to(line, (total, points))
            line_r = jnp.concatenate(
                [jnp.transpose(line_c[b * points : (b + 1) * points])[:1] for b in range(blocks)], axis=1
            )
            key_r = line_r * total + number_r
            key_c = line * total + number
            below = key_r < key_c
            position = total_of(when(below, 1), 1)
            same = total_of(when(below & (line_r == line), 1), 1)
            turn = (SEG * (seg - (number & (slots - 1)))) & (points - 1)
            value = slot * points + turn
            kind = seg * 2 + when(same == 0, 1)
            base = send_rows + step * (blocks + waves)
            for b in range(blocks):
                hit = position == lane_t + b * points
                tab_ref[base + b] = total_of(when(hit, value), 0)
                kinds = column(total_of(when(hit, kind), 0))
                at_b = pl.ds(b * points, points)
                mask_ref[step, at_b, :] = jnp.where((kinds >> 1) == (lane >> bits(SEG)), splice_weight, 0.0)
                keep_ref[step, at_b, :] = jnp.where((kinds & 1) == 1, 0.0, 1.0)
            starts = (0, total // 2, total // 2 + total // 4, total)
            in_c = jnp.zeros((total, points), jnp.bool_)
            in_r = jnp.zeros((lines, total), jnp.bool_)
            for w in range(waves):
                aim_c = lane_t + w * (lines + 1)
                upto = total_of(when(line_c <= aim_c, 1), 0)
                many = total_of(when(line_c == aim_c, 1), 0)
                tab_ref[base + blocks + w] = jnp.where(many > 0, upto - 1 - starts[w], starts[w + 1] - starts[w])
                in_c = in_c | (line_c == aim_c)
                in_r = in_r | (line_r == iota((lines, total), 0) + w * (lines + 1))
            lands = jnp.where(in_r, 1.0, 0.0).astype(bf16)
            covers = jnp.where(seg == (lane_t >> bits(SEG)), 1.0, 0.0).astype(bf16)
            weight_ref[step] = 1.0 - splice_weight * dot(lands, covers)
            into_ref[step] = jnp.where(in_c, splice_weight, 0.0)
        rows = STEPS * (blocks + waves)
        copy = pltpu.make_async_copy(
            tab_ref.at[pl.ds(send_rows, rows)], tab_smem.at[pl.ds(send_rows, rows)], tab_sem.at[1]
        )
        copy.start()
        copy.wait()

    def prepare(step):
        def rows(j, carry):
            block = jnp.broadcast_to(into_ref[step, pl.ds(j, 1), :], (SEG, lines))
            source = j >> bits(slots)
            first = jnp.where(source & half == me & half, half, 0) + ((me - source) & (half - 1))
            first = first * points + (j & (slots - 1)) * SEG
            fold_ref[pl.ds(pl.multiple_of(first, SEG), SEG), :] = block.astype(bf16)
            return carry

        if slots < segments:
            fold_ref[...] = jnp.zeros_like(fold_ref)
        lax.fori_loop(0, total, rows, 0, unroll=8)

        places = step * (blocks + 2) + blocks

        def scale(l, sums):
            value = s_ref[tab_smem[places, 0, l]] * weight_ref[step, pl.ds(l, 1), :]
            y_ref[l] = value
            return jnp.where(lane_s == l, jnp.sum(value, axis=1, keepdims=True), sums)

        return lax.fori_loop(0, lines, scale, jnp.zeros((species, points), f32), unroll=8)

    def collect(step, wave):
        def finish(j, carry):
            data_copy(step, wave, j).wait()
            return carry

        low, high = turns[wave]
        lax.fori_loop(low + (wave == 0), high, finish, 0)

    def filtered(step, wave):
        low, high = turns[wave]
        for i in range(low, high):
            value = recv_refs[step][wave][i - low]
            rest = value - value.astype(bf16).astype(f32)
            both_ref[:, i * points : (i + 1) * points] = jnp.concatenate([value, rest], axis=0).astype(bf16)
        acc = dot(both_ref[:, low * points : high * points], fold_ref[low * points : high * points, :])
        return acc[:species] + acc[species:]

    def run(step, wave, acc):
        base = send_rows + step * (blocks + waves)
        begin = sum(high - low for low, high in turns[:wave]) * slots
        end = begin + (turns[wave][1] - turns[wave][0]) * slots

        at_row = base + (begin >> bits(points))
        at_lane = begin & (points - 1)
        assert at_lane + end - begin <= points

        def one(i, acc):
            code = tab_smem[at_row, 0, at_lane + i]
            value = pltpu.roll(recv_refs[step][wave][code >> bits(points)], code & (points - 1), 1)
            acc = value * mask_ref[step, pl.ds(begin + i, 1), :] + acc * keep_ref[step, pl.ds(begin + i, 1), :]
            sums_refs[wave][i] = acc
            return acc

        sums_refs[wave][end - begin] = jnp.zeros((species, points), f32)
        lax.fori_loop(0, end - begin, one, jnp.zeros((species, points), f32), unroll=32)

    def receive(step, sums, les_done, out):
        base = send_rows + step * (blocks + waves)

        def settle(which):
            def one(l, carry):
                value = y_ref[l]
                for w in which:
                    value = value + sums_refs[w][tab_smem[base + blocks + w, 0, l]]
                y_ref[l] = value
                return carry

            return one

        for wave in range(waves):
            collect(step, wave)
            sums = sums + filtered(step, wave)
            if wave + 1 < waves:
                run(step, wave, None)
            if wave + 2 == waves:
                lax.fori_loop(0, lines, settle(range(waves - 1)), 0, unroll=8)
        les_done(0.5 * mid_ref[...] + (0.5 / points) * sums)
        run(step, waves - 1, None)
        for p in range(parts):
            low, high = p * lines // parts, (p + 1) * lines // parts
            lax.fori_loop(low, high, settle((waves - 1,)), 0, unroll=32)
            if out:
                out[p].start()

    load.wait()
    diffuse(0)
    for copy in rim_copies(0):
        copy.wait()
    middle(0)
    send_table.wait()
    exchange(0)

    def aim_finish(j, carry):
        aim_copy(j).wait()
        return carry

    lax.fori_loop(1, groups, aim_finish, 0)
    arrivals()
    sums = prepare(0)

    def again(field):
        field_ref[1] = field
        for copy in rim_copies(1):
            copy.start()

    receive(0, sums, again, None)
    diffuse(1)
    for copy in rim_copies(1):
        copy.wait()
    middle(1)
    exchange(1)
    sums = prepare(1)
    last = pltpu.make_async_copy(les_ref, les_out, out_sem.at[parts])
    out = [
        pltpu.make_async_copy(
            y_ref.at[pl.ds(p * lines // parts, lines // parts)],
            lines_out.at[pl.ds(p * lines // parts, lines // parts)],
            out_sem.at[p],
        )
        for p in range(parts)
    ]

    def finish(field):
        les_ref[...] = field.reshape(species, 1, lines)
        last.start()

    receive(1, sums, finish, out)
    for copy in out + [last]:
        copy.wait()


def deliver_kernel(les_in, lines_in, les_out, lines_out, les_ref, lines_ref, in_sem, out_sem):
    parts = in_sem.shape[0] - 1
    size = lines_ref.shape[0] // parts
    pairs = [(les_in, les_ref, les_out)]
    for p in range(parts):
        at = pl.ds(p * size, size)
        pairs.append((lines_in.at[at], lines_ref.at[at], lines_out.at[at]))
    takes = [pltpu.make_async_copy(a, b, in_sem.at[n]) for n, (a, b, c) in enumerate(pairs)]
    gives = [pltpu.make_async_copy(b, c, out_sem.at[n]) for n, (a, b, c) in enumerate(pairs)]
    for take in takes:
        take.start()
    for take, give in zip(takes, gives):
        take.wait()
        give.start()
    for give in gives:
        give.wait()


def body(
    les,
    lines,
    triplet_start,
    splice_owner,
    splice_line,
    splice_from,
    splice_to,
    chem_counts,
    diffusivity,
    rates,
    frozen_inverse,
):
    groups = lax.axis_size("grid") * lax.axis_size("line")
    _, _, count, species, points = lines.shape
    segments = points // SEG
    slots = min(segments, max(2, 2 * count // groups))
    total = groups * slots
    blocks = total // points
    rows = STEPS * (2 * blocks + 2 + WAVES)

    dma = pltpu.SemaphoreType.DMA
    field, state = pl.pallas_call(
        functools.partial(kernel, slots),
        out_shape=(
            jax.ShapeDtypeStruct((species, 1, count), f32),
            jax.ShapeDtypeStruct((count, species, points), f32),
        ),
        in_specs=[HBM] * 11,
        out_specs=(HBM, HBM),
        scratch_shapes=[
            pltpu.VMEM((species, 1, count), f32),
            *[pltpu.VMEM((STEPS, count), i32)] * 5,
            pltpu.VMEM((species, species), f32),
            pltpu.VMEM((species, species), f32),
            pltpu.SMEM((species,), f32),
            pltpu.VMEM((1, count), i32),
            *[pltpu.VMEM((species, points), f32)] * 3,
            pltpu.VMEM((count, species, points), f32),
            pltpu.VMEM((count, species, points), f32),
            pltpu.VMEM((count, species, points), f32),
            pltpu.VMEM((STEPS, species, count), i32),
            pltpu.VMEM((species, points, 2 * points), bf16),
            pltpu.VMEM((STEPS, groups, species, points), f32),
            *[
                pltpu.VMEM((groups // part, species, points), f32)
                for part in (2, 4, 4) * STEPS
            ],
            pltpu.VMEM((total // 2 + 1, species, points), f32),
            *[pltpu.VMEM((total // 4 + 1, species, points), f32)] * 2,
            pltpu.VMEM((STEPS, total, points), f32),
            pltpu.VMEM((STEPS, total, points), f32),
            pltpu.VMEM((STEPS, total, count), f32),
            pltpu.VMEM((groups * points, count), bf16),
            pltpu.VMEM((2 * species, groups * points), bf16),
            pltpu.VMEM((STEPS, count, points), f32),
            pltpu.VMEM((STEPS, 4, species, count), f32),
            pltpu.VMEM((STEPS, species, count), f32),
            pltpu.VMEM((species, count), f32),
            pltpu.VMEM((species, count), f32),
            pltpu.VMEM((blocks, STEPS, points), i32),
            pltpu.VMEM((groups, STEPS, points), i32),
            pltpu.VMEM((total, points), i32),
            pltpu.VMEM((rows, 1, points), i32),
            pltpu.SMEM((rows, 1, points), i32),
            dma((11,)),
            dma((2,)),
            dma((STEPS, 4)),
            dma((STEPS, 4)),
            dma((groups,)),
            dma((groups,)),
            dma((STEPS, groups)),
            dma((STEPS, groups)),
            dma((5,)),
        ],
        compiler_params=pltpu.CompilerParams(
            collective_id=0, has_side_effects=True, vmem_limit_bytes=67043328
        ),
        name="steps",
    )(
        les.reshape(species, 1, count),
        lines.reshape(count, species, points),
        triplet_start.reshape(STEPS, count),
        splice_owner.reshape(STEPS, count),
        splice_line.reshape(STEPS, count),
        splice_from.reshape(STEPS, count),
        splice_to.reshape(STEPS, count),
        rates,
        frozen_inverse,
        diffusivity,
        chem_counts.reshape(1, count),
    )
    field, state = pl.pallas_call(
        deliver_kernel,
        out_shape=(jax.ShapeDtypeStruct(field.shape, f32), jax.ShapeDtypeStruct(state.shape, f32)),
        in_specs=[HBM] * 2,
        out_specs=(HBM, HBM),
        scratch_shapes=[
            pltpu.VMEM(field.shape, f32),
            pltpu.VMEM(state.shape, f32),
            dma((9,)),
            dma((9,)),
        ],
        compiler_params=pltpu.CompilerParams(vmem_limit_bytes=67043328),
        name="deliver",
    )(field, state)
    return (field.reshape(les.shape), state.reshape(lines.shape))


def solution(mesh):
    in_specs = (
        P(None, "grid", "line"),
        P("grid", "line", None, None, None),
        P(None, "grid", "line", None),
        P(None, "grid", "line", None, None),
        P(None, "grid", "line", None),
        P(None, "grid", "line", None),
        P(None, "grid", "line", None),
        P("grid", "line", None),
        P(),
        P(),
        P(),
    )
    out_specs = (P(None, "grid", "line"), P("grid", "line", None, None, None))
    return jax.shard_map(body, mesh=mesh, in_specs=in_specs, out_specs=out_specs, check_vma=False)
```

```python
import functools

import jax
import jax.numpy as jnp
from jax import lax
from jax.experimental import pallas as pl
from jax.experimental.pallas import tpu as pltpu
from jax.sharding import PartitionSpec as P

SEG = 16
TRIP = 48
STEPS = 2
SUBSTEPS = 6
WAVES = 3
CHUNK = 64

les_rate = 0.2
relax_rate = 0.5
splice_weight = 0.5

NAMES = ("grid", "line")
MESH = pl.DeviceIdType.MESH
VMEM = pl.BlockSpec(memory_space=pltpu.VMEM)
SMEM = pl.BlockSpec(memory_space=pltpu.SMEM)
HBM = pl.BlockSpec(memory_space=pltpu.HBM)
f32 = jnp.float32
bf16 = jnp.bfloat16
i32 = jnp.int32

dot = functools.partial(jnp.dot, preferred_element_type=jnp.float32)


def halves(value):
    top = value.astype(bf16)
    return top, (value - top.astype(f32)).astype(bf16)


def column(row):
    points = row.shape[1]
    return jnp.transpose(jnp.broadcast_to(row, (points, points)))


def iota(shape, axis):
    return lax.broadcasted_iota(i32, shape, axis)


def bits(size):
    assert size & (size - 1) == 0
    return size.bit_length() - 1


def when(condition, value):
    return jnp.where(condition, value, 0)


def total_of(value, axis):
    return jnp.sum(value, axis=axis, keepdims=True, dtype=i32)


def kernel(
    slots,
    les_hbm,
    lines_hbm,
    start_hbm,
    owner_hbm,
    line_hbm,
    from_hbm,
    to_hbm,
    rates_hbm,
    frozen_hbm,
    coeff_hbm,
    counts_hbm,
    les_out,
    lines_out,
    tiles_out,
    mask_out,
    keep_out,
    table_out,
    les_ref,
    start_ref,
    owner_ref,
    line_ref,
    from_ref,
    to_ref,
    rates_ref,
    frozen_ref,
    coeff_ref,
    counts_row,
    coeffs_ref,
    apart_ref,
    ends_ref,
    y_ref,
    z_ref,
    s_ref,
    order_ref,
    matrix_ref,
    send_ref,
    recv_00,
    recv_01,
    recv_02,
    recv_10,
    recv_11,
    recv_12,
    sums_0,
    sums_1,
    sums_2,
    mask_ref,
    keep_ref,
    into_ref,
    fold_ref,
    both_ref,
    weight_ref,
    rim_ref,
    field_ref,
    mid_ref,
    middle_ref,
    aim_ref,
    got_ref,
    flat_ref,
    tab_ref,
    tab_smem,
    load_sem,
    tab_sem,
    rim_send,
    rim_recv,
    aim_send,
    aim_recv,
    send_sem,
    recv_sem,
    out_sem,
):
    parts = out_sem.shape[0] - 6
    waves = WAVES
    species, _, lines = les_ref.shape
    points = y_ref.shape[2]
    segments = points // SEG
    size = [lax.axis_size(n) for n in NAMES]
    at = [lax.axis_index(n) for n in NAMES]
    groups = size[0] * size[1]
    me = at[0] * size[1] + at[1]
    total = groups * slots
    blocks = total // points
    recv_refs = ((recv_00, recv_01, recv_02), (recv_10, recv_11, recv_12))
    sums_refs = (sums_0, sums_1, sums_2)

    def place(j):
        peer = (me + j) & (groups - 1)
        return peer, (peer >> bits(size[1]), peer & (size[1] - 1))

    half = groups // 2
    turns = ((half, groups), (0, half // 2), (half // 2, half))
    barrier = pltpu.get_barrier_semaphore()

    def greet(j, carry):
        pl.semaphore_signal(barrier, inc=1, device_id=place(j)[1], device_id_type=MESH)
        return carry

    tables = [
        pltpu.make_async_copy(source, target, load_sem.at[n])
        for n, (source, target) in enumerate(
            [
                (coeff_hbm, coeff_ref),
                (owner_hbm, owner_ref),
                (from_hbm, from_ref),
                (line_hbm, line_ref),
                (to_hbm, to_ref),
                (les_hbm, les_ref),
                (start_hbm, start_ref),
                (counts_hbm, counts_row),
                (rates_hbm, rates_ref),
                (frozen_hbm, frozen_ref),
            ]
        )
    ]
    load = pltpu.make_async_copy(lines_hbm, y_ref, load_sem.at[len(tables)])
    for copy in tables:
        copy.start()
    load.start()
    lax.fori_loop(1, groups, greet, 0)

    rims = []
    for axis in (0, 1):
        for move in (1, size[axis] - 1):
            there = list(at)
            there[axis] = lax.rem(at[axis] + move, size[axis])
            rims.append(tuple(there))

    def rim_copies(step):
        return [
            pltpu.make_async_remote_copy(
                src_ref=field_ref.at[step],
                dst_ref=rim_ref.at[step, k],
                send_sem=rim_send.at[step, k],
                recv_sem=rim_recv.at[step, k],
                device_id=rims[k],
                device_id_type=MESH,
            )
            for k in range(4)
        ]

    def aim_copy(j):
        peer, device = place(j)
        return pltpu.make_async_remote_copy(
            src_ref=aim_ref.at[(peer * slots) >> bits(points)],
            dst_ref=got_ref.at[me],
            send_sem=aim_send.at[j],
            recv_sem=aim_recv.at[j],
            device_id=device,
            device_id_type=MESH,
        )

    def turn_of(i, sign):
        low = (me + sign * i) & (half - 1)
        return jnp.where(i < half, me ^ half, me) & half | low

    def data_copy(step, wave, j):
        peer = turn_of(j, 1)
        device = (peer >> bits(size[1]), peer & (size[1] - 1))
        return pltpu.make_async_remote_copy(
            src_ref=send_ref.at[step, peer],
            dst_ref=recv_refs[step][wave].at[j - turns[wave][0]],
            send_sem=send_sem.at[step, j],
            recv_sem=recv_sem.at[step, j],
            device_id=device,
            device_id_type=MESH,
        )

    tables[0].wait()
    lane = iota((points, points), 1)
    row = iota((points, points), 0)
    for n in range(species):
        coeffs_ref[n : n + 1, :] = jnp.full((1, points), coeff_ref[n], f32)
    coeff = coeffs_ref[...]
    root = jnp.sqrt(4.0 * coeff + 1.0)
    theta = -jnp.log(2.0 * coeff / (2.0 * coeff + 1.0 + root))
    scale = 1.0 / (root * (1.0 - jnp.exp(-2.0 * points * theta)))
    along = iota((species, points), 1).astype(f32)
    apart_ref[...] = scale * (jnp.exp(-along * theta) + jnp.exp((along - 2.0 * points) * theta)) - relax_rate / points
    ends_ref[...] = scale * (jnp.exp(-(along + 1.0) * theta) + jnp.exp((along + 1.0 - 2.0 * points) * theta))
    apart = jnp.abs(lane - row)
    ends = jnp.minimum(lane + row, 2 * points - 2 - lane - row)

    def spread(ref, n, index):
        value = jnp.broadcast_to(ref[pl.ds(n, 1), :], (points, points))
        return jnp.take_along_axis(value, index, axis=1, mode="promise_in_bounds")

    def inverse(n, carry):
        top, rest = halves(spread(apart_ref, n, apart) + spread(ends_ref, n, ends))
        matrix_ref[n] = jnp.concatenate([top, rest], axis=1)
        return carry

    lax.fori_loop(0, species, inverse, 0, unroll=8)
    for copy in tables[1:]:
        copy.wait()
    field_ref[0] = les_ref[...].reshape(species, lines)


    for step in range(STEPS):
        owner = owner_ref[step : step + 1, :]
        rank = total_of(when((column(owner) == owner) & (row < lane), 1), 0)
        spot = column(owner * slots + rank)
        turn = (owner - me) & (half - 1)
        key = (jnp.where((owner ^ me) & half == 0, half, 0) + turn) * lines + iota((1, points), 1)
        spot_sorted = total_of(when(column(key) < key, 1), 0)
        first = step * (blocks + 2) + blocks
        tab_ref[first] = spot_sorted
        sorted_code = column(iota((1, points), 1) * 8 + counts_row[...])
        order = total_of(when(column(spot_sorted) == lane, sorted_code), 0)
        tab_ref[first + 1] = order
        order_ref[step] = jnp.broadcast_to(order >> 3, (species, points))
        turn = (SEG * (rank - from_ref[step : step + 1, :])) & (points - 1)
        code = column(spot_sorted * points + turn)
        aim = column(line_ref[step : step + 1, :] * segments + to_ref[step : step + 1, :] + 1)
        for b in range(blocks):
            hit = spot == lane + b * points
            tab_ref[step * (blocks + 2) + b] = total_of(when(hit, code), 0)
            aim_ref[b, step : step + 1, :] = total_of(when(hit, aim), 0)
    send_rows = STEPS * (blocks + 2)
    send_table = pltpu.make_async_copy(tab_ref.at[pl.ds(0, send_rows)], tab_smem.at[pl.ds(0, send_rows)], tab_sem.at[0])
    send_table.start()

    pl.semaphore_wait(barrier, groups - 1)
    for copy in rim_copies(0):
        copy.start()

    def aim_start(j, carry):
        aim_copy(j).start()
        return carry

    lax.fori_loop(1, groups, aim_start, 0)
    got_ref[me] = aim_ref[(me * slots) >> bits(points)]

    flat_y = y_ref.reshape(lines * species, points)
    flat_z = z_ref.reshape(lines * species, points)

    def diffuse(step):
        rel = lane - column(start_ref[step : step + 1, :])
        third = TRIP // 3
        source = jnp.where(
            rel < third,
            3 * rel,
            jnp.where(rel < 2 * third, 3 * (2 * third - 1 - rel) + 1, 3 * (rel - 2 * third) + 2),
        )
        index = jnp.where((rel >= 0) & (rel < TRIP), source + (lane - rel), lane)

        def one(s, carry):
            y = flat_y[pl.ds(s, lines, stride=species), :]
            y = jnp.take_along_axis(y, index, axis=1, mode="promise_in_bounds")
            right = matrix_ref[s]
            out = dot(jnp.concatenate(halves(y), axis=1), jnp.concatenate([right, right], axis=0))
            flat_z[pl.ds(s, lines, stride=species), :] = out[:, :points] + out[:, points:]
            return carry

        lax.fori_loop(0, species, one, 0, unroll=12)

    lane_s = lax.broadcasted_iota(i32, (species, points), 1)

    def middle(step):
        field = field_ref[step]
        up = jnp.where(at[0] > 0, rim_ref[step, 0], 0.0)
        down = jnp.where(at[0] < size[0] - 1, rim_ref[step, 1], 0.0)
        left = jnp.where(at[1] > 0, rim_ref[step, 2], 0.0)
        right = jnp.where(at[1] < size[1] - 1, rim_ref[step, 3], 0.0)
        before = pltpu.roll(jnp.where(lane_s == points - 1, left, field), 1, 1)
        after = pltpu.roll(jnp.where(lane_s == 0, right, field), points - 1, 1)
        mid_ref[...] = field + les_rate * (up + down + before + after - 4.0 * field)

    joint = jnp.dot(
        frozen_ref[...], rates_ref[...], precision=lax.Precision.HIGHEST, preferred_element_type=f32
    )
    joint_top, joint_rest = halves(joint)
    wide = (2 * species, 6 * species)
    place_c = iota(wide, 1)
    block_c = sum((place_c >= species * n).astype(i32) for n in range(1, 6))
    pick = jnp.where(
        iota((species, 6 * species), 0) == (place_c - species * block_c)[:species], 1.0, 0.0
    ).astype(bf16)
    twice_top = dot(jnp.concatenate([joint_top.astype(f32)] * 2, axis=0).astype(bf16), pick)
    twice_rest = dot(jnp.concatenate([joint_rest.astype(f32)] * 2, axis=0).astype(bf16), pick)
    entries = jnp.where((block_c >> 1) == 1, twice_rest, twice_top)
    matrix = jnp.where((iota(wide, 0) >= species).astype(i32) == (block_c & 1), entries, 0.0).astype(bf16)

    segment = lane_s // SEG

    def pack(step, peer):
        tile = jnp.zeros((species, points), f32)
        first = peer * slots
        for k in range(slots):
            code = tab_smem[step * (blocks + 2) + (first >> bits(points)), 0, (first & (points - 1)) + k]
            value = pltpu.roll(s_ref[code >> bits(points)], code & (points - 1), 1)
            tile = jnp.where(segment == k, value, tile)
        return tile

    def chemistry(step, base):
        orders = step * (blocks + 2) + blocks + 1
        mid = middle_ref[...]
        codes = [tab_smem[orders, 0, base + i] for i in range(CHUNK)]
        for sub in range(SUBSTEPS):
            for q in range(0, CHUNK, 4):
                columns = []
                state = []
                for h in (0, 2):
                    if sub == 0:
                        y = jnp.concatenate(
                            [
                                z_ref[codes[i] >> 3] + jnp.broadcast_to(mid[:, base + i : base + i + 1], (species, points))
                                for i in (q + h, q + h + 1)
                            ],
                            axis=0,
                        )
                    else:
                        y = s_ref[pl.ds(base + q + h, 2)].reshape(2 * species, points)
                    state.append(y)
                    top, rest = halves(jnp.tanh(y))
                    columns.append(jnp.concatenate([top, top, rest], axis=0))
                change = dot(matrix, jnp.concatenate(columns, axis=1))
                for h in (0, 1):
                    for k in (0, 1):
                        i = q + 2 * h + k
                        factor = jnp.where(codes[i] & 7 > sub, f32(1.0), f32(0.0))
                        rows = slice(k * species, (k + 1) * species)
                        s_ref[base + i] = state[h][rows] + factor * change[rows, h * points : (h + 1) * points]

    def exchange(step):
        middle_ref[...] = relax_rate * jnp.take_along_axis(
            mid_ref[...], order_ref[step], axis=1, mode="promise_in_bounds"
        )
        many = CHUNK // slots

        def wrap(i):
            peer = turn_of(i, 1)
            send_ref[step, peer] = pack(step, peer)

        for c in range(lines // CHUNK):
            chemistry(step, c * CHUNK)
            for n in range(many):
                wrap(c * many + n)
            for n in range(many):
                data_copy(step, 1 if c * many + n < half // 2 else 2, c * many + n).start()

        def near(i, carry):
            for n in range(2):
                wrap(half + 2 * i + n)
            for n in range(2):
                before = half + 2 * (i - 1) + n

                @pl.when(before > half)
                def _():
                    data_copy(step, 0, before).start()

            return carry

        lax.fori_loop(0, half // 2, near, 0)
        recv_refs[step][0][0] = send_ref[step, me]
        for n in range(groups - 2, groups):
            data_copy(step, 0, n).start()

    def arrivals():
        number = iota((total, 1), 0)
        lane_t = iota((total, points), 1)
        number_r = iota((1, total), 1)
        offset = (me * slots) & (points - 1)
        mine = offset + (iota((total, points), 0) & (slots - 1))
        for step in range(STEPS):
            for r in range(groups):
                flat_ref[r * slots : (r + 1) * slots, :] = jnp.broadcast_to(
                    got_ref[r, step : step + 1, :], (slots, points)
                )
            code = total_of(when(lane_t == mine, flat_ref[...]), 1)
            valid = code > 0
            code = code - 1
            line = jnp.where(valid, code >> bits(segments), lines)
            seg = code & (segments - 1)
            source = number >> bits(slots)
            deep = (me - source) & (half - 1)
            late = jnp.where((source ^ me) & half == 0, 0, jnp.where(deep >= half // 2, 2, 1))
            slot = jnp.where(late == 2, deep - half // 2, deep)
            line = line + late * (lines + 1)
            line_c = jnp.broadcast_to(line, (total, points))
            line_r = jnp.concatenate(
                [jnp.transpose(line_c[b * points : (b + 1) * points])[:1] for b in range(blocks)], axis=1
            )
            key_r = line_r * total + number_r
            key_c = line * total + number
            below = key_r < key_c
            position = total_of(when(below, 1), 1)
            same = total_of(when(below & (line_r == line), 1), 1)
            turn = (SEG * (seg - (number & (slots - 1)))) & (points - 1)
            value = slot * points + turn
            kind = seg * 2 + when(same == 0, 1)
            base = send_rows + step * (blocks + waves)
            for b in range(blocks):
                hit = position == lane_t + b * points
                tab_ref[base + b] = total_of(when(hit, value), 0)
                kinds = column(total_of(when(hit, kind), 0))
                at_b = pl.ds(b * points, points)
                mask_ref[step, at_b, :] = jnp.where((kinds >> 1) == (lane >> bits(SEG)), splice_weight, 0.0)
                keep_ref[step, at_b, :] = jnp.where((kinds & 1) == 1, 0.0, 1.0)
            starts = (0, total // 2, total // 2 + total // 4, total)
            in_c = jnp.zeros((total, points), jnp.bool_)
            in_r = jnp.zeros((lines, total), jnp.bool_)
            for w in range(waves):
                aim_c = lane_t + w * (lines + 1)
                upto = total_of(when(line_c <= aim_c, 1), 0)
                many = total_of(when(line_c == aim_c, 1), 0)
                tab_ref[base + blocks + w] = jnp.where(many > 0, upto - 1 - starts[w], starts[w + 1] - starts[w])
                in_c = in_c | (line_c == aim_c)
                in_r = in_r | (line_r == iota((lines, total), 0) + w * (lines + 1))
            lands = jnp.where(in_r, 1.0, 0.0).astype(bf16)
            covers = jnp.where(seg == (lane_t >> bits(SEG)), 1.0, 0.0).astype(bf16)
            weight_ref[step] = 1.0 - splice_weight * dot(lands, covers)
            into_ref[step] = jnp.where(in_c, splice_weight, 0.0)
        rows = STEPS * (blocks + waves)
        copy = pltpu.make_async_copy(
            tab_ref.at[pl.ds(send_rows, rows)], tab_smem.at[pl.ds(send_rows, rows)], tab_sem.at[1]
        )
        copy.start()
        copy.wait()

    def prepare(step):
        def rows(j, carry):
            block = jnp.broadcast_to(into_ref[step, pl.ds(j, 1), :], (SEG, lines))
            source = j >> bits(slots)
            first = jnp.where(source & half == me & half, half, 0) + ((me - source) & (half - 1))
            first = first * points + (j & (slots - 1)) * SEG
            fold_ref[pl.ds(pl.multiple_of(first, SEG), SEG), :] = block.astype(bf16)
            return carry

        if slots < segments:
            fold_ref[...] = jnp.zeros_like(fold_ref)
        lax.fori_loop(0, total, rows, 0, unroll=8)

        places = step * (blocks + 2) + blocks

        def scale(l, sums):
            value = s_ref[tab_smem[places, 0, l]] * weight_ref[step, pl.ds(l, 1), :]
            y_ref[l] = value
            return jnp.where(lane_s == l, jnp.sum(value, axis=1, keepdims=True), sums)

        return lax.fori_loop(0, lines, scale, jnp.zeros((species, points), f32), unroll=8)

    def collect(step, wave):
        def finish(j, carry):
            data_copy(step, wave, j).wait()
            return carry

        low, high = turns[wave]
        lax.fori_loop(low + (wave == 0), high, finish, 0)

    def filtered(step, wave):
        low, high = turns[wave]
        for i in range(low, high):
            value = recv_refs[step][wave][i - low]
            rest = value - value.astype(bf16).astype(f32)
            both_ref[:, i * points : (i + 1) * points] = jnp.concatenate([value, rest], axis=0).astype(bf16)
        acc = dot(both_ref[:, low * points : high * points], fold_ref[low * points : high * points, :])
        return acc[:species] + acc[species:]

    def run(step, wave, acc):
        base = send_rows + step * (blocks + waves)
        begin = sum(high - low for low, high in turns[:wave]) * slots
        end = begin + (turns[wave][1] - turns[wave][0]) * slots

        at_row = base + (begin >> bits(points))
        at_lane = begin & (points - 1)
        assert at_lane + end - begin <= points

        def one(i, acc):
            code = tab_smem[at_row, 0, at_lane + i]
            value = pltpu.roll(recv_refs[step][wave][code >> bits(points)], code & (points - 1), 1)
            acc = value * mask_ref[step, pl.ds(begin + i, 1), :] + acc * keep_ref[step, pl.ds(begin + i, 1), :]
            sums_refs[wave][i] = acc
            return acc

        sums_refs[wave][end - begin] = jnp.zeros((species, points), f32)
        lax.fori_loop(0, end - begin, one, jnp.zeros((species, points), f32), unroll=32)

    def receive(step, sums, les_done, out):
        base = send_rows + step * (blocks + waves)

        def settle(which):
            def one(l, carry):
                value = y_ref[l]
                for w in which:
                    value = value + sums_refs[w][tab_smem[base + blocks + w, 0, l]]
                y_ref[l] = value
                return carry

            return one

        for wave in range(waves):
            collect(step, wave)
            if wave + 1 < waves:
                run(step, wave, None)
            if wave + 2 == waves:
                lax.fori_loop(0, lines, settle(range(waves - 1)), 0, unroll=8)
                for copy in out[0]:
                    copy.start()
            if wave + 1 == waves:
                for copy in out[1]:
                    copy.start()
            sums = sums + filtered(step, wave)
        les_done(0.5 * mid_ref[...] + (0.5 / points) * sums)
        if not out[0]:
            run(step, waves - 1, None)
            lax.fori_loop(0, lines, settle((waves - 1,)), 0, unroll=32)

    load.wait()
    diffuse(0)
    for copy in rim_copies(0):
        copy.wait()
    middle(0)
    send_table.wait()
    exchange(0)

    def aim_finish(j, carry):
        aim_copy(j).wait()
        return carry

    lax.fori_loop(1, groups, aim_finish, 0)
    arrivals()
    sums = prepare(0)

    def again(field):
        field_ref[1] = field
        for copy in rim_copies(1):
            copy.start()

    receive(0, sums, again, ((), ()))
    diffuse(1)
    for copy in rim_copies(1):
        copy.wait()
    middle(1)
    exchange(1)
    sums = prepare(1)
    final = STEPS - 1
    begin = total - total // 4
    base = send_rows + final * (blocks + waves)
    pairs = [
        (mask_ref.at[final, pl.ds(begin, total - begin)], mask_out),
        (keep_ref.at[final, pl.ds(begin, total - begin)], keep_out),
        (tab_ref.at[base + (begin >> bits(points))], table_out.at[0]),
        (tab_ref.at[base + blocks + waves - 1], table_out.at[1]),
    ]
    for p in range(parts):
        at_p = pl.ds(p * lines // parts, lines // parts)
        pairs.append((y_ref.at[at_p], lines_out.at[at_p]))
    early = [pltpu.make_async_copy(a, b, out_sem.at[n]) for n, (a, b) in enumerate(pairs)]
    last = pltpu.make_async_copy(les_ref, les_out, out_sem.at[parts + 4])
    tiles = pltpu.make_async_copy(recv_refs[final][waves - 1], tiles_out, out_sem.at[parts + 5])

    def finish(field):
        les_ref[...] = field.reshape(species, 1, lines)
        last.start()

    receive(1, sums, finish, (early, [tiles]))
    for copy in early + [tiles, last]:
        copy.wait()


def deliver_kernel(
    les_in,
    lines_in,
    tiles_in,
    mask_in,
    keep_in,
    table_in,
    les_out,
    lines_out,
    les_ref,
    lines_ref,
    tiles_ref,
    mask_ref,
    keep_ref,
    table_ref,
    sums_ref,
    in_sem,
    out_sem,
):
    lines, species, points = lines_ref.shape
    parts = out_sem.shape[0] - 1
    size = lines // parts
    many = mask_ref.shape[0]
    small = [(table_in, table_ref), (tiles_in, tiles_ref), (mask_in, mask_ref), (keep_in, keep_ref), (les_in, les_ref)]
    at = [pl.ds(p * size, size) for p in range(parts)]
    takes = small + [(lines_in.at[a], lines_ref.at[a]) for a in at]
    takes = [pltpu.make_async_copy(a, b, in_sem.at[n]) for n, (a, b) in enumerate(takes)]
    gives = [(lines_ref.at[a], lines_out.at[a]) for a in at] + [(les_ref, les_out)]
    gives = [pltpu.make_async_copy(a, b, out_sem.at[n]) for n, (a, b) in enumerate(gives)]
    for take in takes:
        take.start()
    for take in takes[: len(small)]:
        take.wait()
    gives[parts].start()

    def run(i, acc):
        code = table_ref[0, 0, points - many + i]
        value = pltpu.roll(tiles_ref[code >> bits(points)], code & (points - 1), 1)
        acc = value * mask_ref[pl.ds(i, 1), :] + acc * keep_ref[pl.ds(i, 1), :]
        sums_ref[i] = acc
        return acc

    sums_ref[many] = jnp.zeros((species, points), f32)
    lax.fori_loop(0, many, run, jnp.zeros((species, points), f32), unroll=32)

    def settle(l, carry):
        lines_ref[l] = lines_ref[l] + sums_ref[table_ref[1, 0, l]]
        return carry

    for p in range(parts):
        takes[len(small) + p].wait()
        lax.fori_loop(p * size, (p + 1) * size, settle, 0, unroll=size)
        gives[p].start()
    for give in gives:
        give.wait()


def body(
    les,
    lines,
    triplet_start,
    splice_owner,
    splice_line,
    splice_from,
    splice_to,
    chem_counts,
    diffusivity,
    rates,
    frozen_inverse,
):
    groups = lax.axis_size("grid") * lax.axis_size("line")
    _, _, count, species, points = lines.shape
    segments = points // SEG
    slots = min(segments, max(2, 2 * count // groups))
    total = groups * slots
    blocks = total // points
    rows = STEPS * (2 * blocks + 2 + WAVES)

    dma = pltpu.SemaphoreType.DMA
    quarter = total // 4
    field, *rest = pl.pallas_call(
        functools.partial(kernel, slots),
        out_shape=(
            jax.ShapeDtypeStruct((species, 1, count), f32),
            jax.ShapeDtypeStruct((count, species, points), f32),
            jax.ShapeDtypeStruct((groups // 4, species, points), f32),
            jax.ShapeDtypeStruct((quarter, points), f32),
            jax.ShapeDtypeStruct((quarter, points), f32),
            jax.ShapeDtypeStruct((2, 1, points), i32),
        ),
        in_specs=[HBM] * 11,
        out_specs=(HBM,) * 6,
        scratch_shapes=[
            pltpu.VMEM((species, 1, count), f32),
            *[pltpu.VMEM((STEPS, count), i32)] * 5,
            pltpu.VMEM((species, species), f32),
            pltpu.VMEM((species, species), f32),
            pltpu.SMEM((species,), f32),
            pltpu.VMEM((1, count), i32),
            *[pltpu.VMEM((species, points), f32)] * 3,
            pltpu.VMEM((count, species, points), f32),
            pltpu.VMEM((count, species, points), f32),
            pltpu.VMEM((count, species, points), f32),
            pltpu.VMEM((STEPS, species, count), i32),
            pltpu.VMEM((species, points, 2 * points), bf16),
            pltpu.VMEM((STEPS, groups, species, points), f32),
            *[
                pltpu.VMEM((groups // part, species, points), f32)
                for part in (2, 4, 4) * STEPS
            ],
            pltpu.VMEM((total // 2 + 1, species, points), f32),
            *[pltpu.VMEM((total // 4 + 1, species, points), f32)] * 2,
            pltpu.VMEM((STEPS, total, points), f32),
            pltpu.VMEM((STEPS, total, points), f32),
            pltpu.VMEM((STEPS, total, count), f32),
            pltpu.VMEM((groups * points, count), bf16),
            pltpu.VMEM((2 * species, groups * points), bf16),
            pltpu.VMEM((STEPS, count, points), f32),
            pltpu.VMEM((STEPS, 4, species, count), f32),
            pltpu.VMEM((STEPS, species, count), f32),
            pltpu.VMEM((species, count), f32),
            pltpu.VMEM((species, count), f32),
            pltpu.VMEM((blocks, STEPS, points), i32),
            pltpu.VMEM((groups, STEPS, points), i32),
            pltpu.VMEM((total, points), i32),
            pltpu.VMEM((rows, 1, points), i32),
            pltpu.SMEM((rows, 1, points), i32),
            dma((11,)),
            dma((2,)),
            dma((STEPS, 4)),
            dma((STEPS, 4)),
            dma((groups,)),
            dma((groups,)),
            dma((STEPS, groups)),
            dma((STEPS, groups)),
            dma((10,)),
        ],
        compiler_params=pltpu.CompilerParams(
            collective_id=0, has_side_effects=True, vmem_limit_bytes=67043328
        ),
        name="steps",
    )(
        les.reshape(species, 1, count),
        lines.reshape(count, species, points),
        triplet_start.reshape(STEPS, count),
        splice_owner.reshape(STEPS, count),
        splice_line.reshape(STEPS, count),
        splice_from.reshape(STEPS, count),
        splice_to.reshape(STEPS, count),
        rates,
        frozen_inverse,
        diffusivity,
        chem_counts.reshape(1, count),
    )
    field, state = pl.pallas_call(
        deliver_kernel,
        out_shape=(
            jax.ShapeDtypeStruct(field.shape, f32),
            jax.ShapeDtypeStruct((count, species, points), f32),
        ),
        in_specs=[HBM] * 6,
        out_specs=(HBM, HBM),
        scratch_shapes=[
            pltpu.VMEM(field.shape, f32),
            pltpu.VMEM((count, species, points), f32),
            pltpu.VMEM((groups // 4, species, points), f32),
            pltpu.VMEM((quarter, points), f32),
            pltpu.VMEM((quarter, points), f32),
            pltpu.SMEM((2, 1, points), i32),
            pltpu.VMEM((quarter + 1, species, points), f32),
            dma((13,)),
            dma((9,)),
        ],
        compiler_params=pltpu.CompilerParams(vmem_limit_bytes=67043328),
        name="deliver",
    )(field, *rest)
    return (field.reshape(les.shape), state.reshape(lines.shape))


def solution(mesh):
    in_specs = (
        P(None, "grid", "line"),
        P("grid", "line", None, None, None),
        P(None, "grid", "line", None),
        P(None, "grid", "line", None, None),
        P(None, "grid", "line", None),
        P(None, "grid", "line", None),
        P(None, "grid", "line", None),
        P("grid", "line", None),
        P(),
        P(),
        P(),
    )
    out_specs = (P(None, "grid", "line"), P("grid", "line", None, None, None))
    return jax.shard_map(body, mesh=mesh, in_specs=in_specs, out_specs=out_specs, check_vma=False)
```

```python
import functools

import jax
import jax.numpy as jnp
from jax import lax
from jax.experimental import pallas as pl
from jax.experimental.pallas import tpu as pltpu
from jax.sharding import PartitionSpec as P

SEG = 16
TRIP = 48
STEPS = 2
SUBSTEPS = 6
WAVES = 3
CHUNK = 64

les_rate = 0.2
relax_rate = 0.5
splice_weight = 0.5

NAMES = ("grid", "line")
MESH = pl.DeviceIdType.MESH
VMEM = pl.BlockSpec(memory_space=pltpu.VMEM)
SMEM = pl.BlockSpec(memory_space=pltpu.SMEM)
HBM = pl.BlockSpec(memory_space=pltpu.HBM)
f32 = jnp.float32
bf16 = jnp.bfloat16
i32 = jnp.int32

dot = functools.partial(jnp.dot, preferred_element_type=jnp.float32)


def halves(value):
    top = value.astype(bf16)
    return top, (value - top.astype(f32)).astype(bf16)


def column(row):
    points = row.shape[1]
    return jnp.transpose(jnp.broadcast_to(row, (points, points)))


def iota(shape, axis):
    return lax.broadcasted_iota(i32, shape, axis)


def bits(size):
    assert size & (size - 1) == 0
    return size.bit_length() - 1


def when(condition, value):
    return jnp.where(condition, value, 0)


def total_of(value, axis):
    return jnp.sum(value, axis=axis, keepdims=True, dtype=i32)


def kernel(
    slots,
    les_hbm,
    lines_hbm,
    start_hbm,
    owner_hbm,
    line_hbm,
    from_hbm,
    to_hbm,
    rates_hbm,
    frozen_hbm,
    coeff_hbm,
    counts_hbm,
    les_out,
    lines_out,
    tiles_out,
    mask_out,
    keep_out,
    table_out,
    les_ref,
    start_ref,
    owner_ref,
    line_ref,
    from_ref,
    to_ref,
    rates_ref,
    frozen_ref,
    coeff_ref,
    counts_row,
    coeffs_ref,
    apart_ref,
    ends_ref,
    y_ref,
    z_ref,
    s_ref,
    order_ref,
    matrix_ref,
    send_ref,
    recv_00,
    recv_01,
    recv_02,
    recv_10,
    recv_11,
    recv_12,
    sums_0,
    sums_1,
    sums_2,
    mask_ref,
    keep_ref,
    into_ref,
    fold_ref,
    both_ref,
    weight_ref,
    rim_ref,
    field_ref,
    mid_ref,
    middle_ref,
    aim_ref,
    got_ref,
    flat_ref,
    tab_ref,
    tab_smem,
    load_sem,
    tab_sem,
    rim_send,
    rim_recv,
    aim_send,
    aim_recv,
    send_sem,
    recv_sem,
    out_sem,
):
    parts = out_sem.shape[0] - 6
    waves = WAVES
    species, _, lines = les_ref.shape
    points = y_ref.shape[2]
    segments = points // SEG
    size = [lax.axis_size(n) for n in NAMES]
    at = [lax.axis_index(n) for n in NAMES]
    groups = size[0] * size[1]
    me = at[0] * size[1] + at[1]
    total = groups * slots
    blocks = total // points
    recv_refs = ((recv_00, recv_01, recv_02), (recv_10, recv_11, recv_12))
    sums_refs = (sums_0, sums_1, sums_2)

    def place(j):
        peer = (me + j) & (groups - 1)
        return peer, (peer >> bits(size[1]), peer & (size[1] - 1))

    half = groups // 2
    turns = ((half, groups), (0, half // 2), (half // 2, half))
    barrier = pltpu.get_barrier_semaphore()

    def greet(j, carry):
        pl.semaphore_signal(barrier, inc=1, device_id=place(j)[1], device_id_type=MESH)
        return carry

    tables = [
        pltpu.make_async_copy(source, target, load_sem.at[n])
        for n, (source, target) in enumerate(
            [
                (coeff_hbm, coeff_ref),
                (owner_hbm, owner_ref),
                (from_hbm, from_ref),
                (line_hbm, line_ref),
                (to_hbm, to_ref),
                (les_hbm, les_ref),
                (start_hbm, start_ref),
                (counts_hbm, counts_row),
                (rates_hbm, rates_ref),
                (frozen_hbm, frozen_ref),
            ]
        )
    ]
    load = pltpu.make_async_copy(lines_hbm, y_ref, load_sem.at[len(tables)])
    for copy in tables:
        copy.start()
    load.start()
    rim_ref[...] = jnp.zeros_like(rim_ref)
    lax.fori_loop(1, groups, greet, 0)

    rims = []
    for axis in (0, 1):
        for move in (1, size[axis] - 1):
            there = list(at)
            there[axis] = lax.rem(at[axis] + move, size[axis])
            rims.append(tuple(there))

    def rim_copies(step):
        return [
            pltpu.make_async_remote_copy(
                src_ref=field_ref.at[step],
                dst_ref=rim_ref.at[step, k],
                send_sem=rim_send.at[step, k],
                recv_sem=rim_recv.at[step, k],
                device_id=rims[k],
                device_id_type=MESH,
            )
            for k in range(4)
        ]

    inner = [at[0] < size[0] - 1, at[0] > 0, at[1] < size[1] - 1, at[1] > 0]

    def rim_start(step):
        for k, copy in enumerate(rim_copies(step)):
            pl.when(inner[k])(copy.start)

    def rim_wait(step):
        for k, copy in enumerate(rim_copies(step)):
            pl.when(inner[k])(copy.wait_send)
            pl.when(inner[k ^ 1])(copy.wait_recv)

    def aim_copy(j):
        peer, device = place(j)
        return pltpu.make_async_remote_copy(
            src_ref=aim_ref.at[(peer * slots) >> bits(points)],
            dst_ref=got_ref.at[me],
            send_sem=aim_send.at[j],
            recv_sem=aim_recv.at[j],
            device_id=device,
            device_id_type=MESH,
        )

    def turn_of(i, sign):
        low = (me + sign * i) & (half - 1)
        return jnp.where(i < half, me ^ half, me) & half | low

    def data_copy(step, wave, j):
        peer = turn_of(j, 1)
        device = (peer >> bits(size[1]), peer & (size[1] - 1))
        return pltpu.make_async_remote_copy(
            src_ref=send_ref.at[step, peer],
            dst_ref=recv_refs[step][wave].at[j - turns[wave][0]],
            send_sem=send_sem.at[step, j],
            recv_sem=recv_sem.at[step, j],
            device_id=device,
            device_id_type=MESH,
        )

    tables[0].wait()
    lane = iota((points, points), 1)
    row = iota((points, points), 0)
    for n in range(species):
        coeffs_ref[n : n + 1, :] = jnp.full((1, points), coeff_ref[n], f32)
    coeff = coeffs_ref[...]
    root = jnp.sqrt(4.0 * coeff + 1.0)
    theta = -jnp.log(2.0 * coeff / (2.0 * coeff + 1.0 + root))
    scale = 1.0 / (root * (1.0 - jnp.exp(-2.0 * points * theta)))
    along = iota((species, points), 1).astype(f32)
    apart_ref[...] = scale * (jnp.exp(-along * theta) + jnp.exp((along - 2.0 * points) * theta)) - relax_rate / points
    ends_ref[...] = scale * (jnp.exp(-(along + 1.0) * theta) + jnp.exp((along + 1.0 - 2.0 * points) * theta))
    apart = jnp.abs(lane - row)
    ends = jnp.minimum(lane + row, 2 * points - 2 - lane - row)

    def spread(ref, n, index):
        value = jnp.broadcast_to(ref[pl.ds(n, 1), :], (points, points))
        return jnp.take_along_axis(value, index, axis=1, mode="promise_in_bounds")

    def inverse(n, carry):
        top, rest = halves(spread(apart_ref, n, apart) + spread(ends_ref, n, ends))
        matrix_ref[n] = jnp.concatenate([top, rest], axis=1)
        return carry

    lax.fori_loop(0, species, inverse, 0, unroll=8)
    for copy in tables[1:]:
        copy.wait()
    field_ref[0] = les_ref[...].reshape(species, lines)
    pl.semaphore_wait(barrier, groups - 1)
    rim_start(0)


    for step in range(STEPS):
        owner = owner_ref[step : step + 1, :]
        rank = total_of(when((column(owner) == owner) & (row < lane), 1), 0)
        spot = column(owner * slots + rank)
        turn = (owner - me) & (half - 1)
        key = (jnp.where((owner ^ me) & half == 0, half, 0) + turn) * lines + iota((1, points), 1)
        spot_sorted = total_of(when(column(key) < key, 1), 0)
        first = step * (blocks + 2) + blocks
        tab_ref[first] = spot_sorted
        sorted_code = column(iota((1, points), 1) * 8 + counts_row[...])
        order = total_of(when(column(spot_sorted) == lane, sorted_code), 0)
        tab_ref[first + 1] = order
        order_ref[step] = jnp.broadcast_to(order >> 3, (species, points))
        turn = (SEG * (rank - from_ref[step : step + 1, :])) & (points - 1)
        code = column(spot_sorted * points + turn)
        aim = column(line_ref[step : step + 1, :] * segments + to_ref[step : step + 1, :] + 1)
        for b in range(blocks):
            hit = spot == lane + b * points
            tab_ref[step * (blocks + 2) + b] = total_of(when(hit, code), 0)
            aim_ref[b, step : step + 1, :] = total_of(when(hit, aim), 0)
    send_rows = STEPS * (blocks + 2)
    send_table = pltpu.make_async_copy(tab_ref.at[pl.ds(0, send_rows)], tab_smem.at[pl.ds(0, send_rows)], tab_sem.at[0])
    send_table.start()


    def aim_start(j, carry):
        aim_copy(j).start()
        return carry

    lax.fori_loop(1, groups, aim_start, 0)
    got_ref[me] = aim_ref[(me * slots) >> bits(points)]

    flat_y = y_ref.reshape(lines * species, points)
    flat_z = z_ref.reshape(lines * species, points)

    def diffuse(step):
        rel = lane - column(start_ref[step : step + 1, :])
        third = TRIP // 3
        source = jnp.where(
            rel < third,
            3 * rel,
            jnp.where(rel < 2 * third, 3 * (2 * third - 1 - rel) + 1, 3 * (rel - 2 * third) + 2),
        )
        index = jnp.where((rel >= 0) & (rel < TRIP), source + (lane - rel), lane)

        def one(s, carry):
            y = flat_y[pl.ds(s, lines, stride=species), :]
            y = jnp.take_along_axis(y, index, axis=1, mode="promise_in_bounds")
            right = matrix_ref[s]
            out = dot(jnp.concatenate(halves(y), axis=1), jnp.concatenate([right, right], axis=0))
            flat_z[pl.ds(s, lines, stride=species), :] = out[:, :points] + out[:, points:]
            return carry

        lax.fori_loop(0, species, one, 0, unroll=12)

    lane_s = lax.broadcasted_iota(i32, (species, points), 1)

    def middle(step):
        field = field_ref[step]
        up, down, left, right = (rim_ref[step, k] for k in range(4))
        before = pltpu.roll(jnp.where(lane_s == points - 1, left, field), 1, 1)
        after = pltpu.roll(jnp.where(lane_s == 0, right, field), points - 1, 1)
        mid_ref[...] = field + les_rate * (up + down + before + after - 4.0 * field)

    joint = jnp.dot(
        frozen_ref[...], rates_ref[...], precision=lax.Precision.HIGHEST, preferred_element_type=f32
    )
    joint_top, joint_rest = halves(joint)
    wide = (2 * species, 6 * species)
    place_c = iota(wide, 1)
    block_c = sum((place_c >= species * n).astype(i32) for n in range(1, 6))
    pick = jnp.where(
        iota((species, 6 * species), 0) == (place_c - species * block_c)[:species], 1.0, 0.0
    ).astype(bf16)
    twice_top = dot(jnp.concatenate([joint_top.astype(f32)] * 2, axis=0).astype(bf16), pick)
    twice_rest = dot(jnp.concatenate([joint_rest.astype(f32)] * 2, axis=0).astype(bf16), pick)
    entries = jnp.where((block_c >> 1) == 1, twice_rest, twice_top)
    matrix = jnp.where((iota(wide, 0) >= species).astype(i32) == (block_c & 1), entries, 0.0).astype(bf16)

    segment = lane_s // SEG

    def pack(step, peer):
        tile = jnp.zeros((species, points), f32)
        first = peer * slots
        for k in range(slots):
            code = tab_smem[step * (blocks + 2) + (first >> bits(points)), 0, (first & (points - 1)) + k]
            value = pltpu.roll(s_ref[code >> bits(points)], code & (points - 1), 1)
            tile = jnp.where(segment == k, value, tile)
        return tile

    def chemistry(step, base):
        orders = step * (blocks + 2) + blocks + 1
        mid = middle_ref[...]
        codes = [tab_smem[orders, 0, base + i] for i in range(CHUNK)]
        for sub in range(SUBSTEPS):
            for q in range(0, CHUNK, 4):
                columns = []
                state = []
                for h in (0, 2):
                    if sub == 0:
                        y = jnp.concatenate(
                            [
                                z_ref[codes[i] >> 3] + jnp.broadcast_to(mid[:, base + i : base + i + 1], (species, points))
                                for i in (q + h, q + h + 1)
                            ],
                            axis=0,
                        )
                    else:
                        y = s_ref[pl.ds(base + q + h, 2)].reshape(2 * species, points)
                    state.append(y)
                    top, rest = halves(jnp.tanh(y))
                    columns.append(jnp.concatenate([top, top, rest], axis=0))
                change = dot(matrix, jnp.concatenate(columns, axis=1))
                for h in (0, 1):
                    for k in (0, 1):
                        i = q + 2 * h + k
                        factor = jnp.where(codes[i] & 7 > sub, f32(1.0), f32(0.0))
                        rows = slice(k * species, (k + 1) * species)
                        s_ref[base + i] = state[h][rows] + factor * change[rows, h * points : (h + 1) * points]

    def exchange(step):
        middle_ref[...] = relax_rate * jnp.take_along_axis(
            mid_ref[...], order_ref[step], axis=1, mode="promise_in_bounds"
        )
        many = CHUNK // slots

        def wrap(i):
            peer = turn_of(i, 1)
            send_ref[step, peer] = pack(step, peer)

        for c in range(lines // CHUNK):
            chemistry(step, c * CHUNK)
            for n in range(many):
                wrap(c * many + n)
            for n in range(many):
                data_copy(step, 1 if c * many + n < half // 2 else 2, c * many + n).start()

        def near(i, carry):
            for n in range(2):
                wrap(half + 2 * i + n)
            for n in range(2):
                before = half + 2 * (i - 1) + n

                @pl.when(before > half)
                def _():
                    data_copy(step, 0, before).start()

            return carry

        lax.fori_loop(0, half // 2, near, 0)
        recv_refs[step][0][0] = send_ref[step, me]
        for n in range(groups - 2, groups):
            data_copy(step, 0, n).start()

    def arrivals():
        number = iota((total, 1), 0)
        lane_t = iota((total, points), 1)
        number_r = iota((1, total), 1)
        offset = (me * slots) & (points - 1)
        mine = offset + (iota((total, points), 0) & (slots - 1))
        for step in range(STEPS):
            for r in range(groups):
                flat_ref[r * slots : (r + 1) * slots, :] = jnp.broadcast_to(
                    got_ref[r, step : step + 1, :], (slots, points)
                )
            code = total_of(when(lane_t == mine, flat_ref[...]), 1)
            valid = code > 0
            code = code - 1
            line = jnp.where(valid, code >> bits(segments), lines)
            seg = code & (segments - 1)
            source = number >> bits(slots)
            deep = (me - source) & (half - 1)
            late = jnp.where((source ^ me) & half == 0, 0, jnp.where(deep >= half // 2, 2, 1))
            slot = jnp.where(late == 2, deep - half // 2, deep)
            line = line + late * (lines + 1)
            line_c = jnp.broadcast_to(line, (total, points))
            line_r = jnp.concatenate(
                [jnp.transpose(line_c[b * points : (b + 1) * points])[:1] for b in range(blocks)], axis=1
            )
            key_r = line_r * total + number_r
            key_c = line * total + number
            below = key_r < key_c
            position = total_of(when(below, 1), 1)
            same = total_of(when(below & (line_r == line), 1), 1)
            turn = (SEG * (seg - (number & (slots - 1)))) & (points - 1)
            value = slot * points + turn
            kind = seg * 2 + when(same == 0, 1)
            base = send_rows + step * (blocks + waves)
            for b in range(blocks):
                hit = position == lane_t + b * points
                tab_ref[base + b] = total_of(when(hit, value), 0)
                kinds = column(total_of(when(hit, kind), 0))
                at_b = pl.ds(b * points, points)
                mask_ref[step, at_b, :] = jnp.where((kinds >> 1) == (lane >> bits(SEG)), splice_weight, 0.0)
                keep_ref[step, at_b, :] = jnp.where((kinds & 1) == 1, 0.0, 1.0)
            starts = (0, total // 2, total // 2 + total // 4, total)
            in_c = jnp.zeros((total, points), jnp.bool_)
            in_r = jnp.zeros((lines, total), jnp.bool_)
            for w in range(waves):
                aim_c = lane_t + w * (lines + 1)
                upto = total_of(when(line_c <= aim_c, 1), 0)
                many = total_of(when(line_c == aim_c, 1), 0)
                tab_ref[base + blocks + w] = jnp.where(many > 0, upto - 1 - starts[w], starts[w + 1] - starts[w])
                in_c = in_c | (line_c == aim_c)
                in_r = in_r | (line_r == iota((lines, total), 0) + w * (lines + 1))
            lands = jnp.where(in_r, 1.0, 0.0).astype(bf16)
            covers = jnp.where(seg == (lane_t >> bits(SEG)), 1.0, 0.0).astype(bf16)
            weight_ref[step] = 1.0 - splice_weight * dot(lands, covers)
            into_ref[step] = jnp.where(in_c, splice_weight, 0.0)
        rows = STEPS * (blocks + waves)
        copy = pltpu.make_async_copy(
            tab_ref.at[pl.ds(send_rows, rows)], tab_smem.at[pl.ds(send_rows, rows)], tab_sem.at[1]
        )
        copy.start()
        copy.wait()

    def prepare(step):
        def rows(j, carry):
            block = jnp.broadcast_to(into_ref[step, pl.ds(j, 1), :], (SEG, lines))
            source = j >> bits(slots)
            first = jnp.where(source & half == me & half, half, 0) + ((me - source) & (half - 1))
            first = first * points + (j & (slots - 1)) * SEG
            fold_ref[pl.ds(pl.multiple_of(first, SEG), SEG), :] = block.astype(bf16)
            return carry

        if slots < segments:
            fold_ref[...] = jnp.zeros_like(fold_ref)
        lax.fori_loop(0, total, rows, 0, unroll=8)

        places = step * (blocks + 2) + blocks

        def scale(l, sums):
            value = s_ref[tab_smem[places, 0, l]] * weight_ref[step, pl.ds(l, 1), :]
            y_ref[l] = value
            return jnp.where(lane_s == l, jnp.sum(value, axis=1, keepdims=True), sums)

        return lax.fori_loop(0, lines, scale, jnp.zeros((species, points), f32), unroll=8)

    def collect(step, wave):
        def finish(j, carry):
            data_copy(step, wave, j).wait()
            return carry

        low, high = turns[wave]
        lax.fori_loop(low + (wave == 0), high, finish, 0)

    def filtered(step, wave):
        low, high = turns[wave]
        for i in range(low, high):
            value = recv_refs[step][wave][i - low]
            rest = value - value.astype(bf16).astype(f32)
            both_ref[:, i * points : (i + 1) * points] = jnp.concatenate([value, rest], axis=0).astype(bf16)
        acc = dot(both_ref[:, low * points : high * points], fold_ref[low * points : high * points, :])
        return acc[:species] + acc[species:]

    def run(step, wave, acc):
        base = send_rows + step * (blocks + waves)
        begin = sum(high - low for low, high in turns[:wave]) * slots
        end = begin + (turns[wave][1] - turns[wave][0]) * slots

        at_row = base + (begin >> bits(points))
        at_lane = begin & (points - 1)
        assert at_lane + end - begin <= points

        def one(i, acc):
            code = tab_smem[at_row, 0, at_lane + i]
            value = pltpu.roll(recv_refs[step][wave][code >> bits(points)], code & (points - 1), 1)
            acc = value * mask_ref[step, pl.ds(begin + i, 1), :] + acc * keep_ref[step, pl.ds(begin + i, 1), :]
            sums_refs[wave][i] = acc
            return acc

        sums_refs[wave][end - begin] = jnp.zeros((species, points), f32)
        lax.fori_loop(0, end - begin, one, jnp.zeros((species, points), f32), unroll=32)

    def receive(step, sums, les_done, out):
        base = send_rows + step * (blocks + waves)

        def settle(which):
            def one(l, carry):
                value = y_ref[l]
                for w in which:
                    value = value + sums_refs[w][tab_smem[base + blocks + w, 0, l]]
                y_ref[l] = value
                return carry

            return one

        for wave in range(waves):
            collect(step, wave)
            if wave + 1 < waves:
                run(step, wave, None)
            if wave + 2 == waves:
                lax.fori_loop(0, lines, settle(range(waves - 1)), 0, unroll=8)
                for copy in out[0]:
                    copy.start()
            if wave + 1 == waves:
                for copy in out[1]:
                    copy.start()
            sums = sums + filtered(step, wave)
        les_done(0.5 * mid_ref[...] + (0.5 / points) * sums)
        if not out[0]:
            run(step, waves - 1, None)
            lax.fori_loop(0, lines, settle((waves - 1,)), 0, unroll=32)

    load.wait()
    diffuse(0)
    rim_wait(0)
    middle(0)
    send_table.wait()
    exchange(0)

    def aim_finish(j, carry):
        aim_copy(j).wait()
        return carry

    lax.fori_loop(1, groups, aim_finish, 0)
    arrivals()
    sums = prepare(0)

    def again(field):
        field_ref[1] = field
        rim_start(1)

    receive(0, sums, again, ((), ()))
    diffuse(1)
    rim_wait(1)
    middle(1)
    exchange(1)
    sums = prepare(1)
    final = STEPS - 1
    begin = total - total // 4
    base = send_rows + final * (blocks + waves)
    pairs = [
        (mask_ref.at[final, pl.ds(begin, total - begin)], mask_out),
        (keep_ref.at[final, pl.ds(begin, total - begin)], keep_out),
        (tab_ref.at[base + (begin >> bits(points))], table_out.at[0]),
        (tab_ref.at[base + blocks + waves - 1], table_out.at[1]),
    ]
    for p in range(parts):
        at_p = pl.ds(p * lines // parts, lines // parts)
        pairs.append((y_ref.at[at_p], lines_out.at[at_p]))
    early = [pltpu.make_async_copy(a, b, out_sem.at[n]) for n, (a, b) in enumerate(pairs)]
    last = pltpu.make_async_copy(les_ref, les_out, out_sem.at[parts + 4])
    tiles = pltpu.make_async_copy(recv_refs[final][waves - 1], tiles_out, out_sem.at[parts + 5])

    def finish(field):
        les_ref[...] = field.reshape(species, 1, lines)
        last.start()

    receive(1, sums, finish, (early, [tiles]))
    for copy in early + [tiles, last]:
        copy.wait()


def deliver_kernel(
    les_in,
    lines_in,
    tiles_in,
    mask_in,
    keep_in,
    table_in,
    les_out,
    lines_out,
    les_ref,
    lines_ref,
    tiles_ref,
    mask_ref,
    keep_ref,
    table_ref,
    sums_ref,
    in_sem,
    out_sem,
):
    lines, species, points = lines_ref.shape
    parts = out_sem.shape[0] - 1
    size = lines // parts
    many = mask_ref.shape[0]
    small = [(table_in, table_ref), (tiles_in, tiles_ref), (mask_in, mask_ref), (keep_in, keep_ref), (les_in, les_ref)]
    at = [pl.ds(p * size, size) for p in range(parts)]
    takes = small + [(lines_in.at[a], lines_ref.at[a]) for a in at]
    takes = [pltpu.make_async_copy(a, b, in_sem.at[n]) for n, (a, b) in enumerate(takes)]
    gives = [(lines_ref.at[a], lines_out.at[a]) for a in at] + [(les_ref, les_out)]
    gives = [pltpu.make_async_copy(a, b, out_sem.at[n]) for n, (a, b) in enumerate(gives)]
    for take in takes:
        take.start()
    for take in takes[: len(small)]:
        take.wait()
    gives[parts].start()

    def run(i, acc):
        code = table_ref[0, 0, points - many + i]
        value = pltpu.roll(tiles_ref[code >> bits(points)], code & (points - 1), 1)
        acc = value * mask_ref[pl.ds(i, 1), :] + acc * keep_ref[pl.ds(i, 1), :]
        sums_ref[i] = acc
        return acc

    sums_ref[many] = jnp.zeros((species, points), f32)
    lax.fori_loop(0, many, run, jnp.zeros((species, points), f32), unroll=32)

    def settle(l, carry):
        lines_ref[l] = lines_ref[l] + sums_ref[table_ref[1, 0, l]]
        return carry

    for p in range(parts):
        takes[len(small) + p].wait()
        lax.fori_loop(p * size, (p + 1) * size, settle, 0, unroll=size)
        gives[p].start()
    for give in gives:
        give.wait()


def body(
    les,
    lines,
    triplet_start,
    splice_owner,
    splice_line,
    splice_from,
    splice_to,
    chem_counts,
    diffusivity,
    rates,
    frozen_inverse,
):
    groups = lax.axis_size("grid") * lax.axis_size("line")
    _, _, count, species, points = lines.shape
    segments = points // SEG
    slots = min(segments, max(2, 2 * count // groups))
    total = groups * slots
    blocks = total // points
    rows = STEPS * (2 * blocks + 2 + WAVES)

    dma = pltpu.SemaphoreType.DMA
    quarter = total // 4
    field, *rest = pl.pallas_call(
        functools.partial(kernel, slots),
        out_shape=(
            jax.ShapeDtypeStruct((species, 1, count), f32),
            jax.ShapeDtypeStruct((count, species, points), f32),
            jax.ShapeDtypeStruct((groups // 4, species, points), f32),
            jax.ShapeDtypeStruct((quarter, points), f32),
            jax.ShapeDtypeStruct((quarter, points), f32),
            jax.ShapeDtypeStruct((2, 1, points), i32),
        ),
        in_specs=[HBM] * 11,
        out_specs=(HBM,) * 6,
        scratch_shapes=[
            pltpu.VMEM((species, 1, count), f32),
            *[pltpu.VMEM((STEPS, count), i32)] * 5,
            pltpu.VMEM((species, species), f32),
            pltpu.VMEM((species, species), f32),
            pltpu.SMEM((species,), f32),
            pltpu.VMEM((1, count), i32),
            *[pltpu.VMEM((species, points), f32)] * 3,
            pltpu.VMEM((count, species, points), f32),
            pltpu.VMEM((count, species, points), f32),
            pltpu.VMEM((count, species, points), f32),
            pltpu.VMEM((STEPS, species, count), i32),
            pltpu.VMEM((species, points, 2 * points), bf16),
            pltpu.VMEM((STEPS, groups, species, points), f32),
            *[
                pltpu.VMEM((groups // part, species, points), f32)
                for part in (2, 4, 4) * STEPS
            ],
            pltpu.VMEM((total // 2 + 1, species, points), f32),
            *[pltpu.VMEM((total // 4 + 1, species, points), f32)] * 2,
            pltpu.VMEM((STEPS, total, points), f32),
            pltpu.VMEM((STEPS, total, points), f32),
            pltpu.VMEM((STEPS, total, count), f32),
            pltpu.VMEM((groups * points, count), bf16),
            pltpu.VMEM((2 * species, groups * points), bf16),
            pltpu.VMEM((STEPS, count, points), f32),
            pltpu.VMEM((STEPS, 4, species, count), f32),
            pltpu.VMEM((STEPS, species, count), f32),
            pltpu.VMEM((species, count), f32),
            pltpu.VMEM((species, count), f32),
            pltpu.VMEM((blocks, STEPS, points), i32),
            pltpu.VMEM((groups, STEPS, points), i32),
            pltpu.VMEM((total, points), i32),
            pltpu.VMEM((rows, 1, points), i32),
            pltpu.SMEM((rows, 1, points), i32),
            dma((11,)),
            dma((2,)),
            dma((STEPS, 4)),
            dma((STEPS, 4)),
            dma((groups,)),
            dma((groups,)),
            dma((STEPS, groups)),
            dma((STEPS, groups)),
            dma((10,)),
        ],
        compiler_params=pltpu.CompilerParams(
            collective_id=0, has_side_effects=True, vmem_limit_bytes=67043328
        ),
        name="steps",
    )(
        les.reshape(species, 1, count),
        lines.reshape(count, species, points),
        triplet_start.reshape(STEPS, count),
        splice_owner.reshape(STEPS, count),
        splice_line.reshape(STEPS, count),
        splice_from.reshape(STEPS, count),
        splice_to.reshape(STEPS, count),
        rates,
        frozen_inverse,
        diffusivity,
        chem_counts.reshape(1, count),
    )
    field, state = pl.pallas_call(
        deliver_kernel,
        out_shape=(
            jax.ShapeDtypeStruct(field.shape, f32),
            jax.ShapeDtypeStruct((count, species, points), f32),
        ),
        in_specs=[HBM] * 6,
        out_specs=(HBM, HBM),
        scratch_shapes=[
            pltpu.VMEM(field.shape, f32),
            pltpu.VMEM((count, species, points), f32),
            pltpu.VMEM((groups // 4, species, points), f32),
            pltpu.VMEM((quarter, points), f32),
            pltpu.VMEM((quarter, points), f32),
            pltpu.SMEM((2, 1, points), i32),
            pltpu.VMEM((quarter + 1, species, points), f32),
            dma((13,)),
            dma((9,)),
        ],
        compiler_params=pltpu.CompilerParams(vmem_limit_bytes=67043328),
        name="deliver",
    )(field, *rest)
    return (field.reshape(les.shape), state.reshape(lines.shape))


def solution(mesh):
    in_specs = (
        P(None, "grid", "line"),
        P("grid", "line", None, None, None),
        P(None, "grid", "line", None),
        P(None, "grid", "line", None, None),
        P(None, "grid", "line", None),
        P(None, "grid", "line", None),
        P(None, "grid", "line", None),
        P("grid", "line", None),
        P(),
        P(),
        P(),
    )
    out_specs = (P(None, "grid", "line"), P("grid", "line", None, None, None))
    return jax.shard_map(body, mesh=mesh, in_specs=in_specs, out_specs=out_specs, check_vma=False)
```

```python
import functools

import jax
import jax.numpy as jnp
from jax import lax
from jax.experimental import pallas as pl
from jax.experimental.pallas import tpu as pltpu
from jax.sharding import PartitionSpec as P

SEG = 16
TRIP = 48
STEPS = 2
SUBSTEPS = 6
WAVES = 3
CHUNK = 64

les_rate = 0.2
relax_rate = 0.5
splice_weight = 0.5

NAMES = ("grid", "line")
MESH = pl.DeviceIdType.MESH
VMEM = pl.BlockSpec(memory_space=pltpu.VMEM)
SMEM = pl.BlockSpec(memory_space=pltpu.SMEM)
HBM = pl.BlockSpec(memory_space=pltpu.HBM)
f32 = jnp.float32
bf16 = jnp.bfloat16
i32 = jnp.int32

dot = functools.partial(jnp.dot, preferred_element_type=jnp.float32)


def halves(value):
    top = value.astype(bf16)
    return top, (value - top.astype(f32)).astype(bf16)


def column(row):
    points = row.shape[1]
    return jnp.transpose(jnp.broadcast_to(row, (points, points)))


def iota(shape, axis):
    return lax.broadcasted_iota(i32, shape, axis)


def bits(size):
    assert size & (size - 1) == 0
    return size.bit_length() - 1


def when(condition, value):
    return jnp.where(condition, value, 0)


def total_of(value, axis):
    return jnp.sum(value, axis=axis, keepdims=True, dtype=i32)


def kernel(
    slots,
    les_hbm,
    lines_hbm,
    start_hbm,
    owner_hbm,
    line_hbm,
    from_hbm,
    to_hbm,
    rates_hbm,
    frozen_hbm,
    coeff_hbm,
    counts_hbm,
    les_out,
    lines_out,
    tiles_out,
    mask_out,
    keep_out,
    table_out,
    les_ref,
    start_ref,
    owner_ref,
    line_ref,
    from_ref,
    to_ref,
    rates_ref,
    frozen_ref,
    coeff_ref,
    counts_row,
    coeffs_ref,
    apart_ref,
    ends_ref,
    y_ref,
    z_ref,
    s_ref,
    order_ref,
    matrix_ref,
    send_ref,
    recv_00,
    recv_01,
    recv_02,
    recv_10,
    recv_11,
    recv_12,
    sums_0,
    sums_1,
    sums_2,
    mask_ref,
    keep_ref,
    into_ref,
    fold_ref,
    both_ref,
    weight_ref,
    rim_ref,
    field_ref,
    mid_ref,
    middle_ref,
    aim_ref,
    got_ref,
    flat_ref,
    tab_ref,
    tab_smem,
    load_sem,
    tab_sem,
    rim_send,
    rim_recv,
    aim_send,
    aim_recv,
    send_sem,
    recv_sem,
    out_sem,
):
    parts = out_sem.shape[0] - 6
    waves = WAVES
    species, _, lines = les_ref.shape
    points = y_ref.shape[2]
    segments = points // SEG
    size = [lax.axis_size(n) for n in NAMES]
    at = [lax.axis_index(n) for n in NAMES]
    groups = size[0] * size[1]
    me = at[0] * size[1] + at[1]
    total = groups * slots
    blocks = total // points
    recv_refs = ((recv_00, recv_01, recv_02), (recv_10, recv_11, recv_12))
    sums_refs = (sums_0, sums_1, sums_2)

    def place(j):
        peer = (me + j) & (groups - 1)
        return peer, (peer >> bits(size[1]), peer & (size[1] - 1))

    half = groups // 2
    turns = ((half, groups), (0, half // 2), (half // 2, half))
    barrier = pltpu.get_barrier_semaphore()

    def greet(j, carry):
        pl.semaphore_signal(barrier, inc=1, device_id=place(j)[1], device_id_type=MESH)
        return carry

    tables = [
        pltpu.make_async_copy(source, target, load_sem.at[n])
        for n, (source, target) in enumerate(
            [
                (coeff_hbm, coeff_ref),
                (owner_hbm, owner_ref),
                (from_hbm, from_ref),
                (line_hbm, line_ref),
                (to_hbm, to_ref),
                (les_hbm, les_ref),
                (start_hbm, start_ref),
                (counts_hbm, counts_row),
                (rates_hbm, rates_ref),
                (frozen_hbm, frozen_ref),
            ]
        )
    ]
    load = pltpu.make_async_copy(lines_hbm, y_ref, load_sem.at[len(tables)])
    for copy in tables:
        copy.start()
    load.start()
    rim_ref[...] = jnp.zeros_like(rim_ref)
    lax.fori_loop(1, groups, greet, 0)

    rims = []
    for axis in (0, 1):
        for move in (1, size[axis] - 1):
            there = list(at)
            there[axis] = lax.rem(at[axis] + move, size[axis])
            rims.append(tuple(there))

    def rim_copies(step):
        return [
            pltpu.make_async_remote_copy(
                src_ref=field_ref.at[step],
                dst_ref=rim_ref.at[step, k],
                send_sem=rim_send.at[step, k],
                recv_sem=rim_recv.at[step, k],
                device_id=rims[k],
                device_id_type=MESH,
            )
            for k in range(4)
        ]

    inner = [at[0] < size[0] - 1, at[0] > 0, at[1] < size[1] - 1, at[1] > 0]

    def rim_start(step):
        for k, copy in enumerate(rim_copies(step)):
            pl.when(inner[k])(copy.start)

    def rim_wait(step):
        for k, copy in enumerate(rim_copies(step)):
            pl.when(inner[k])(copy.wait_send)
            pl.when(inner[k ^ 1])(copy.wait_recv)

    def aim_copy(j):
        peer, device = place(j)
        return pltpu.make_async_remote_copy(
            src_ref=aim_ref.at[(peer * slots) >> bits(points)],
            dst_ref=got_ref.at[me],
            send_sem=aim_send.at[j],
            recv_sem=aim_recv.at[j],
            device_id=device,
            device_id_type=MESH,
        )

    def turn_of(i, sign):
        low = (me + sign * i) & (half - 1)
        return jnp.where(i < half, me ^ half, me) & half | low

    def data_copy(step, wave, j):
        peer = turn_of(j, 1)
        device = (peer >> bits(size[1]), peer & (size[1] - 1))
        return pltpu.make_async_remote_copy(
            src_ref=send_ref.at[step, peer],
            dst_ref=recv_refs[step][wave].at[j - turns[wave][0]],
            send_sem=send_sem.at[step, j],
            recv_sem=recv_sem.at[step, j],
            device_id=device,
            device_id_type=MESH,
        )

    tables[0].wait()
    lane = iota((points, points), 1)
    row = iota((points, points), 0)
    for n in range(species):
        coeffs_ref[n : n + 1, :] = jnp.full((1, points), coeff_ref[n], f32)
    coeff = coeffs_ref[...]
    root = jnp.sqrt(4.0 * coeff + 1.0)
    theta = -jnp.log(2.0 * coeff / (2.0 * coeff + 1.0 + root))
    scale = 1.0 / (root * (1.0 - jnp.exp(-2.0 * points * theta)))
    along = iota((species, points), 1).astype(f32)
    apart_ref[...] = scale * (jnp.exp(-along * theta) + jnp.exp((along - 2.0 * points) * theta)) - relax_rate / points
    ends_ref[...] = scale * (jnp.exp(-(along + 1.0) * theta) + jnp.exp((along + 1.0 - 2.0 * points) * theta))
    apart = jnp.abs(lane - row)
    ends = jnp.minimum(lane + row, 2 * points - 2 - lane - row)

    def spread(ref, n, index):
        value = jnp.broadcast_to(ref[pl.ds(n, 1), :], (points, points))
        return jnp.take_along_axis(value, index, axis=1, mode="promise_in_bounds")

    def inverse(n, carry):
        top, rest = halves(spread(apart_ref, n, apart) + spread(ends_ref, n, ends))
        matrix_ref[n] = jnp.concatenate([top, rest], axis=1)
        return carry

    lax.fori_loop(0, species, inverse, 0, unroll=8)
    for copy in tables[1:]:
        copy.wait()
    field_ref[0] = les_ref[...].reshape(species, lines)
    pl.semaphore_wait(barrier, groups - 1)
    rim_start(0)


    for step in range(STEPS):
        owner = owner_ref[step : step + 1, :]
        rank = total_of(when((column(owner) == owner) & (row < lane), 1), 0)
        spot = column(owner * slots + rank)
        turn = (owner - me) & (half - 1)
        key = (jnp.where((owner ^ me) & half == 0, half, 0) + turn) * lines + iota((1, points), 1)
        spot_sorted = total_of(when(column(key) < key, 1), 0)
        first = step * (blocks + 2) + blocks
        tab_ref[first] = spot_sorted
        sorted_code = column(iota((1, points), 1) * 8 + counts_row[...])
        order = total_of(when(column(spot_sorted) == lane, sorted_code), 0)
        tab_ref[first + 1] = order
        order_ref[step] = jnp.broadcast_to(order >> 3, (species, points))
        turn = (SEG * (rank - from_ref[step : step + 1, :])) & (points - 1)
        code = column(spot_sorted * points + turn)
        aim = column(line_ref[step : step + 1, :] * segments + to_ref[step : step + 1, :] + 1)
        for b in range(blocks):
            hit = spot == lane + b * points
            tab_ref[step * (blocks + 2) + b] = total_of(when(hit, code), 0)
            aim_ref[b, step : step + 1, :] = total_of(when(hit, aim), 0)
    send_rows = STEPS * (blocks + 2)
    send_table = pltpu.make_async_copy(tab_ref.at[pl.ds(0, send_rows)], tab_smem.at[pl.ds(0, send_rows)], tab_sem.at[0])
    send_table.start()


    flat_y = y_ref.reshape(lines * species, points)
    flat_z = z_ref.reshape(lines * species, points)

    def diffuse(step):
        rel = lane - column(start_ref[step : step + 1, :])
        third = TRIP // 3
        source = jnp.where(
            rel < third,
            3 * rel,
            jnp.where(rel < 2 * third, 3 * (2 * third - 1 - rel) + 1, 3 * (rel - 2 * third) + 2),
        )
        index = jnp.where((rel >= 0) & (rel < TRIP), source + (lane - rel), lane)

        def one(s, carry):
            y = flat_y[pl.ds(s, lines, stride=species), :]
            y = jnp.take_along_axis(y, index, axis=1, mode="promise_in_bounds")
            right = matrix_ref[s]
            out = dot(jnp.concatenate(halves(y), axis=1), jnp.concatenate([right, right], axis=0))
            flat_z[pl.ds(s, lines, stride=species), :] = out[:, :points] + out[:, points:]
            return carry

        lax.fori_loop(0, species, one, 0, unroll=12)

    lane_s = lax.broadcasted_iota(i32, (species, points), 1)

    def middle(step):
        field = field_ref[step]
        up, down, left, right = (rim_ref[step, k] for k in range(4))
        before = pltpu.roll(jnp.where(lane_s == points - 1, left, field), 1, 1)
        after = pltpu.roll(jnp.where(lane_s == 0, right, field), points - 1, 1)
        mid_ref[...] = field + les_rate * (up + down + before + after - 4.0 * field)

    joint = jnp.dot(
        frozen_ref[...], rates_ref[...], precision=lax.Precision.HIGHEST, preferred_element_type=f32
    )
    joint_top, joint_rest = halves(joint)
    wide = (2 * species, 6 * species)
    place_c = iota(wide, 1)
    block_c = sum((place_c >= species * n).astype(i32) for n in range(1, 6))
    pick = jnp.where(
        iota((species, 6 * species), 0) == (place_c - species * block_c)[:species], 1.0, 0.0
    ).astype(bf16)
    twice_top = dot(jnp.concatenate([joint_top.astype(f32)] * 2, axis=0).astype(bf16), pick)
    twice_rest = dot(jnp.concatenate([joint_rest.astype(f32)] * 2, axis=0).astype(bf16), pick)
    entries = jnp.where((block_c >> 1) == 1, twice_rest, twice_top)
    matrix = jnp.where((iota(wide, 0) >= species).astype(i32) == (block_c & 1), entries, 0.0).astype(bf16)

    segment = lane_s // SEG

    def pack(step, peer):
        tile = jnp.zeros((species, points), f32)
        first = peer * slots
        for k in range(slots):
            code = tab_smem[step * (blocks + 2) + (first >> bits(points)), 0, (first & (points - 1)) + k]
            value = pltpu.roll(s_ref[code >> bits(points)], code & (points - 1), 1)
            tile = jnp.where(segment == k, value, tile)
        return tile

    def chemistry(step, base):
        orders = step * (blocks + 2) + blocks + 1
        mid = middle_ref[...]
        codes = [tab_smem[orders, 0, base + i] for i in range(CHUNK)]
        for sub in range(SUBSTEPS):
            for q in range(0, CHUNK, 4):
                columns = []
                state = []
                for h in (0, 2):
                    if sub == 0:
                        y = jnp.concatenate(
                            [
                                z_ref[codes[i] >> 3] + jnp.broadcast_to(mid[:, base + i : base + i + 1], (species, points))
                                for i in (q + h, q + h + 1)
                            ],
                            axis=0,
                        )
                    else:
                        y = s_ref[pl.ds(base + q + h, 2)].reshape(2 * species, points)
                    state.append(y)
                    top, rest = halves(jnp.tanh(y))
                    columns.append(jnp.concatenate([top, top, rest], axis=0))
                change = dot(matrix, jnp.concatenate(columns, axis=1))
                for h in (0, 1):
                    for k in (0, 1):
                        i = q + 2 * h + k
                        factor = jnp.where(codes[i] & 7 > sub, f32(1.0), f32(0.0))
                        rows = slice(k * species, (k + 1) * species)
                        s_ref[base + i] = state[h][rows] + factor * change[rows, h * points : (h + 1) * points]

    def exchange(step):
        middle_ref[...] = relax_rate * jnp.take_along_axis(
            mid_ref[...], order_ref[step], axis=1, mode="promise_in_bounds"
        )
        many = CHUNK // slots

        def wrap(i):
            peer = turn_of(i, 1)
            send_ref[step, peer] = pack(step, peer)

        for c in range(lines // CHUNK):
            chemistry(step, c * CHUNK)
            for n in range(many + 2):
                if n < many:
                    wrap(c * many + n)
                if n >= 2:
                    turn = c * many + n - 2
                    data_copy(step, 1 if turn < half // 2 else 2, turn).start()

        def near(i, carry):
            for n in range(2):
                wrap(half + 2 * i + n)
            for n in range(2):
                before = half + 2 * (i - 1) + n

                @pl.when(before > half)
                def _():
                    data_copy(step, 0, before).start()

            return carry

        lax.fori_loop(0, half // 2, near, 0)
        recv_refs[step][0][0] = send_ref[step, me]
        for n in range(groups - 2, groups):
            data_copy(step, 0, n).start()

    def arrivals():
        number = iota((total, 1), 0)
        lane_t = iota((total, points), 1)
        number_r = iota((1, total), 1)
        offset = (me * slots) & (points - 1)
        mine = offset + (iota((total, points), 0) & (slots - 1))
        for step in range(STEPS):
            for r in range(groups):
                flat_ref[r * slots : (r + 1) * slots, :] = jnp.broadcast_to(
                    got_ref[r, step : step + 1, :], (slots, points)
                )
            code = total_of(when(lane_t == mine, flat_ref[...]), 1)
            valid = code > 0
            code = code - 1
            line = jnp.where(valid, code >> bits(segments), lines)
            seg = code & (segments - 1)
            source = number >> bits(slots)
            deep = (me - source) & (half - 1)
            late = jnp.where((source ^ me) & half == 0, 0, jnp.where(deep >= half // 2, 2, 1))
            slot = jnp.where(late == 2, deep - half // 2, deep)
            line = line + late * (lines + 1)
            line_c = jnp.broadcast_to(line, (total, points))
            line_r = jnp.concatenate(
                [jnp.transpose(line_c[b * points : (b + 1) * points])[:1] for b in range(blocks)], axis=1
            )
            key_r = line_r * total + number_r
            key_c = line * total + number
            below = key_r < key_c
            position = total_of(when(below, 1), 1)
            same = total_of(when(below & (line_r == line), 1), 1)
            turn = (SEG * (seg - (number & (slots - 1)))) & (points - 1)
            value = slot * points + turn
            kind = seg * 2 + when(same == 0, 1)
            base = send_rows + step * (blocks + waves)
            for b in range(blocks):
                hit = position == lane_t + b * points
                tab_ref[base + b] = total_of(when(hit, value), 0)
                kinds = column(total_of(when(hit, kind), 0))
                at_b = pl.ds(b * points, points)
                mask_ref[step, at_b, :] = jnp.where((kinds >> 1) == (lane >> bits(SEG)), splice_weight, 0.0)
                keep_ref[step, at_b, :] = jnp.where((kinds & 1) == 1, 0.0, 1.0)
            starts = (0, total // 2, total // 2 + total // 4, total)
            in_c = jnp.zeros((total, points), jnp.bool_)
            in_r = jnp.zeros((lines, total), jnp.bool_)
            for w in range(waves):
                aim_c = lane_t + w * (lines + 1)
                upto = total_of(when(line_c <= aim_c, 1), 0)
                many = total_of(when(line_c == aim_c, 1), 0)
                tab_ref[base + blocks + w] = jnp.where(many > 0, upto - 1 - starts[w], starts[w + 1] - starts[w])
                in_c = in_c | (line_c == aim_c)
                in_r = in_r | (line_r == iota((lines, total), 0) + w * (lines + 1))
            lands = jnp.where(in_r, 1.0, 0.0).astype(bf16)
            covers = jnp.where(seg == (lane_t >> bits(SEG)), 1.0, 0.0).astype(bf16)
            weight_ref[step] = 1.0 - splice_weight * dot(lands, covers)
            into_ref[step] = jnp.where(in_c, splice_weight, 0.0)
        rows = STEPS * (blocks + waves)
        copy = pltpu.make_async_copy(
            tab_ref.at[pl.ds(send_rows, rows)], tab_smem.at[pl.ds(send_rows, rows)], tab_sem.at[1]
        )
        copy.start()
        copy.wait()

    def prepare(step):
        def rows(j, carry):
            block = jnp.broadcast_to(into_ref[step, pl.ds(j, 1), :], (SEG, lines))
            source = j >> bits(slots)
            first = jnp.where(source & half == me & half, half, 0) + ((me - source) & (half - 1))
            first = first * points + (j & (slots - 1)) * SEG
            fold_ref[pl.ds(pl.multiple_of(first, SEG), SEG), :] = block.astype(bf16)
            return carry

        if slots < segments:
            fold_ref[...] = jnp.zeros_like(fold_ref)
        lax.fori_loop(0, total, rows, 0, unroll=8)

        places = step * (blocks + 2) + blocks

        def scale(l, sums):
            value = s_ref[tab_smem[places, 0, l]] * weight_ref[step, pl.ds(l, 1), :]
            y_ref[l] = value
            return jnp.where(lane_s == l, jnp.sum(value, axis=1, keepdims=True), sums)

        return lax.fori_loop(0, lines, scale, jnp.zeros((species, points), f32), unroll=8)

    def collect(step, wave):
        def finish(j, carry):
            data_copy(step, wave, j).wait()
            return carry

        low, high = turns[wave]
        lax.fori_loop(low + (wave == 0), high, finish, 0)

    def filtered(step, wave):
        low, high = turns[wave]
        for i in range(low, high):
            value = recv_refs[step][wave][i - low]
            rest = value - value.astype(bf16).astype(f32)
            both_ref[:, i * points : (i + 1) * points] = jnp.concatenate([value, rest], axis=0).astype(bf16)
        acc = dot(both_ref[:, low * points : high * points], fold_ref[low * points : high * points, :])
        return acc[:species] + acc[species:]

    def run(step, wave, acc):
        base = send_rows + step * (blocks + waves)
        begin = sum(high - low for low, high in turns[:wave]) * slots
        end = begin + (turns[wave][1] - turns[wave][0]) * slots

        at_row = base + (begin >> bits(points))
        at_lane = begin & (points - 1)
        assert at_lane + end - begin <= points

        def one(i, acc):
            code = tab_smem[at_row, 0, at_lane + i]
            value = pltpu.roll(recv_refs[step][wave][code >> bits(points)], code & (points - 1), 1)
            acc = value * mask_ref[step, pl.ds(begin + i, 1), :] + acc * keep_ref[step, pl.ds(begin + i, 1), :]
            sums_refs[wave][i] = acc
            return acc

        sums_refs[wave][end - begin] = jnp.zeros((species, points), f32)
        lax.fori_loop(0, end - begin, one, jnp.zeros((species, points), f32), unroll=32)

    def receive(step, sums, les_done, out):
        base = send_rows + step * (blocks + waves)

        def settle(which):
            def one(l, carry):
                value = y_ref[l]
                for w in which:
                    value = value + sums_refs[w][tab_smem[base + blocks + w, 0, l]]
                y_ref[l] = value
                return carry

            return one

        for wave in range(waves):
            collect(step, wave)
            if wave + 1 < waves:
                run(step, wave, None)
            if wave + 2 == waves:
                lax.fori_loop(0, lines, settle(range(waves - 1)), 0, unroll=8)
                for copy in out[0]:
                    copy.start()
            if wave + 1 == waves:
                for copy in out[1]:
                    copy.start()
            sums = sums + filtered(step, wave)
        les_done(0.5 * mid_ref[...] + (0.5 / points) * sums)
        if not out[0]:
            run(step, waves - 1, None)
            lax.fori_loop(0, lines, settle((waves - 1,)), 0, unroll=32)

    load.wait()
    diffuse(0)
    def aim_start(j, carry):
        aim_copy(j).start()
        return carry

    lax.fori_loop(1, groups, aim_start, 0)
    got_ref[me] = aim_ref[(me * slots) >> bits(points)]

    rim_wait(0)
    middle(0)
    send_table.wait()
    exchange(0)

    def aim_finish(j, carry):
        aim_copy(j).wait()
        return carry

    lax.fori_loop(1, groups, aim_finish, 0)
    arrivals()
    sums = prepare(0)

    def again(field):
        field_ref[1] = field
        rim_start(1)

    receive(0, sums, again, ((), ()))
    diffuse(1)
    rim_wait(1)
    middle(1)
    exchange(1)
    sums = prepare(1)
    final = STEPS - 1
    begin = total - total // 4
    base = send_rows + final * (blocks + waves)
    pairs = [
        (mask_ref.at[final, pl.ds(begin, total - begin)], mask_out),
        (keep_ref.at[final, pl.ds(begin, total - begin)], keep_out),
        (tab_ref.at[base + (begin >> bits(points))], table_out.at[0]),
        (tab_ref.at[base + blocks + waves - 1], table_out.at[1]),
    ]
    for p in range(parts):
        at_p = pl.ds(p * lines // parts, lines // parts)
        pairs.append((y_ref.at[at_p], lines_out.at[at_p]))
    early = [pltpu.make_async_copy(a, b, out_sem.at[n]) for n, (a, b) in enumerate(pairs)]
    last = pltpu.make_async_copy(les_ref, les_out, out_sem.at[parts + 4])
    tiles = pltpu.make_async_copy(recv_refs[final][waves - 1], tiles_out, out_sem.at[parts + 5])

    def finish(field):
        les_ref[...] = field.reshape(species, 1, lines)
        last.start()

    receive(1, sums, finish, (early, [tiles]))
    for copy in early + [tiles, last]:
        copy.wait()


def deliver_kernel(
    les_in,
    lines_in,
    tiles_in,
    mask_in,
    keep_in,
    table_in,
    les_out,
    lines_out,
    les_ref,
    lines_ref,
    tiles_ref,
    mask_ref,
    keep_ref,
    table_ref,
    sums_ref,
    in_sem,
    out_sem,
):
    lines, species, points = lines_ref.shape
    parts = out_sem.shape[0] - 1
    size = lines // parts
    many = mask_ref.shape[0]
    small = [(table_in, table_ref), (tiles_in, tiles_ref), (mask_in, mask_ref), (keep_in, keep_ref), (les_in, les_ref)]
    at = [pl.ds(p * size, size) for p in range(parts)]
    takes = small + [(lines_in.at[a], lines_ref.at[a]) for a in at]
    takes = [pltpu.make_async_copy(a, b, in_sem.at[n]) for n, (a, b) in enumerate(takes)]
    gives = [(lines_ref.at[a], lines_out.at[a]) for a in at] + [(les_ref, les_out)]
    gives = [pltpu.make_async_copy(a, b, out_sem.at[n]) for n, (a, b) in enumerate(gives)]
    for take in takes:
        take.start()
    for take in takes[: len(small)]:
        take.wait()
    gives[parts].start()

    def run(i, acc):
        code = table_ref[0, 0, points - many + i]
        value = pltpu.roll(tiles_ref[code >> bits(points)], code & (points - 1), 1)
        acc = value * mask_ref[pl.ds(i, 1), :] + acc * keep_ref[pl.ds(i, 1), :]
        sums_ref[i] = acc
        return acc

    sums_ref[many] = jnp.zeros((species, points), f32)
    lax.fori_loop(0, many, run, jnp.zeros((species, points), f32), unroll=32)

    def settle(l, carry):
        lines_ref[l] = lines_ref[l] + sums_ref[table_ref[1, 0, l]]
        return carry

    for p in range(parts):
        takes[len(small) + p].wait()
        lax.fori_loop(p * size, (p + 1) * size, settle, 0, unroll=size)
        gives[p].start()
    for give in gives:
        give.wait()


def body(
    les,
    lines,
    triplet_start,
    splice_owner,
    splice_line,
    splice_from,
    splice_to,
    chem_counts,
    diffusivity,
    rates,
    frozen_inverse,
):
    groups = lax.axis_size("grid") * lax.axis_size("line")
    _, _, count, species, points = lines.shape
    segments = points // SEG
    slots = min(segments, max(2, 2 * count // groups))
    total = groups * slots
    blocks = total // points
    rows = STEPS * (2 * blocks + 2 + WAVES)

    dma = pltpu.SemaphoreType.DMA
    quarter = total // 4
    field, *rest = pl.pallas_call(
        functools.partial(kernel, slots),
        out_shape=(
            jax.ShapeDtypeStruct((species, 1, count), f32),
            jax.ShapeDtypeStruct((count, species, points), f32),
            jax.ShapeDtypeStruct((groups // 4, species, points), f32),
            jax.ShapeDtypeStruct((quarter, points), f32),
            jax.ShapeDtypeStruct((quarter, points), f32),
            jax.ShapeDtypeStruct((2, 1, points), i32),
        ),
        in_specs=[HBM] * 11,
        out_specs=(HBM,) * 6,
        scratch_shapes=[
            pltpu.VMEM((species, 1, count), f32),
            *[pltpu.VMEM((STEPS, count), i32)] * 5,
            pltpu.VMEM((species, species), f32),
            pltpu.VMEM((species, species), f32),
            pltpu.SMEM((species,), f32),
            pltpu.VMEM((1, count), i32),
            *[pltpu.VMEM((species, points), f32)] * 3,
            pltpu.VMEM((count, species, points), f32),
            pltpu.VMEM((count, species, points), f32),
            pltpu.VMEM((count, species, points), f32),
            pltpu.VMEM((STEPS, species, count), i32),
            pltpu.VMEM((species, points, 2 * points), bf16),
            pltpu.VMEM((STEPS, groups, species, points), f32),
            *[
                pltpu.VMEM((groups // part, species, points), f32)
                for part in (2, 4, 4) * STEPS
            ],
            pltpu.VMEM((total // 2 + 1, species, points), f32),
            *[pltpu.VMEM((total // 4 + 1, species, points), f32)] * 2,
            pltpu.VMEM((STEPS, total, points), f32),
            pltpu.VMEM((STEPS, total, points), f32),
            pltpu.VMEM((STEPS, total, count), f32),
            pltpu.VMEM((groups * points, count), bf16),
            pltpu.VMEM((2 * species, groups * points), bf16),
            pltpu.VMEM((STEPS, count, points), f32),
            pltpu.VMEM((STEPS, 4, species, count), f32),
            pltpu.VMEM((STEPS, species, count), f32),
            pltpu.VMEM((species, count), f32),
            pltpu.VMEM((species, count), f32),
            pltpu.VMEM((blocks, STEPS, points), i32),
            pltpu.VMEM((groups, STEPS, points), i32),
            pltpu.VMEM((total, points), i32),
            pltpu.VMEM((rows, 1, points), i32),
            pltpu.SMEM((rows, 1, points), i32),
            dma((11,)),
            dma((2,)),
            dma((STEPS, 4)),
            dma((STEPS, 4)),
            dma((groups,)),
            dma((groups,)),
            dma((STEPS, groups)),
            dma((STEPS, groups)),
            dma((10,)),
        ],
        compiler_params=pltpu.CompilerParams(
            collective_id=0, has_side_effects=True, vmem_limit_bytes=67043328
        ),
        name="steps",
    )(
        les.reshape(species, 1, count),
        lines.reshape(count, species, points),
        triplet_start.reshape(STEPS, count),
        splice_owner.reshape(STEPS, count),
        splice_line.reshape(STEPS, count),
        splice_from.reshape(STEPS, count),
        splice_to.reshape(STEPS, count),
        rates,
        frozen_inverse,
        diffusivity,
        chem_counts.reshape(1, count),
    )
    field, state = pl.pallas_call(
        deliver_kernel,
        out_shape=(
            jax.ShapeDtypeStruct(field.shape, f32),
            jax.ShapeDtypeStruct((count, species, points), f32),
        ),
        in_specs=[HBM] * 6,
        out_specs=(HBM, HBM),
        scratch_shapes=[
            pltpu.VMEM(field.shape, f32),
            pltpu.VMEM((count, species, points), f32),
            pltpu.VMEM((groups // 4, species, points), f32),
            pltpu.VMEM((quarter, points), f32),
            pltpu.VMEM((quarter, points), f32),
            pltpu.SMEM((2, 1, points), i32),
            pltpu.VMEM((quarter + 1, species, points), f32),
            dma((9,)),
            dma((5,)),
        ],
        compiler_params=pltpu.CompilerParams(vmem_limit_bytes=67043328),
        name="deliver",
    )(field, *rest)
    return (field.reshape(les.shape), state.reshape(lines.shape))


def solution(mesh):
    in_specs = (
        P(None, "grid", "line"),
        P("grid", "line", None, None, None),
        P(None, "grid", "line", None),
        P(None, "grid", "line", None, None),
        P(None, "grid", "line", None),
        P(None, "grid", "line", None),
        P(None, "grid", "line", None),
        P("grid", "line", None),
        P(),
        P(),
        P(),
    )
    out_specs = (P(None, "grid", "line"), P("grid", "line", None, None, None))
    return jax.shard_map(body, mesh=mesh, in_specs=in_specs, out_specs=out_specs, check_vma=False)
```
